8 devices in a mesh: dp: 2 (over z, y), tp: 4 (over x, core).
Axes of the slice: x: 2, y: 2, z: 1, core: 2. Of those that a mesh axis runs over, the one named last changes fastest.
Arguments:
- hidden_in: bfloat16 [32, 512, 768], P('dp', 'tp'), parts along dimension 0
- ln1_gain: bfloat16 [768], replicated
- ln1_bias: bfloat16 [768], replicated
- w_q: bfloat16 [768, 768], P(None, 'tp')
- b_q: bfloat16 [768], P('tp')
- w_k: bfloat16 [768, 768], P(None, 'tp')
- w_v: bfloat16 [768, 768], P(None, 'tp')
- b_v: bfloat16 [768], P('tp')
- w_o: bfloat16 [768, 768], P('tp')
- b_o: bfloat16 [768], replicated
- ln2_gain: bfloat16 [768], replicated
- ln2_bias: bfloat16 [768], replicated
- w_fc1: bfloat16 [768, 3072], P(None, 'tp')
- b_fc1: bfloat16 [3072], P('tp')
- w_fc2: bfloat16 [3072, 768], P('tp')
- b_fc2: bfloat16 [768], replicated
- post_gain: bfloat16 [768], replicated
- post_bias: bfloat16 [768], replicated
- w_ck: bfloat16 [4, 768, 768], P(None, None, 'tp')
- w_cv: bfloat16 [4, 768, 768], P(None, None, 'tp')
- b_cv: bfloat16 [4, 768], P(None, 'tp')
Outputs:
- output 1: bfloat16 [32, 512, 768], P('dp', 'tp'), parts along dimension 0
- output 2: bfloat16 [4, 32, 512, 12, 64], P(None, 'dp', None, 'tp'), parts along dimension 1
- output 3: bfloat16 [4, 32, 512, 12, 64], P(None, 'dp', None, 'tp'), parts along dimension 1
There are 2 independent parts. The reference program is written for one: setup_inputs(seed, part) draws one part's arguments, and reference() takes and returns one part's arrays. A program takes and returns all parts, laid end to end along the dimension named above; an argument that names none is the same for every part.
All inputs are finite; a program needn't handle non-finite values.
Results may differ from the reference program's by a relative error of at most 0.0152507.
Values are sent between devices in bfloat16 or wider.
A program may use at most 1 GiB of HBM per device.

```python
import jax
import jax.numpy as jnp
from jax import lax

BATCH_SIZE = 16
NUM_FRAMES = 512
D_MODEL = 768
NUM_HEADS = 12
FF_DIM = 3072
NUM_LAYERS = 4

HEAD_DIM = D_MODEL // NUM_HEADS
ATTN_SCALE = HEAD_DIM ** -0.25
LN_EPS = 1e-5


def draw_normal(key, shape, scale, offset=0.0):
    sample = jax.random.normal(key, shape, jnp.float32)
    return (offset + scale * sample).astype(jnp.bfloat16)


def setup_inputs(seed: int = 0, part: int = 0) -> dict:
    keys = jax.random.split(jax.random.key(seed), 20)
    part_key = jax.random.fold_in(jax.random.key(seed + 1), part)
    w_scale = D_MODEL ** -0.5
    ffn_scale = FF_DIM ** -0.5
    return {
        "hidden_in": draw_normal(part_key, (BATCH_SIZE, NUM_FRAMES, D_MODEL), 1.0),
        "ln1_gain": draw_normal(keys[0], (D_MODEL,), 0.2, 1.0),
        "ln1_bias": draw_normal(keys[1], (D_MODEL,), 0.3),
        "w_q": draw_normal(keys[2], (D_MODEL, D_MODEL), 1.3 * w_scale),
        "b_q": draw_normal(keys[3], (D_MODEL,), 0.5),
        "w_k": draw_normal(keys[4], (D_MODEL, D_MODEL), 1.3 * w_scale),
        "w_v": draw_normal(keys[5], (D_MODEL, D_MODEL), w_scale),
        "b_v": draw_normal(keys[6], (D_MODEL,), 0.5),
        "w_o": draw_normal(keys[7], (D_MODEL, D_MODEL), w_scale),
        "b_o": draw_normal(keys[8], (D_MODEL,), 0.3),
        "ln2_gain": draw_normal(keys[9], (D_MODEL,), 0.2, 1.0),
        "ln2_bias": draw_normal(keys[10], (D_MODEL,), 0.3),
        "w_fc1": draw_normal(keys[11], (D_MODEL, FF_DIM), w_scale),
        "b_fc1": draw_normal(keys[12], (FF_DIM,), 0.5),
        "w_fc2": draw_normal(keys[13], (FF_DIM, D_MODEL), 1.5 * ffn_scale),
        "b_fc2": draw_normal(keys[14], (D_MODEL,), 0.3),
        "post_gain": draw_normal(keys[15], (D_MODEL,), 0.2, 1.0),
        "post_bias": draw_normal(keys[16], (D_MODEL,), 0.3),
        "w_ck": draw_normal(keys[17], (NUM_LAYERS, D_MODEL, D_MODEL), w_scale),
        "w_cv": draw_normal(keys[18], (NUM_LAYERS, D_MODEL, D_MODEL), w_scale),
        "b_cv": draw_normal(keys[19], (NUM_LAYERS, D_MODEL), 0.5),
    }


def layer_norm(values, ln_gain, ln_bias):
    centered = values.astype(jnp.float32)
    centered = centered - jnp.mean(centered, axis=-1, keepdims=True)
    row_var = jnp.mean(centered * centered, axis=-1, keepdims=True)
    normed = centered * lax.rsqrt(row_var + LN_EPS)
    return (normed * ln_gain.astype(jnp.float32) + ln_bias.astype(jnp.float32)).astype(jnp.bfloat16)


def split_heads(flat):
    return flat.reshape(BATCH_SIZE, NUM_FRAMES, NUM_HEADS, HEAD_DIM).transpose(0, 2, 1, 3).reshape(BATCH_SIZE * NUM_HEADS, NUM_FRAMES, HEAD_DIM)


def head_attention(triple):
    q_head, k_head, v_head = triple
    scores = jnp.dot(q_head, k_head.T, preferred_element_type=jnp.float32)
    attn_probs = jax.nn.softmax(scores, axis=-1).astype(jnp.bfloat16)
    return jnp.dot(attn_probs, v_head, preferred_element_type=jnp.float32).astype(jnp.bfloat16)


def reference(hidden_in, ln1_gain, ln1_bias, w_q, b_q, w_k, w_v, b_v, w_o, b_o, ln2_gain, ln2_bias, w_fc1, b_fc1, w_fc2, b_fc2, post_gain, post_bias, w_ck, w_cv, b_cv):
    tok_rows = BATCH_SIZE * NUM_FRAMES
    flat_in = hidden_in.reshape(tok_rows, D_MODEL)
    normed1 = layer_norm(flat_in, ln1_gain, ln1_bias)
    q_flat = ((jnp.dot(normed1, w_q, preferred_element_type=jnp.float32) + b_q.astype(jnp.float32)) * ATTN_SCALE).astype(jnp.bfloat16)
    k_flat = (jnp.dot(normed1, w_k, preferred_element_type=jnp.float32) * ATTN_SCALE).astype(jnp.bfloat16)
    v_flat = (jnp.dot(normed1, w_v, preferred_element_type=jnp.float32) + b_v.astype(jnp.float32)).astype(jnp.bfloat16)
    attn_heads = lax.map(head_attention, (split_heads(q_flat), split_heads(k_flat), split_heads(v_flat)))
    attn_flat = attn_heads.reshape(BATCH_SIZE, NUM_HEADS, NUM_FRAMES, HEAD_DIM).transpose(0, 2, 1, 3).reshape(tok_rows, D_MODEL)
    attn_out = (jnp.dot(attn_flat, w_o, preferred_element_type=jnp.float32) + b_o.astype(jnp.float32)).astype(jnp.bfloat16)
    resid_one = (flat_in.astype(jnp.float32) + attn_out.astype(jnp.float32)).astype(jnp.bfloat16)
    normed2 = layer_norm(resid_one, ln2_gain, ln2_bias)
    hidden_act = jax.nn.gelu(jnp.dot(normed2, w_fc1, preferred_element_type=jnp.float32) + b_fc1.astype(jnp.float32), approximate=False).astype(jnp.bfloat16)
    mlp_out = (jnp.dot(hidden_act, w_fc2, preferred_element_type=jnp.float32) + b_fc2.astype(jnp.float32)).astype(jnp.bfloat16)
    resid_two = (resid_one.astype(jnp.float32) + mlp_out.astype(jnp.float32)).astype(jnp.bfloat16)
    enc_flat = layer_norm(resid_two, post_gain, post_bias)

    def cache_layer(layer_weights):
        wk_layer, wv_layer, bv_layer = layer_weights
        k_layer = jnp.dot(enc_flat, wk_layer, preferred_element_type=jnp.float32).astype(jnp.bfloat16)
        v_layer = (jnp.dot(enc_flat, wv_layer, preferred_element_type=jnp.float32) + bv_layer.astype(jnp.float32)).astype(jnp.bfloat16)
        return k_layer, v_layer

    k_all, v_all = lax.map(cache_layer, (w_ck, w_cv, b_cv))
    cache_shape = (NUM_LAYERS, BATCH_SIZE, NUM_FRAMES, NUM_HEADS, HEAD_DIM)
    return enc_flat.reshape(BATCH_SIZE, NUM_FRAMES, D_MODEL), k_all.reshape(cache_shape), v_all.reshape(cache_shape)
```

```python
import functools

import jax
import jax.numpy as jnp
from jax import lax
from jax.experimental import pallas as pl
from jax.experimental.pallas import tpu as pltpu
from jax.sharding import PartitionSpec as P

HEAD_DIM = 64
ATTN_SCALE = HEAD_DIM ** -0.25
LN_EPS = 1e-5
SQRT_HALF = 0.5 ** 0.5
MESH = pl.DeviceIdType.MESH
BF16, F32 = jnp.bfloat16, jnp.float32

CLIPS, FRAMES, WIDTH, HIDDEN = 16, 512, 768, 3072
LOC_FRAMES = FRAMES // 4
SHARED, ONLY = 4, 2
SLOTS = SHARED + ONLY
LAG = 2
LN_ROWS = 64
SEND_ORDER = ("q", "k", "v", 0, "o", 1, 2, "w1a", "w1b", "w2a", "w2b", 3, 4, 5)

NT = (((1,), (1,)), ((), ()))
NN = (((1,), (0,)), ((), ()))


def dot(lhs, rhs, dims=NN):
    return lax.dot_general(lhs, rhs, dims, preferred_element_type=F32)


def norm_rows(values, gain, bias):
    centered = values.astype(F32)
    centered = centered - jnp.mean(centered, axis=-1, keepdims=True)
    row_var = jnp.mean(centered * centered, axis=-1, keepdims=True)
    return (centered * lax.rsqrt(row_var + LN_EPS) * gain + bias).astype(BF16)


def only_clip(chip, core, slot):
    return 2 * SHARED + (2 * chip + core) * ONLY + slot


def clip_of(chip, core, slot):
    return only_clip(chip, core, slot) if slot < ONLY else core * SHARED + slot - ONLY


def rows_of(ref, start, count):
    return ref.at[pl.ds(pl.multiple_of(start, 16), count), :]


def encoder_kernel(x_hbm, wq_hbm, wk_hbm, wv_hbm, wo_hbm, w1_hbm, w2_hbm, rep_ref, loc_hbm, e_hbm,
                   xbuf, wq, wk, wv, wo, w1, w2, small, abuf, qbuf, ktbuf, vbuf, obuf, mbuf, gbuf, acc, bias,
                   x_send, x_recv, x_loc, w_send, w_recv, w_loc, s_send, s_recv, s_loc, e_send, e_recv, e_loc):
    group, tp = lax.axis_index("dp"), lax.axis_index("tp")
    chip, core = tp // 2, tp % 2
    other_chip, other_core = 1 - chip, 1 - core
    t_sib = 2 * chip + other_core
    t_far = 2 * other_chip + core
    t_diag = 2 * other_chip + other_core
    sib = {"dp": group, "tp": t_sib}
    far = {"dp": group, "tp": t_far}
    diag = {"dp": group, "tp": t_diag}
    side = {"dp": 1 - group, "tp": tp}

    def remote(src, dst, send, recv, device):
        return pltpu.make_async_remote_copy(src_ref=src, dst_ref=dst, send_sem=send, recv_sem=recv, device_id=device, device_id_type=MESH)

    def frames(slot, owner):
        return xbuf.at[slot, pl.ds(pl.multiple_of(owner * LOC_FRAMES, LOC_FRAMES), LOC_FRAMES), :]

    def x_copy(slot, link):
        device, there_chip, there_core = ((sib, chip, other_core), (far, other_chip, core), (diag, other_chip, other_core))[link]
        return remote(x_hbm.at[clip_of(there_chip, there_core, slot)], frames(slot, tp), x_send.at[slot, link], x_recv.at[slot, link], device)

    def x_local(slot):
        return pltpu.make_async_copy(x_hbm.at[clip_of(chip, core, slot)], frames(slot, tp), x_loc.at[slot])

    def x_wait(slot):
        pltpu.make_async_copy(x_hbm.at[0], frames(slot, tp), x_loc.at[slot]).wait()
        for link, owner in enumerate((t_sib, t_far, t_diag)):
            remote(x_hbm.at[0], frames(slot, owner), x_send.at[slot, link], x_recv.at[slot, link], sib).wait_recv()

    units = {
        "q": (0, wq_hbm, wq, 192, 0, 192), "k": (1, wk_hbm, wk, 192, 0, 192), "v": (2, wv_hbm, wv, 192, 0, 192),
        "o": (3, wo_hbm, wo, 192, 0, 192),
        "w1a": (4, w1_hbm, w1, 768, 0, 384), "w1b": (5, w1_hbm, w1, 768, 384, 384),
        "w2a": (6, w2_hbm, w2, 768, 0, 384), "w2b": (7, w2_hbm, w2, 768, 384, 384),
    }

    def w_local(name):
        idx, src, dst, shard, first, count = units[name]
        return pltpu.make_async_copy(src.at[pl.ds(first, count), :], rows_of(dst, tp * shard + first, count), w_loc.at[idx])

    def w_sib(name, owner):
        idx, src, dst, shard, first, count = units[name]
        return remote(src.at[pl.ds(first, count), :], rows_of(dst, owner * shard + first, count), w_send.at[idx, 0], w_recv.at[idx, 0], sib)

    def w_far(name, owner):
        idx, src, dst, shard, first, count = units[name]
        half = count // 2
        return remote(rows_of(src, first + group * half, half), rows_of(dst, owner * shard + first + group * half, half),
                      w_send.at[idx, 1], w_recv.at[idx, 1], far)

    def w_relay(name, owner, part, sem, recv, device):
        idx, src, dst, shard, first, count = units[name]
        half = count // 2
        piece = rows_of(dst, owner * shard + first + part * half, half)
        return remote(piece, piece, w_send.at[idx, sem], w_recv.at[idx, recv], device)

    def w_start(name):
        w_far(name, tp).start()
        w_local(name).start()
        w_sib(name, tp).start()

    def w_stage1(name):
        w_far(name, t_far).wait_recv()
        w_relay(name, t_far, group, 3, 2, side).start()
        w_relay(name, t_far, group, 2, 3, sib).start()

    def w_stage2(name):
        w_relay(name, t_far, 1 - group, 3, 2, side).wait_recv()
        w_relay(name, t_far, 1 - group, 4, 4, sib).start()

    def w_wait_near(name):
        w_local(name).wait()
        w_sib(name, t_sib).wait_recv()

    def w_wait_far(name):
        w_relay(name, t_diag, group, 2, 3, sib).wait_recv()
        w_relay(name, t_diag, 1 - group, 4, 4, sib).wait_recv()

    def w_drain(name):
        w_sib(name, tp).wait_send()
        w_far(name, tp).wait_send()
        w_relay(name, t_far, group, 3, 2, side).wait_send()
        w_relay(name, t_far, group, 2, 3, sib).wait_send()
        w_relay(name, t_far, 1 - group, 4, 4, sib).wait_send()

    def s_copy(link, owner):
        device = (sib, far, diag)[link]
        return remote(loc_hbm, small.at[owner], s_send.at[link], s_recv.at[link], device)

    def e_local(slot, clip):
        return pltpu.make_async_copy(xbuf.at[slot], e_hbm.at[clip], e_loc.at[slot])

    def e_sib(slot, clip):
        return remote(xbuf.at[slot], e_hbm.at[clip], e_send.at[slot], e_recv.at[slot], sib)

    def e_far(slot, clip):
        return remote(xbuf.at[slot], e_hbm.at[clip], e_send.at[SLOTS + slot], e_recv.at[SLOTS + slot], far)

    def e_relay(slot, clip):
        sem = SLOTS + ONLY + slot
        return remote(e_hbm.at[clip], e_hbm.at[clip], e_send.at[sem], e_recv.at[sem], sib)

    barrier = pltpu.get_barrier_semaphore()
    for device in (sib, far, diag, side):
        pl.semaphore_signal(barrier, inc=1, device_id=device, device_id_type=MESH)
    pl.semaphore_wait(barrier, 4)

    small_local = pltpu.make_async_copy(loc_hbm, small.at[tp], s_loc)
    small_local.start()
    for link in range(3):
        s_copy(link, tp).start()
    for item in SEND_ORDER:
        if isinstance(item, str):
            w_start(item)
        else:
            x_copy(item, 1).start()
            x_copy(item, 2).start()
            x_local(item).start()
            x_copy(item, 0).start()

    small_local.wait()
    for link, owner in enumerate((t_sib, t_far, t_diag)):
        s_copy(link, owner).wait_recv()
    bias[0:1, :] = small[0, 1:2, :] + small[1, 1:2, :] + small[2, 1:2, :] + small[3, 1:2, :]
    bias[1:2, :] = small[0, 2:3, :] + small[1, 2:3, :] + small[2, 2:3, :] + small[3, 2:3, :]
    for name in ("q", "k", "v"):
        w_stage1(name)
    for name in ("q", "k", "v"):
        w_stage2(name)
    for name in ("q", "k", "v"):
        w_wait_near(name)
        w_wait_far(name)

    def rep(row):
        return rep_ref[row:row + 1, :]

    def norm_into(dst_store, src_load, gain, shift):
        for first in range(0, FRAMES, LN_ROWS):
            dst_store(first, norm_rows(src_load(first), gain, shift))

    def attention(slot, step):
        x_wait(slot)

        def put_a(first, value):
            abuf[first:first + LN_ROWS, :] = value

        norm_into(put_a, lambda first: xbuf[slot, pl.ds(first, LN_ROWS), :], rep(0), rep(1))
        for col in range(0, WIDTH, 256):
            cols = slice(col, col + 256)
            qbuf[:, cols] = ((dot(abuf[...], wq[cols, :], NT) + bias[0:1, cols]) * ATTN_SCALE).astype(BF16)
            vbuf[:, cols] = (dot(abuf[...], wv[cols, :], NT) + bias[1:2, cols]).astype(BF16)
            ktbuf[cols, :] = (dot(wk[cols, :], abuf[...], NT) * ATTN_SCALE).astype(BF16)

        lane = lax.broadcasted_iota(jnp.int32, (1, 128), 1)
        keep = [(lane < 64).astype(F32).astype(BF16), (lane >= 64).astype(F32).astype(BF16)]

        def pair_body(pair, _):
            cols = pl.ds(pl.multiple_of(pair * 128, 128), 128)
            keys_t = ktbuf[cols, :]
            values = vbuf[:, cols]
            parts = [(first, head) for first in (0, 256) for head in (0, 1)]

            def scores_of(part):
                first, head = part
                return dot(qbuf[first:first + 256, cols] * keep[head], keys_t)

            scores = scores_of(parts[0])
            outs = {}
            for index, part in enumerate(parts):
                ahead = scores_of(parts[index + 1]) if index + 1 < len(parts) else None
                top = jnp.max(scores, axis=-1, keepdims=True)
                weight = jnp.exp(scores - top)
                total = jnp.sum(weight, axis=-1, keepdims=True)
                outs[part] = dot(weight.astype(BF16), values) * (1.0 / total)
                scores = ahead
            for first in (0, 256):
                obuf[first:first + 256, cols] = jnp.where(lane < 64, outs[(first, 0)], outs[(first, 1)]).astype(BF16)
            return 0

        lax.fori_loop(0, 6, pair_body, 0)

        @pl.when(step == 0)
        def _():
            w_stage1("o")
            w_stage2("o")
            w_wait_near("o")
            w_wait_far("o")

        for col in range(0, WIDTH, 256):
            cols = slice(col, col + 256)
            branch = (dot(obuf[...], wo[:, cols]) + rep_ref[6:7, cols]).astype(BF16)
            xbuf[slot, :, cols] = (xbuf[slot, :, cols].astype(F32) + branch.astype(F32)).astype(BF16)

        def put_m(first, value):
            mbuf[slot, pl.ds(first, LN_ROWS), :] = value

        norm_into(put_m, lambda first: xbuf[slot, pl.ds(first, LN_ROWS), :], rep(2), rep(3))

    def hidden_half(slot, which):
        for half in range(2):
            shard = 2 * which + half
            for col in range(0, 768, 256):
                w1_part = w1[pl.ds(pl.multiple_of(shard * 768, 768), 768), col:col + 256]
                inner = dot(mbuf[slot], w1_part) + small[shard, 0:1, col:col + 256]
                gbuf[:, half * 768 + col:half * 768 + col + 256] = (0.5 * inner * (1.0 + lax.erf(inner * SQRT_HALF))).astype(BF16)

    def second_product(which, cols):
        return dot(gbuf[...], w2[pl.ds(pl.multiple_of(which * 1536, 1536), 1536), cols])

    def mlp_near(slot):
        hidden_half(slot, chip)
        for col in range(0, WIDTH, 256):
            cols = slice(col, col + 256)
            acc[slot, :, cols] = second_product(chip, cols)

    def mlp_far(slot):
        hidden_half(slot, other_chip)
        for col in range(0, WIDTH, 256):
            cols = slice(col, col + 256)
            branch = (acc[slot, :, cols] + second_product(other_chip, cols) + rep_ref[7:8, cols]).astype(BF16)
            xbuf[slot, :, cols] = (xbuf[slot, :, cols].astype(F32) + branch.astype(F32)).astype(BF16)

        def put_e(first, value):
            xbuf[slot, pl.ds(first, LN_ROWS), :] = value

        norm_into(put_e, lambda first: xbuf[slot, pl.ds(first, LN_ROWS), :], rep(4), rep(5))

        @pl.when(slot < ONLY)
        def _():
            clip = only_clip(chip, core, slot)
            e_far(slot, clip).start()
            e_local(slot, clip).start()
            e_sib(slot, clip).start()

        @pl.when(slot >= ONLY)
        def _():
            clip = core * SHARED + slot - ONLY
            e_local(slot, clip).start()
            e_sib(slot, clip).start()

    mlp_units = ("w1a", "w1b", "w2a", "w2b")

    def step_body(step, _):
        @pl.when(step < SLOTS)
        def _():
            attention(step, step)

        @pl.when(step == 0)
        def _():
            for name in mlp_units:
                w_wait_near(name)

        @pl.when(step < SLOTS)
        def _():
            mlp_near(step)

        @pl.when(step == LAG)
        def _():
            for name in mlp_units:
                w_stage1(name)
            for name in mlp_units:
                w_stage2(name)
            for name in mlp_units:
                w_wait_far(name)

        @pl.when(step >= LAG)
        def _():
            mlp_far(step - LAG)

        return 0

    lax.fori_loop(0, SLOTS + LAG, step_body, 0)

    for slot in range(ONLY):
        clip = only_clip(other_chip, core, slot)
        e_far(slot, clip).wait_recv()
        e_relay(slot, clip).start()
    for slot in range(SLOTS):
        clip = clip_of(chip, core, slot)
        e_local(slot, clip).wait()
        e_sib(slot, clip).wait_send()
        e_sib(slot, clip_of(chip, other_core, slot)).wait_recv()
    for slot in range(ONLY):
        e_far(slot, only_clip(chip, core, slot)).wait_send()
        e_relay(slot, only_clip(other_chip, core, slot)).wait_send()
        e_relay(slot, only_clip(other_chip, other_core, slot)).wait_recv()
    for slot in range(SLOTS):
        for link in range(3):
            x_copy(slot, link).wait_send()
    for name in units:
        w_drain(name)
    for link in range(3):
        s_copy(link, tp).wait_send()


def encode(x, wq_t, wk_t, wv_t, wo, w1, w2, rep, loc):
    dma = pltpu.SemaphoreType.DMA
    any_spec = pl.BlockSpec(memory_space=pl.ANY)
    return pl.pallas_call(
        encoder_kernel,
        out_shape=jax.ShapeDtypeStruct((CLIPS, FRAMES, WIDTH), BF16),
        in_specs=[any_spec] * 7 + [pl.BlockSpec(memory_space=pltpu.VMEM), any_spec],
        out_specs=any_spec,
        scratch_shapes=[
            pltpu.VMEM((SLOTS, FRAMES, WIDTH), BF16),
            pltpu.VMEM((WIDTH, WIDTH), BF16), pltpu.VMEM((WIDTH, WIDTH), BF16), pltpu.VMEM((WIDTH, WIDTH), BF16),
            pltpu.VMEM((WIDTH, WIDTH), BF16),
            pltpu.VMEM((HIDDEN, WIDTH), BF16), pltpu.VMEM((HIDDEN, WIDTH), BF16),
            pltpu.VMEM((4, 8, WIDTH), F32),
            pltpu.VMEM((FRAMES, WIDTH), BF16), pltpu.VMEM((FRAMES, WIDTH), BF16), pltpu.VMEM((WIDTH, FRAMES), BF16),
            pltpu.VMEM((FRAMES, WIDTH), BF16), pltpu.VMEM((FRAMES, WIDTH), BF16),
            pltpu.VMEM((SLOTS, FRAMES, WIDTH), BF16),
            pltpu.VMEM((FRAMES, 2 * WIDTH), BF16),
            pltpu.VMEM((SLOTS, FRAMES, WIDTH), F32),
            pltpu.VMEM((8, WIDTH), F32),
            dma((SLOTS, 3)), dma((SLOTS, 3)), dma((SLOTS,)),
            dma((8, 5)), dma((8, 5)), dma((8,)),
            dma((3,)), dma((3,)), dma,
            dma((SLOTS + 2 * ONLY,)), dma((SLOTS + 2 * ONLY,)), dma((SLOTS,)),
        ],
        compiler_params=pltpu.CompilerParams(collective_id=0, has_side_effects=True, vmem_limit_bytes=64 * 1024 * 1024 - 128 * 1024),
        name="encoder",
    )(x, wq_t, wk_t, wv_t, wo, w1, w2, rep, loc)


def cache_kernel(tp_ref, e_ref, wk_ref, wv_ref, bias_ref, k_ref, v_ref, enc_ref):
    enc_ref[0] = e_ref[0, pl.ds(pl.multiple_of(tp_ref[0] * LOC_FRAMES, LOC_FRAMES), LOC_FRAMES), :]
    for layer in range(4):
        k_ref[layer, 0] = dot(wk_ref[layer], e_ref[0], NT).astype(BF16)
        shift = jnp.concatenate([bias_ref[layer]] * 4, axis=1)
        v_ref[layer, 0] = (dot(wv_ref[layer], e_ref[0], NT) + shift).astype(BF16)


def caches(tp, e_all, wck_t, wcv_t, bias):
    cache = jax.ShapeDtypeStruct((4, CLIPS, 192, FRAMES), BF16)
    cache_spec = pl.BlockSpec((4, 1, 192, FRAMES), lambda clip, tp_ref: (0, clip, 0, 0))
    whole = lambda clip, tp_ref: (0, 0, 0)
    return pl.pallas_call(
        cache_kernel,
        out_shape=(cache, cache, jax.ShapeDtypeStruct((CLIPS, LOC_FRAMES, WIDTH), BF16)),
        grid_spec=pltpu.PrefetchScalarGridSpec(
            num_scalar_prefetch=1,
            grid=(CLIPS,),
            in_specs=[
                pl.BlockSpec((1, FRAMES, WIDTH), lambda clip, tp_ref: (clip, 0, 0)),
                pl.BlockSpec((4, 192, WIDTH), whole), pl.BlockSpec((4, 192, WIDTH), whole),
                pl.BlockSpec((4, 192, 128), whole),
            ],
            out_specs=(cache_spec, cache_spec, pl.BlockSpec((1, LOC_FRAMES, WIDTH), lambda clip, tp_ref: (clip, 0, 0))),
        ),
        compiler_params=pltpu.CompilerParams(dimension_semantics=("arbitrary",), vmem_limit_bytes=40 * 1024 * 1024),
        name="caches",
    )(tp, e_all, wck_t, wcv_t, bias)


def device_body(hidden_loc, ln1_gain, ln1_bias, w_q, b_q, w_k, w_v, b_v, w_o, b_o, ln2_gain, ln2_bias, w_fc1, b_fc1, w_fc2, b_fc2, post_gain, post_bias, w_ck, w_cv, b_cv):
    tp = lax.axis_index("tp")
    rep = jnp.stack([ln1_gain, ln1_bias, ln2_gain, ln2_bias, post_gain, post_bias, b_o, b_fc2]).astype(F32)
    mine = jnp.arange(WIDTH) // 192 == tp
    placed = lambda vec: jnp.where(mine, jnp.concatenate([vec] * 4), jnp.zeros((), BF16))
    zero = jnp.zeros((WIDTH,), BF16)
    loc = jnp.stack([b_fc1, placed(b_q), placed(b_v), zero, zero, zero, zero, zero]).astype(F32)
    e_all = encode(hidden_loc, w_q.T, w_k.T, w_v.T, w_o, w_fc1, w_fc2, rep, loc)
    bias = jnp.broadcast_to(b_cv.astype(F32)[:, :, None], (4, 192, 128))
    k_t, v_t, enc_loc = caches(tp.astype(jnp.int32).reshape(1), e_all, w_ck.transpose(0, 2, 1), w_cv.transpose(0, 2, 1), bias)
    shape = (4, CLIPS, FRAMES, 3, HEAD_DIM)
    return enc_loc, k_t.transpose(0, 1, 3, 2).reshape(shape), v_t.transpose(0, 1, 3, 2).reshape(shape)


def solution(mesh):
    in_specs = (P("dp", "tp", None), P(), P(), P(None, "tp"), P("tp"), P(None, "tp"), P(None, "tp"), P("tp"), P("tp", None), P(), P(), P(), P(None, "tp"), P("tp"), P("tp", None), P(), P(), P(), P(None, None, "tp"), P(None, None, "tp"), P(None, "tp"))
    out_specs = (P("dp", "tp", None), P(None, "dp", None, "tp", None), P(None, "dp", None, "tp", None))
    return jax.shard_map(device_body, mesh=mesh, in_specs=in_specs, out_specs=out_specs, check_vma=False)
```

```python
import functools

import jax
import jax.numpy as jnp
from jax import lax
from jax.experimental import pallas as pl
from jax.experimental.pallas import tpu as pltpu
from jax.sharding import PartitionSpec as P

HEAD_DIM = 64
ATTN_SCALE = HEAD_DIM ** -0.25
LN_EPS = 1e-5
SQRT_HALF = 0.5 ** 0.5
MESH = pl.DeviceIdType.MESH
BF16, F32 = jnp.bfloat16, jnp.float32

CLIPS, FRAMES, WIDTH, HIDDEN = 16, 512, 768, 3072
LOC_FRAMES = FRAMES // 4
SHARED, ONLY = 4, 2
SLOTS = SHARED + ONLY
LAG = 5
LN_ROWS = 64
SEND_ORDER = ("q", "k", "v", 0, "o", 1, 2, 3, "w1a", "w1b", 4, "w2a", "w2b", 5)
RELAYS = {
    (4, 0): ((1, "w1a"), (1, "w1b")),
    (5, 0): ((2, "w1a"), (2, "w1b")),
    (5, 1): ((1, "w2a"), (1, "w2b")),
    (5, 2): ((2, "w2a"), (2, "w2b")),
}

NT = (((1,), (1,)), ((), ()))
NN = (((1,), (0,)), ((), ()))
TN = (((0,), (0,)), ((), ()))


def dot(lhs, rhs, dims=NN):
    return lax.dot_general(lhs, rhs, dims, preferred_element_type=F32)


def norm_rows(values, gain, bias):
    centered = values.astype(F32)
    centered = centered - jnp.mean(centered, axis=-1, keepdims=True)
    row_var = jnp.mean(centered * centered, axis=-1, keepdims=True)
    return (centered * lax.rsqrt(row_var + LN_EPS) * gain + bias).astype(BF16)


def only_clip(chip, core, slot):
    return 2 * SHARED + (2 * chip + core) * ONLY + slot


def clip_of(chip, core, slot):
    return only_clip(chip, core, slot) if slot < ONLY else core * SHARED + slot - ONLY


def rows_of(ref, start, count):
    return ref.at[pl.ds(pl.multiple_of(start, 16), count), :]


def encoder_kernel(x_hbm, wq_hbm, wk_hbm, wv_hbm, wo_hbm, w1_hbm, w2_hbm,
                   g1_ref, s1_ref, g2_ref, s2_ref, g3_ref, s3_ref, bo_ref, b2_ref, b1_ref, bq_ref, bv_ref, e_hbm,
                   rep_ref, loc, xbuf, wq, wk, wv, wo, w1, w2, small, abuf, qbuf, ktbuf, vbuf, obuf, mbuf, gbuf, acc, bias,
                   x_send, x_recv, x_loc, w_send, w_recv, w_loc, s_send, s_recv, e_send, e_recv, e_loc):
    group, tp = lax.axis_index("dp"), lax.axis_index("tp")
    chip, core = tp // 2, tp % 2
    other_chip, other_core = 1 - chip, 1 - core
    t_sib = 2 * chip + other_core
    t_far = 2 * other_chip + core
    t_diag = 2 * other_chip + other_core
    sib = {"dp": group, "tp": t_sib}
    far = {"dp": group, "tp": t_far}
    diag = {"dp": group, "tp": t_diag}
    side = {"dp": 1 - group, "tp": tp}

    def remote(src, dst, send, recv, device):
        return pltpu.make_async_remote_copy(src_ref=src, dst_ref=dst, send_sem=send, recv_sem=recv, device_id=device, device_id_type=MESH)

    def frames(slot, owner):
        return xbuf.at[slot, pl.ds(pl.multiple_of(owner * LOC_FRAMES, LOC_FRAMES), LOC_FRAMES), :]

    def x_copy(slot, link):
        device, there_chip, there_core = ((sib, chip, other_core), (far, other_chip, core), (diag, other_chip, other_core))[link]
        return remote(x_hbm.at[clip_of(there_chip, there_core, slot)], frames(slot, tp), x_send.at[slot, link], x_recv.at[slot, link], device)

    def x_local(slot):
        return pltpu.make_async_copy(x_hbm.at[clip_of(chip, core, slot)], frames(slot, tp), x_loc.at[slot])

    def x_wait(slot):
        pltpu.make_async_copy(x_hbm.at[0], frames(slot, tp), x_loc.at[slot]).wait()
        for link, owner in enumerate((t_sib, t_far, t_diag)):
            remote(x_hbm.at[0], frames(slot, owner), x_send.at[slot, link], x_recv.at[slot, link], sib).wait_recv()

    units = {
        "q": (0, wq_hbm, wq, 192, 0, 192), "k": (1, wk_hbm, wk, 192, 0, 192), "v": (2, wv_hbm, wv, 192, 0, 192),
        "o": (3, wo_hbm, wo, 192, 0, 192),
        "w1a": (4, w1_hbm, w1, 768, 0, 384), "w1b": (5, w1_hbm, w1, 768, 384, 384),
        "w2a": (6, w2_hbm, w2, 768, 0, 384), "w2b": (7, w2_hbm, w2, 768, 384, 384),
    }

    def w_local(name):
        idx, src, dst, shard, first, count = units[name]
        return pltpu.make_async_copy(src.at[pl.ds(first, count), :], rows_of(dst, tp * shard + first, count), w_loc.at[idx])

    def w_sib(name, owner):
        idx, src, dst, shard, first, count = units[name]
        return remote(src.at[pl.ds(first, count), :], rows_of(dst, owner * shard + first, count), w_send.at[idx, 0], w_recv.at[idx, 0], sib)

    def w_far(name, owner):
        idx, src, dst, shard, first, count = units[name]
        half = count // 2
        return remote(rows_of(src, first + group * half, half), rows_of(dst, owner * shard + first + group * half, half),
                      w_send.at[idx, 1], w_recv.at[idx, 1], far)

    def w_relay(name, owner, part, sem, recv, device):
        idx, src, dst, shard, first, count = units[name]
        half = count // 2
        piece = rows_of(dst, owner * shard + first + part * half, half)
        return remote(piece, piece, w_send.at[idx, sem], w_recv.at[idx, recv], device)

    def w_start(name):
        w_far(name, tp).start()
        w_local(name).start()
        w_sib(name, tp).start()

    def w_stage1(name):
        w_far(name, t_far).wait_recv()
        w_relay(name, t_far, group, 3, 2, side).start()
        w_relay(name, t_far, group, 2, 3, sib).start()

    def w_stage2(name):
        w_relay(name, t_far, 1 - group, 3, 2, side).wait_recv()
        w_relay(name, t_far, 1 - group, 4, 4, sib).start()

    def w_wait_near(name):
        w_local(name).wait()
        w_sib(name, t_sib).wait_recv()

    def w_wait_far(name):
        w_relay(name, t_diag, group, 2, 3, sib).wait_recv()
        w_relay(name, t_diag, 1 - group, 4, 4, sib).wait_recv()

    def w_drain(name):
        w_sib(name, tp).wait_send()
        w_far(name, tp).wait_send()
        w_relay(name, t_far, group, 3, 2, side).wait_send()
        w_relay(name, t_far, group, 2, 3, sib).wait_send()
        w_relay(name, t_far, 1 - group, 4, 4, sib).wait_send()

    def s_copy(link, owner):
        device = (sib, far, diag)[link]
        return remote(loc, small.at[owner], s_send.at[link], s_recv.at[link], device)

    def e_local(slot, clip):
        return pltpu.make_async_copy(xbuf.at[slot], e_hbm.at[clip], e_loc.at[slot])

    def e_sib(slot, clip):
        return remote(xbuf.at[slot], e_hbm.at[clip], e_send.at[slot], e_recv.at[slot], sib)

    def e_far(slot, clip):
        return remote(xbuf.at[slot], e_hbm.at[clip], e_send.at[SLOTS + slot], e_recv.at[SLOTS + slot], far)

    def e_relay(slot, clip):
        sem = SLOTS + ONLY + slot
        return remote(e_hbm.at[clip], e_hbm.at[clip], e_send.at[sem], e_recv.at[sem], sib)

    for row, ref in enumerate((g1_ref, s1_ref, g2_ref, s2_ref, g3_ref, s3_ref, bo_ref, b2_ref)):
        rep_ref[row:row + 1, :] = ref[...].astype(F32).reshape(1, WIDTH)
    place = lax.broadcasted_iota(jnp.int32, (192, WIDTH), 0) + tp * 192 == lax.broadcasted_iota(jnp.int32, (192, WIDTH), 1)
    place = place.astype(F32).astype(BF16)
    loc[0:1, :] = b1_ref[...].astype(F32).reshape(1, WIDTH)
    for row, ref in ((1, bq_ref), (2, bv_ref)):
        vector = jnp.broadcast_to(ref[...].astype(F32).reshape(1, 192), (16, 192)).astype(BF16)
        loc[row:row + 1, :] = dot(vector, place)[0:1, :]
    loc[3:8, :] = jnp.zeros((5, WIDTH), F32)
    small[tp] = loc[...]

    barrier = pltpu.get_barrier_semaphore()
    for device in (sib, far, diag, side):
        pl.semaphore_signal(barrier, inc=1, device_id=device, device_id_type=MESH)
    pl.semaphore_wait(barrier, 4)

    for item in SEND_ORDER:
        if item == 0:
            for link in range(3):
                s_copy(link, tp).start()
        if isinstance(item, str):
            w_start(item)
        else:
            x_copy(item, 1).start()
            x_copy(item, 2).start()
            x_local(item).start()
            x_copy(item, 0).start()

    for link, owner in enumerate((t_sib, t_far, t_diag)):
        s_copy(link, owner).wait_recv()
    bias[0:1, :] = small[0, 1:2, :] + small[1, 1:2, :] + small[2, 1:2, :] + small[3, 1:2, :]
    bias[1:2, :] = small[0, 2:3, :] + small[1, 2:3, :] + small[2, 2:3, :] + small[3, 2:3, :]
    for name in ("q", "k", "v"):
        w_stage1(name)
    for name in ("q", "k", "v"):
        w_stage2(name)
    for name in ("q", "k", "v"):
        w_wait_near(name)
        w_wait_far(name)

    def rep(row):
        return rep_ref[row:row + 1, :]

    def norm_into(dst_store, src_load, gain, shift):
        for first in range(0, FRAMES, LN_ROWS):
            dst_store(first, norm_rows(src_load(first), gain, shift))

    def attention(slot, step):
        x_wait(slot)

        def put_a(first, value):
            abuf[first:first + LN_ROWS, :] = value

        norm_into(put_a, lambda first: xbuf[slot, pl.ds(first, LN_ROWS), :], rep(0), rep(1))
        for col in range(0, WIDTH, 256):
            cols = slice(col, col + 256)
            qbuf[:, cols] = ((dot(abuf[...], wq[cols, :], NT) + bias[0:1, cols]) * ATTN_SCALE).astype(BF16)
            vbuf[:, cols] = (dot(abuf[...], wv[cols, :], NT) + bias[1:2, cols]).astype(BF16)
            ktbuf[cols, :] = (dot(wk[cols, :], abuf[...], NT) * ATTN_SCALE).astype(BF16)

        lane = lax.broadcasted_iota(jnp.int32, (1, 128), 1)
        keep = [(lane < 64).astype(F32).astype(BF16), (lane >= 64).astype(F32).astype(BF16)]

        def pair_body(pair, _):
            cols = pl.ds(pl.multiple_of(pair * 128, 128), 128)
            keys_t = ktbuf[cols, :]
            values = vbuf[:, cols]
            parts = [(first, head) for first in (0, 256) for head in (0, 1)]

            def scores_of(part):
                first, head = part
                return dot(qbuf[first:first + 256, cols] * keep[head], keys_t)

            scores = scores_of(parts[0])
            outs = {}
            for index, part in enumerate(parts):
                ahead = scores_of(parts[index + 1]) if index + 1 < len(parts) else None
                top = jnp.max(scores, axis=-1, keepdims=True)
                weight = jnp.exp(scores - top)
                total = jnp.sum(weight, axis=-1, keepdims=True)
                outs[part] = dot(weight.astype(BF16), values) * (1.0 / total)
                scores = ahead
            for first in (0, 256):
                obuf[first:first + 256, cols] = jnp.where(lane < 64, outs[(first, 0)], outs[(first, 1)]).astype(BF16)
            return 0

        lax.fori_loop(0, 6, pair_body, 0)

        @pl.when(step == 0)
        def _():
            w_stage1("o")
            w_stage2("o")
            w_wait_near("o")
            w_wait_far("o")

        for col in range(0, WIDTH, 256):
            cols = slice(col, col + 256)
            branch = (dot(obuf[...], wo[:, cols]) + rep_ref[6:7, cols]).astype(BF16)
            xbuf[slot, :, cols] = (xbuf[slot, :, cols].astype(F32) + branch.astype(F32)).astype(BF16)

        def put_m(first, value):
            mbuf[slot, pl.ds(first, LN_ROWS), :] = value

        norm_into(put_m, lambda first: xbuf[slot, pl.ds(first, LN_ROWS), :], rep(2), rep(3))

    def hidden_half(slot, which):
        for half in range(2):
            shard = 2 * which + half
            for col in range(0, 768, 256):
                w1_part = w1[pl.ds(pl.multiple_of(shard * 768, 768), 768), col:col + 256]
                inner = dot(mbuf[slot], w1_part) + small[shard, 0:1, col:col + 256]
                gbuf[:, half * 768 + col:half * 768 + col + 256] = (0.5 * inner * (1.0 + lax.erf(inner * SQRT_HALF))).astype(BF16)

    def second_product(which, cols):
        return dot(gbuf[...], w2[pl.ds(pl.multiple_of(which * 1536, 1536), 1536), cols])

    def mlp_near(slot):
        hidden_half(slot, chip)
        for col in range(0, WIDTH, 256):
            cols = slice(col, col + 256)
            acc[slot, :, cols] = second_product(chip, cols)

    def mlp_far(slot):
        hidden_half(slot, other_chip)
        for col in range(0, WIDTH, 256):
            cols = slice(col, col + 256)
            branch = (acc[slot, :, cols] + second_product(other_chip, cols) + rep_ref[7:8, cols]).astype(BF16)
            xbuf[slot, :, cols] = (xbuf[slot, :, cols].astype(F32) + branch.astype(F32)).astype(BF16)

        def put_e(first, value):
            xbuf[slot, pl.ds(first, LN_ROWS), :] = value

        norm_into(put_e, lambda first: xbuf[slot, pl.ds(first, LN_ROWS), :], rep(4), rep(5))

        @pl.when(slot < ONLY)
        def _():
            clip = only_clip(chip, core, slot)
            e_far(slot, clip).start()
            e_local(slot, clip).start()
            e_sib(slot, clip).start()

        @pl.when(slot >= ONLY)
        def _():
            clip = core * SHARED + slot - ONLY
            e_local(slot, clip).start()
            e_sib(slot, clip).start()

    mlp_units = ("w1a", "w1b", "w2a", "w2b")

    def relays(step, place):
        for (when, where), todo in RELAYS.items():
            if where == place:
                @pl.when(step == when)
                def _():
                    for stage, name in todo:
                        (w_stage1 if stage == 1 else w_stage2)(name)

    def step_body(step, _):
        relays(step, 0)

        @pl.when(step < SLOTS)
        def _():
            attention(step, step)

        relays(step, 1)

        @pl.when(step == 0)
        def _():
            for name in mlp_units:
                w_wait_near(name)

        @pl.when(step < SLOTS)
        def _():
            mlp_near(step)

        relays(step, 2)

        @pl.when(step == LAG)
        def _():
            for name in mlp_units:
                w_wait_far(name)

        @pl.when(step >= LAG)
        def _():
            mlp_far(step - LAG)

        return 0

    lax.fori_loop(0, SLOTS + LAG, step_body, 0)

    for slot in range(ONLY):
        clip = only_clip(other_chip, core, slot)
        e_far(slot, clip).wait_recv()
        e_relay(slot, clip).start()
    for slot in range(SLOTS):
        clip = clip_of(chip, core, slot)
        e_local(slot, clip).wait()
        e_sib(slot, clip).wait_send()
        e_sib(slot, clip_of(chip, other_core, slot)).wait_recv()
    for slot in range(ONLY):
        e_far(slot, only_clip(chip, core, slot)).wait_send()
        e_relay(slot, only_clip(other_chip, core, slot)).wait_send()
        e_relay(slot, only_clip(other_chip, other_core, slot)).wait_recv()
    for slot in range(SLOTS):
        for link in range(3):
            x_copy(slot, link).wait_send()
    for name in units:
        w_drain(name)
    for link in range(3):
        s_copy(link, tp).wait_send()


def encode(x, weights, vectors):
    dma = pltpu.SemaphoreType.DMA
    any_spec = pl.BlockSpec(memory_space=pl.ANY)
    return pl.pallas_call(
        encoder_kernel,
        out_shape=jax.ShapeDtypeStruct((CLIPS, FRAMES, WIDTH), BF16),
        in_specs=[any_spec] * 7 + [pl.BlockSpec(memory_space=pltpu.VMEM)] * 11,
        out_specs=any_spec,
        scratch_shapes=[
            pltpu.VMEM((8, WIDTH), F32), pltpu.VMEM((8, WIDTH), F32),
            pltpu.VMEM((SLOTS, FRAMES, WIDTH), BF16),
            pltpu.VMEM((WIDTH, WIDTH), BF16), pltpu.VMEM((WIDTH, WIDTH), BF16), pltpu.VMEM((WIDTH, WIDTH), BF16),
            pltpu.VMEM((WIDTH, WIDTH), BF16),
            pltpu.VMEM((HIDDEN, WIDTH), BF16), pltpu.VMEM((HIDDEN, WIDTH), BF16),
            pltpu.VMEM((4, 8, WIDTH), F32),
            pltpu.VMEM((FRAMES, WIDTH), BF16), pltpu.VMEM((FRAMES, WIDTH), BF16), pltpu.VMEM((WIDTH, FRAMES), BF16),
            pltpu.VMEM((FRAMES, WIDTH), BF16), pltpu.VMEM((FRAMES, WIDTH), BF16),
            pltpu.VMEM((SLOTS, FRAMES, WIDTH), BF16),
            pltpu.VMEM((FRAMES, 2 * WIDTH), BF16),
            pltpu.VMEM((SLOTS, FRAMES, WIDTH), F32),
            pltpu.VMEM((8, WIDTH), F32),
            dma((SLOTS, 3)), dma((SLOTS, 3)), dma((SLOTS,)),
            dma((8, 5)), dma((8, 5)), dma((8,)),
            dma((3,)), dma((3,)),
            dma((SLOTS + 2 * ONLY,)), dma((SLOTS + 2 * ONLY,)), dma((SLOTS,)),
        ],
        compiler_params=pltpu.CompilerParams(collective_id=0, has_side_effects=True, vmem_limit_bytes=64 * 1024 * 1024 - 128 * 1024),
        name="encoder",
    )(x, *weights, *vectors)


def cache_kernel(tp_ref, e_ref, wk_ref, wv_ref, bias_ref, k_ref, v_ref, enc_ref, shift):
    @pl.when(pl.program_id(0) == 0)
    def _():
        rows = jnp.concatenate([bias_ref[...].astype(F32), jnp.zeros((4, 192), F32)], axis=0)
        for layer in range(4):
            pick = (lax.broadcasted_iota(jnp.int32, (8, 128), 0) == layer).astype(F32)
            shift[layer * 192:layer * 192 + 192, :] = dot(rows, pick, TN)

    enc_ref[0] = e_ref[0, pl.ds(pl.multiple_of(tp_ref[0] * LOC_FRAMES, LOC_FRAMES), LOC_FRAMES), :]
    for first in range(0, FRAMES, 256):
        frames = slice(first, first + 256)
        keys = dot(wk_ref[...].reshape(WIDTH, WIDTH), e_ref[0, frames, :], NT).astype(BF16)
        values = (dot(wv_ref[...].reshape(WIDTH, WIDTH), e_ref[0, frames, :], NT) + jnp.concatenate([shift[...]] * 2, axis=1)).astype(BF16)
        for layer in range(4):
            k_ref[layer, 0, :, frames] = keys[layer * 192:layer * 192 + 192, :]
            v_ref[layer, 0, :, frames] = values[layer * 192:layer * 192 + 192, :]


def caches(tp, e_all, wck_t, wcv_t, bias):
    cache = jax.ShapeDtypeStruct((4, CLIPS, 192, FRAMES), BF16)
    cache_spec = pl.BlockSpec((4, 1, 192, FRAMES), lambda clip, tp_ref: (0, clip, 0, 0))
    whole = lambda clip, tp_ref: (0, 0, 0)
    return pl.pallas_call(
        cache_kernel,
        out_shape=(cache, cache, jax.ShapeDtypeStruct((CLIPS, LOC_FRAMES, WIDTH), BF16)),
        grid_spec=pltpu.PrefetchScalarGridSpec(
            num_scalar_prefetch=1,
            grid=(CLIPS,),
            in_specs=[
                pl.BlockSpec((1, FRAMES, WIDTH), lambda clip, tp_ref: (clip, 0, 0)),
                pl.BlockSpec((4, 192, WIDTH), whole), pl.BlockSpec((4, 192, WIDTH), whole),
                pl.BlockSpec((4, 192), lambda clip, tp_ref: (0, 0)),
            ],
            out_specs=(cache_spec, cache_spec, pl.BlockSpec((1, LOC_FRAMES, WIDTH), lambda clip, tp_ref: (clip, 0, 0))),
            scratch_shapes=[pltpu.VMEM((WIDTH, 128), F32)],
        ),
        compiler_params=pltpu.CompilerParams(dimension_semantics=("arbitrary",), vmem_limit_bytes=64 * 1024 * 1024 - 128 * 1024),
        name="caches",
    )(tp, e_all, wck_t, wcv_t, bias)


def device_body(hidden_loc, ln1_gain, ln1_bias, w_q, b_q, w_k, w_v, b_v, w_o, b_o, ln2_gain, ln2_bias, w_fc1, b_fc1, w_fc2, b_fc2, post_gain, post_bias, w_ck, w_cv, b_cv):
    weights = (w_q.T, w_k.T, w_v.T, w_o, w_fc1, w_fc2)
    vectors = (ln1_gain, ln1_bias, ln2_gain, ln2_bias, post_gain, post_bias, b_o, b_fc2, b_fc1, b_q, b_v)
    e_all = encode(hidden_loc, weights, vectors)
    tp = lax.axis_index("tp").astype(jnp.int32).reshape(1)
    k_t, v_t, enc_loc = caches(tp, e_all, w_ck.transpose(0, 2, 1), w_cv.transpose(0, 2, 1), b_cv)
    shape = (4, CLIPS, FRAMES, 3, HEAD_DIM)
    return enc_loc, k_t.transpose(0, 1, 3, 2).reshape(shape), v_t.transpose(0, 1, 3, 2).reshape(shape)


def solution(mesh):
    in_specs = (P("dp", "tp", None), P(), P(), P(None, "tp"), P("tp"), P(None, "tp"), P(None, "tp"), P("tp"), P("tp", None), P(), P(), P(), P(None, "tp"), P("tp"), P("tp", None), P(), P(), P(), P(None, None, "tp"), P(None, None, "tp"), P(None, "tp"))
    out_specs = (P("dp", "tp", None), P(None, "dp", None, "tp", None), P(None, "dp", None, "tp", None))
    return jax.shard_map(device_body, mesh=mesh, in_specs=in_specs, out_specs=out_specs, check_vma=False)
```

```python
import functools

import jax
import jax.numpy as jnp
from jax import lax
from jax.experimental import pallas as pl
from jax.experimental.pallas import tpu as pltpu
from jax.sharding import PartitionSpec as P

HEAD_DIM = 64
ATTN_SCALE = HEAD_DIM ** -0.25
LN_EPS = 1e-5
SQRT_HALF = 0.5 ** 0.5
MESH = pl.DeviceIdType.MESH
BF16, F32 = jnp.bfloat16, jnp.float32

CLIPS, FRAMES, WIDTH, HIDDEN = 16, 512, 768, 3072
LOC_FRAMES, LOC_COLS = FRAMES // 4, WIDTH // 4
WIDE = (slice(0, 512), slice(512, 768))
SHARED, ONLY = 4, 2
SLOTS = SHARED + ONLY
LAG = 3
LN_ROWS = 64
SEND_ORDER = ("q", "k", "v", 0, "o", 1, 2, "w1a", "w1b", 3, "w2a", "w2b", 4, 5)
RELAYS = {
    (3, 0): ((1, "w1a"), (1, "w1b")),
    (3, 1): ((2, "w1a"), (2, "w1b"), (1, "w2a"), (1, "w2b")),
    (3, 2): ((2, "w2a"), (2, "w2b")),
}

NT = (((1,), (1,)), ((), ()))
NN = (((1,), (0,)), ((), ()))
TN = (((0,), (0,)), ((), ()))


def dot(lhs, rhs, dims=NN):
    return lax.dot_general(lhs, rhs, dims, preferred_element_type=F32)


def norm_rows(values, gain, bias):
    centered = values.astype(F32)
    centered = centered - jnp.mean(centered, axis=-1, keepdims=True)
    row_var = jnp.mean(centered * centered, axis=-1, keepdims=True)
    return (centered * lax.rsqrt(row_var + LN_EPS) * gain + bias).astype(BF16)


def only_clip(chip, core, slot):
    return 2 * SHARED + (2 * chip + core) * ONLY + slot


def clip_of(chip, core, slot):
    return only_clip(chip, core, slot) if slot < ONLY else core * SHARED + slot - ONLY


def rows_of(ref, start, count):
    return ref.at[pl.ds(pl.multiple_of(start, 16), count), :]


def encoder_kernel(x_hbm, wq_hbm, wk_hbm, wv_hbm, wo_hbm, w1_hbm, w2_hbm,
                   g1_ref, s1_ref, g2_ref, s2_ref, g3_ref, s3_ref, bo_ref, b2_ref, b1_ref, bq_ref, bv_ref, e_hbm,
                   rep_ref, loc, b1_row, xbuf, wqv, wk, wo, w1, w2, small, abuf, qvbuf, ktbuf, obuf, mbuf, gbuf, acc, bias,
                   x_send, x_recv, x_loc, w_send, w_recv, w_loc, s_send, s_recv, e_send, e_recv, e_loc):
    group, tp = lax.axis_index("dp"), lax.axis_index("tp")
    chip, core = tp // 2, tp % 2
    other_chip, other_core = 1 - chip, 1 - core
    t_sib = 2 * chip + other_core
    t_far = 2 * other_chip + core
    t_diag = 2 * other_chip + other_core
    sib = {"dp": group, "tp": t_sib}
    far = {"dp": group, "tp": t_far}
    diag = {"dp": group, "tp": t_diag}
    side = {"dp": 1 - group, "tp": tp}

    def remote(src, dst, send, recv, device):
        return pltpu.make_async_remote_copy(src_ref=src, dst_ref=dst, send_sem=send, recv_sem=recv, device_id=device, device_id_type=MESH)

    def frames(slot, owner):
        return xbuf.at[slot, pl.ds(pl.multiple_of(owner * LOC_FRAMES, LOC_FRAMES), LOC_FRAMES), :]

    def x_copy(slot, link):
        device, there_chip, there_core = ((sib, chip, other_core), (far, other_chip, core), (diag, other_chip, other_core))[link]
        return remote(x_hbm.at[clip_of(there_chip, there_core, slot)], frames(slot, tp), x_send.at[slot, link], x_recv.at[slot, link], device)

    def x_local(slot):
        return pltpu.make_async_copy(x_hbm.at[clip_of(chip, core, slot)], frames(slot, tp), x_loc.at[slot])

    def x_wait(slot):
        pltpu.make_async_copy(x_hbm.at[0], frames(slot, tp), x_loc.at[slot]).wait()
        for link, owner in enumerate((t_sib, t_far, t_diag)):
            remote(x_hbm.at[0], frames(slot, owner), x_send.at[slot, link], x_recv.at[slot, link], sib).wait_recv()

    def at_rows(dst, base):
        shard = LOC_COLS if dst is not w2 else WIDTH
        return lambda owner, first, count: rows_of(dst, base + owner * shard + first, count)

    def at_columns(owner, first, count):
        return w1.at[pl.ds(pl.multiple_of(first, 16), count), pl.ds(pl.multiple_of(owner * WIDTH, WIDTH), WIDTH)]

    units = {
        "q": (0, wq_hbm, at_rows(wqv, 0), 0, 192), "k": (1, wk_hbm, at_rows(wk, 0), 0, 192),
        "v": (2, wv_hbm, at_rows(wqv, WIDTH), 0, 192), "o": (3, wo_hbm, at_rows(wo, 0), 0, 192),
        "w1a": (4, w1_hbm, at_columns, 0, 384), "w1b": (5, w1_hbm, at_columns, 384, 384),
        "w2a": (6, w2_hbm, at_rows(w2, 0), 0, 384), "w2b": (7, w2_hbm, at_rows(w2, 0), 384, 384),
    }

    def w_local(name):
        idx, src, place, first, count = units[name]
        return pltpu.make_async_copy(src.at[pl.ds(first, count), :], place(tp, first, count), w_loc.at[idx])

    def w_sib(name, owner):
        idx, src, place, first, count = units[name]
        return remote(src.at[pl.ds(first, count), :], place(owner, first, count), w_send.at[idx, 0], w_recv.at[idx, 0], sib)

    def w_far(name, owner):
        idx, src, place, first, count = units[name]
        half = count // 2
        return remote(rows_of(src, first + group * half, half), place(owner, first + group * half, half),
                      w_send.at[idx, 1], w_recv.at[idx, 1], far)

    def w_relay(name, owner, part, sem, recv, device):
        idx, src, place, first, count = units[name]
        half = count // 2
        piece = place(owner, first + part * half, half)
        return remote(piece, piece, w_send.at[idx, sem], w_recv.at[idx, recv], device)

    def w_start(name):
        w_far(name, tp).start()
        w_local(name).start()
        w_sib(name, tp).start()

    def w_stage1(name):
        w_far(name, t_far).wait_recv()
        w_relay(name, t_far, group, 3, 2, side).start()
        w_relay(name, t_far, group, 2, 3, sib).start()

    def w_stage2(name):
        w_relay(name, t_far, 1 - group, 3, 2, side).wait_recv()
        w_relay(name, t_far, 1 - group, 4, 4, sib).start()

    def w_wait_near(name):
        w_local(name).wait()
        w_sib(name, t_sib).wait_recv()

    def w_wait_far(name):
        w_relay(name, t_diag, group, 2, 3, sib).wait_recv()
        w_relay(name, t_diag, 1 - group, 4, 4, sib).wait_recv()

    def w_drain(name):
        w_sib(name, tp).wait_send()
        w_far(name, tp).wait_send()
        w_relay(name, t_far, group, 3, 2, side).wait_send()
        w_relay(name, t_far, group, 2, 3, sib).wait_send()
        w_relay(name, t_far, 1 - group, 4, 4, sib).wait_send()

    def s_copy(link, owner):
        device = (sib, far, diag)[link]
        return remote(loc, small.at[owner], s_send.at[link], s_recv.at[link], device)

    def e_local(slot, clip):
        return pltpu.make_async_copy(xbuf.at[slot], e_hbm.at[clip], e_loc.at[slot])

    def e_sib(slot, clip):
        return remote(xbuf.at[slot], e_hbm.at[clip], e_send.at[slot], e_recv.at[slot], sib)

    def e_far(slot, clip):
        return remote(xbuf.at[slot], e_hbm.at[clip], e_send.at[SLOTS + slot], e_recv.at[SLOTS + slot], far)

    def e_relay(slot, clip):
        sem = SLOTS + ONLY + slot
        return remote(e_hbm.at[clip], e_hbm.at[clip], e_send.at[sem], e_recv.at[sem], sib)

    for row, ref in enumerate((g1_ref, s1_ref, g2_ref, s2_ref, g3_ref, s3_ref, bo_ref, b2_ref)):
        rep_ref[row:row + 1, :] = ref[...].astype(F32).reshape(1, WIDTH)
    place = lax.broadcasted_iota(jnp.int32, (192, WIDTH), 0) + tp * 192 == lax.broadcasted_iota(jnp.int32, (192, WIDTH), 1)
    place = place.astype(F32).astype(BF16)
    loc[0:1, :] = b1_ref[...].astype(F32).reshape(1, WIDTH)
    for row, ref in ((1, bq_ref), (2, bv_ref)):
        vector = jnp.broadcast_to(ref[...].astype(F32).reshape(1, 192), (16, 192)).astype(BF16)
        loc[row:row + 1, :] = dot(vector, place)[0:1, :]
    loc[3:8, :] = jnp.zeros((5, WIDTH), F32)
    small[tp] = loc[...]

    barrier = pltpu.get_barrier_semaphore()
    for device in (sib, far, diag, side):
        pl.semaphore_signal(barrier, inc=1, device_id=device, device_id_type=MESH)
    pl.semaphore_wait(barrier, 4)

    for item in SEND_ORDER:
        if item == 0:
            for link in range(3):
                s_copy(link, tp).start()
        if isinstance(item, str):
            w_start(item)
        else:
            x_copy(item, 1).start()
            x_copy(item, 2).start()
            x_local(item).start()
            x_copy(item, 0).start()

    for link, owner in enumerate((t_sib, t_far, t_diag)):
        s_copy(link, owner).wait_recv()
    bias[0:1, 0:WIDTH] = small[0, 1:2, :] + small[1, 1:2, :] + small[2, 1:2, :] + small[3, 1:2, :]
    bias[0:1, WIDTH:2 * WIDTH] = small[0, 2:3, :] + small[1, 2:3, :] + small[2, 2:3, :] + small[3, 2:3, :]
    for owner in range(4):
        b1_row[0:1, owner * WIDTH:owner * WIDTH + WIDTH] = small[owner, 0:1, :]
    for name in ("q", "k", "v"):
        w_stage1(name)
    for name in ("q", "k", "v"):
        w_stage2(name)
    for name in ("q", "k", "v"):
        w_wait_near(name)
        w_wait_far(name)

    def rep(row):
        return rep_ref[row:row + 1, :]

    def norm_into(dst_store, src_load, gain, shift):
        for first in range(0, FRAMES, LN_ROWS):
            dst_store(first, norm_rows(src_load(first), gain, shift))

    def attention(slot, step):
        x_wait(slot)

        def put_a(first, value):
            abuf[first:first + LN_ROWS, :] = value

        norm_into(put_a, lambda first: xbuf[slot, pl.ds(first, LN_ROWS), :], rep(0), rep(1))
        scale = jnp.where(lax.broadcasted_iota(jnp.int32, (1, 2 * WIDTH), 1) < WIDTH, ATTN_SCALE, 1.0)
        ktbuf[...] = (dot(wk[...], abuf[...], NT) * ATTN_SCALE).astype(BF16)
        for col in range(0, 2 * WIDTH, 512):
            cols = slice(col, col + 512)
            qvbuf[:, cols] = ((dot(abuf[...], wqv[cols, :], NT) + bias[0:1, cols]) * scale[:, cols]).astype(BF16)

        lane = lax.broadcasted_iota(jnp.int32, (1, 128), 1)
        keep = [(lane < 64).astype(F32).astype(BF16), (lane >= 64).astype(F32).astype(BF16)]

        def pair_body(pair, _):
            cols = pl.ds(pl.multiple_of(pair * 128, 128), 128)
            keys_t = ktbuf[cols, :]
            values = qvbuf[:, pl.ds(pl.multiple_of(WIDTH + pair * 128, 128), 128)]

            def scores_of(head):
                return dot(qvbuf[:, cols] * keep[head], keys_t)

            scores = scores_of(0)
            outs = []
            for head in range(2):
                ahead = scores_of(1) if head == 0 else None
                top = jnp.max(scores, axis=-1, keepdims=True)
                weight = jnp.exp(scores - top)
                total = jnp.sum(weight, axis=-1, keepdims=True)
                outs.append(dot(weight.astype(BF16), values) * (1.0 / total))
                scores = ahead
            obuf[:, cols] = jnp.where(lane < 64, outs[0], outs[1]).astype(BF16)
            return 0

        lax.fori_loop(0, 6, pair_body, 0)

        @pl.when(step == 0)
        def _():
            w_stage1("o")
            w_stage2("o")
            w_wait_near("o")
            w_wait_far("o")

        for cols in WIDE:
            branch = (dot(obuf[...], wo[:, cols]) + rep_ref[6:7, cols]).astype(BF16)
            xbuf[slot, :, cols] = (xbuf[slot, :, cols].astype(F32) + branch.astype(F32)).astype(BF16)

        def put_m(first, value):
            mbuf[slot, pl.ds(first, LN_ROWS), :] = value

        norm_into(put_m, lambda first: xbuf[slot, pl.ds(first, LN_ROWS), :], rep(2), rep(3))

    def hidden_half(slot, which):
        def product(col):
            return dot(mbuf[slot], w1[:, pl.ds(pl.multiple_of(which * 1536 + col, 512), 512)])

        ahead = product(0)
        for col in range(0, 1536, 512):
            inner = ahead + b1_row[0:1, pl.ds(pl.multiple_of(which * 1536 + col, 512), 512)]
            if col + 512 < 1536:
                ahead = product(col + 512)
            gbuf[:, col:col + 512] = (0.5 * inner * (1.0 + lax.erf(inner * SQRT_HALF))).astype(BF16)

    def second_product(which, cols):
        return dot(gbuf[...], w2[pl.ds(pl.multiple_of(which * 1536, 1536), 1536), cols])

    def mlp_near(slot):
        hidden_half(slot, chip)
        for cols in WIDE:
            acc[slot, :, cols] = second_product(chip, cols)

    def mlp_far(slot):
        hidden_half(slot, other_chip)
        for cols in WIDE:
            branch = (acc[slot, :, cols] + second_product(other_chip, cols) + rep_ref[7:8, cols]).astype(BF16)
            xbuf[slot, :, cols] = (xbuf[slot, :, cols].astype(F32) + branch.astype(F32)).astype(BF16)

        def put_e(first, value):
            xbuf[slot, pl.ds(first, LN_ROWS), :] = value

        norm_into(put_e, lambda first: xbuf[slot, pl.ds(first, LN_ROWS), :], rep(4), rep(5))

        @pl.when(slot < ONLY)
        def _():
            clip = only_clip(chip, core, slot)
            e_far(slot, clip).start()
            e_local(slot, clip).start()
            e_sib(slot, clip).start()

        @pl.when(slot >= ONLY)
        def _():
            clip = core * SHARED + slot - ONLY
            e_local(slot, clip).start()
            e_sib(slot, clip).start()

    mlp_units = ("w1a", "w1b", "w2a", "w2b")

    def relays(step, place):
        for (when, where), todo in RELAYS.items():
            if where == place:
                @pl.when(step == when)
                def _():
                    for stage, name in todo:
                        (w_stage1 if stage == 1 else w_stage2)(name)

    def step_body(step, _):
        relays(step, 0)

        @pl.when(step < SLOTS)
        def _():
            attention(step, step)

        relays(step, 1)

        @pl.when(step == 0)
        def _():
            for name in mlp_units:
                w_wait_near(name)

        @pl.when(step < SLOTS)
        def _():
            mlp_near(step)

        relays(step, 2)

        @pl.when(step == LAG)
        def _():
            for name in mlp_units:
                w_wait_far(name)

        @pl.when(step >= LAG)
        def _():
            mlp_far(step - LAG)

        return 0

    lax.fori_loop(0, SLOTS + LAG, step_body, 0)

    for slot in range(ONLY):
        clip = only_clip(other_chip, core, slot)
        e_far(slot, clip).wait_recv()
        e_relay(slot, clip).start()
    for slot in range(SLOTS):
        clip = clip_of(chip, core, slot)
        e_local(slot, clip).wait()
        e_sib(slot, clip).wait_send()
        e_sib(slot, clip_of(chip, other_core, slot)).wait_recv()
    for slot in range(ONLY):
        e_far(slot, only_clip(chip, core, slot)).wait_send()
        e_relay(slot, only_clip(other_chip, core, slot)).wait_send()
        e_relay(slot, only_clip(other_chip, other_core, slot)).wait_recv()
    for slot in range(SLOTS):
        for link in range(3):
            x_copy(slot, link).wait_send()
    for name in units:
        w_drain(name)
    for link in range(3):
        s_copy(link, tp).wait_send()


def encode(x, weights, vectors):
    dma = pltpu.SemaphoreType.DMA
    any_spec = pl.BlockSpec(memory_space=pl.ANY)
    return pl.pallas_call(
        encoder_kernel,
        out_shape=jax.ShapeDtypeStruct((CLIPS, FRAMES, WIDTH), BF16),
        in_specs=[any_spec] * 7 + [pl.BlockSpec(memory_space=pltpu.VMEM)] * 11,
        out_specs=any_spec,
        scratch_shapes=[
            pltpu.VMEM((8, WIDTH), F32), pltpu.VMEM((8, WIDTH), F32), pltpu.VMEM((8, HIDDEN), F32),
            pltpu.VMEM((SLOTS, FRAMES, WIDTH), BF16),
            pltpu.VMEM((2 * WIDTH, WIDTH), BF16), pltpu.VMEM((WIDTH, WIDTH), BF16), pltpu.VMEM((WIDTH, WIDTH), BF16),
            pltpu.VMEM((WIDTH, HIDDEN), BF16), pltpu.VMEM((HIDDEN, WIDTH), BF16),
            pltpu.VMEM((4, 8, WIDTH), F32),
            pltpu.VMEM((FRAMES, WIDTH), BF16), pltpu.VMEM((FRAMES, 2 * WIDTH), BF16), pltpu.VMEM((WIDTH, FRAMES), BF16),
            pltpu.VMEM((FRAMES, WIDTH), BF16),
            pltpu.VMEM((SLOTS, FRAMES, WIDTH), BF16),
            pltpu.VMEM((FRAMES, 2 * WIDTH), BF16),
            pltpu.VMEM((SLOTS, FRAMES, WIDTH), F32),
            pltpu.VMEM((8, 2 * WIDTH), F32),
            dma((SLOTS, 3)), dma((SLOTS, 3)), dma((SLOTS,)),
            dma((8, 5)), dma((8, 5)), dma((8,)),
            dma((3,)), dma((3,)),
            dma((SLOTS + 2 * ONLY,)), dma((SLOTS + 2 * ONLY,)), dma((SLOTS,)),
        ],
        compiler_params=pltpu.CompilerParams(collective_id=0, has_side_effects=True, vmem_limit_bytes=64 * 1024 * 1024 - 128 * 1024),
        name="encoder",
    )(x, *weights, *vectors)


def cache_kernel(tp_ref, e_ref, wk_hbm, wv_hbm, bias_ref, k_ref, v_ref, enc_ref, weights, shift, sems):
    @pl.when(pl.program_id(0) == 0)
    def _():
        copies = [pltpu.make_async_copy(src.at[layer], weights.at[pl.ds(which * WIDTH + layer * LOC_COLS, LOC_COLS), :], sems.at[which, layer])
                  for which, src in enumerate((wk_hbm, wv_hbm)) for layer in range(4)]
        for copy in copies:
            copy.start()
        rows = jnp.concatenate([bias_ref[...].astype(F32), jnp.zeros((4, LOC_COLS), F32)], axis=0)
        for layer in range(4):
            pick = (lax.broadcasted_iota(jnp.int32, (8, 128), 0) == layer).astype(F32)
            shift[layer * LOC_COLS:(layer + 1) * LOC_COLS, :] = dot(rows, pick, TN)
        for copy in copies:
            copy.wait()

    enc_ref[0] = e_ref[0, pl.ds(pl.multiple_of(tp_ref[0] * LOC_FRAMES, LOC_FRAMES), LOC_FRAMES), :]
    both = dot(weights[...], e_ref[0], NT)
    for layer in range(4):
        rows = slice(layer * LOC_COLS, (layer + 1) * LOC_COLS)
        k_ref[layer, 0] = both[rows, :].astype(BF16)
        v_ref[layer, 0] = (both[WIDTH + layer * LOC_COLS:WIDTH + (layer + 1) * LOC_COLS, :] + jnp.concatenate([shift[rows, :]] * 4, axis=1)).astype(BF16)


def caches(tp, e_all, wck_t, wcv_t, bias):
    cache = jax.ShapeDtypeStruct((4, CLIPS, LOC_COLS, FRAMES), BF16)
    cache_spec = pl.BlockSpec((4, 1, LOC_COLS, FRAMES), lambda clip, tp_ref: (0, clip, 0, 0))
    any_spec = pl.BlockSpec(memory_space=pl.ANY)
    return pl.pallas_call(
        cache_kernel,
        out_shape=(cache, cache, jax.ShapeDtypeStruct((CLIPS, LOC_FRAMES, WIDTH), BF16)),
        grid_spec=pltpu.PrefetchScalarGridSpec(
            num_scalar_prefetch=1,
            grid=(CLIPS,),
            in_specs=[
                pl.BlockSpec((1, FRAMES, WIDTH), lambda clip, tp_ref: (clip, 0, 0)),
                any_spec, any_spec,
                pl.BlockSpec((4, LOC_COLS), lambda clip, tp_ref: (0, 0)),
            ],
            out_specs=(cache_spec, cache_spec, pl.BlockSpec((1, LOC_FRAMES, WIDTH), lambda clip, tp_ref: (clip, 0, 0))),
            scratch_shapes=[pltpu.VMEM((2 * WIDTH, WIDTH), BF16), pltpu.VMEM((WIDTH, 128), F32), pltpu.SemaphoreType.DMA((2, 4))],
        ),
        compiler_params=pltpu.CompilerParams(dimension_semantics=("arbitrary",), vmem_limit_bytes=64 * 1024 * 1024 - 128 * 1024),
        name="caches",
    )(tp, e_all, wck_t, wcv_t, bias)


def device_body(hidden_loc, ln1_gain, ln1_bias, w_q, b_q, w_k, w_v, b_v, w_o, b_o, ln2_gain, ln2_bias, w_fc1, b_fc1, w_fc2, b_fc2, post_gain, post_bias, w_ck, w_cv, b_cv):
    weights = (w_q.T, w_k.T, w_v.T, w_o, w_fc1, w_fc2)
    vectors = (ln1_gain, ln1_bias, ln2_gain, ln2_bias, post_gain, post_bias, b_o, b_fc2, b_fc1, b_q, b_v)
    e_all = encode(hidden_loc, weights, vectors)
    tp = lax.axis_index("tp").astype(jnp.int32).reshape(1)
    k_t, v_t, enc_loc = caches(tp, e_all, w_ck.transpose(0, 2, 1), w_cv.transpose(0, 2, 1), b_cv)
    shape = (4, CLIPS, FRAMES, 3, HEAD_DIM)
    return enc_loc, k_t.transpose(0, 1, 3, 2).reshape(shape), v_t.transpose(0, 1, 3, 2).reshape(shape)


def solution(mesh):
    in_specs = (P("dp", "tp", None), P(), P(), P(None, "tp"), P("tp"), P(None, "tp"), P(None, "tp"), P("tp"), P("tp", None), P(), P(), P(), P(None, "tp"), P("tp"), P("tp", None), P(), P(), P(), P(None, None, "tp"), P(None, None, "tp"), P(None, "tp"))
    out_specs = (P("dp", "tp", None), P(None, "dp", None, "tp", None), P(None, "dp", None, "tp", None))
    return jax.shard_map(device_body, mesh=mesh, in_specs=in_specs, out_specs=out_specs, check_vma=False)
```

```python
import functools

import jax
import jax.numpy as jnp
from jax import lax
from jax.experimental import pallas as pl
from jax.experimental.pallas import tpu as pltpu
from jax.sharding import PartitionSpec as P

HEAD_DIM = 64
ATTN_SCALE = HEAD_DIM ** -0.25
LN_EPS = 1e-5
SQRT_HALF = 0.5 ** 0.5
MESH = pl.DeviceIdType.MESH
BF16, F32 = jnp.bfloat16, jnp.float32

CLIPS, FRAMES, WIDTH, HIDDEN = 16, 512, 768, 3072
LOC_FRAMES, LOC_COLS = FRAMES // 4, WIDTH // 4
WIDE = (slice(0, 512), slice(512, 768))
SHARED, ONLY = 6, 1
SLOTS = SHARED + ONLY
LAG = 3
LN_ROWS = 64
SEND_ORDER = ("q", "k", "v", 0, "o", 1, 2, "w1a", "w1b", 3, "w2a", "w2b", 4, 5, 6)
RELAYS = {
    (3, 0): ((1, "w1a"), (1, "w1b")),
    (3, 1): ((2, "w1a"), (2, "w1b"), (1, "w2a"), (1, "w2b")),
    (3, 2): ((2, "w2a"), (2, "w2b")),
}
OUT_SLOTS = 6

NT = (((1,), (1,)), ((), ()))
NN = (((1,), (0,)), ((), ()))
TN = (((0,), (0,)), ((), ()))


def dot(lhs, rhs, dims=NN):
    return lax.dot_general(lhs, rhs, dims, preferred_element_type=F32)


def norm_rows(values, gain, bias):
    centered = values.astype(F32)
    centered = centered - jnp.mean(centered, axis=-1, keepdims=True)
    row_var = jnp.mean(centered * centered, axis=-1, keepdims=True)
    return (centered * lax.rsqrt(row_var + LN_EPS) * gain + bias).astype(BF16)


def only_clip(chip, core, slot):
    return 2 * SHARED + (2 * chip + core) * ONLY + slot


def clip_of(chip, core, slot):
    return only_clip(chip, core, slot) if slot < ONLY else core * SHARED + slot - ONLY


def rows_of(ref, start, count):
    return ref.at[pl.ds(pl.multiple_of(start, 16), count), :]


def encoder_kernel(x_hbm, wq_hbm, wk_hbm, wv_hbm, wo_hbm, w1_hbm, w2_hbm,
                   g1_ref, s1_ref, g2_ref, s2_ref, g3_ref, s3_ref, bo_ref, b2_ref, b1_ref, bq_ref, bv_ref, e_hbm,
                   rep_ref, loc, b1_row, xbuf, wqv, wk, wo, w1, w2, small, abuf, qvbuf, ktbuf, obuf, mbuf, gbuf, acc, bias,
                   x_send, x_recv, x_loc, w_send, w_recv, w_loc, s_send, s_recv, e_send, e_recv, e_loc):
    group, tp = lax.axis_index("dp"), lax.axis_index("tp")
    chip, core = tp // 2, tp % 2
    other_chip, other_core = 1 - chip, 1 - core
    t_sib = 2 * chip + other_core
    t_far = 2 * other_chip + core
    t_diag = 2 * other_chip + other_core
    sib = {"dp": group, "tp": t_sib}
    far = {"dp": group, "tp": t_far}
    diag = {"dp": group, "tp": t_diag}
    side = {"dp": 1 - group, "tp": tp}

    def remote(src, dst, send, recv, device):
        return pltpu.make_async_remote_copy(src_ref=src, dst_ref=dst, send_sem=send, recv_sem=recv, device_id=device, device_id_type=MESH)

    def frames(slot, owner):
        return xbuf.at[slot, pl.ds(pl.multiple_of(owner * LOC_FRAMES, LOC_FRAMES), LOC_FRAMES), :]

    def x_copy(slot, link):
        device, there_chip, there_core = ((sib, chip, other_core), (far, other_chip, core), (diag, other_chip, other_core))[link]
        return remote(x_hbm.at[clip_of(there_chip, there_core, slot)], frames(slot, tp), x_send.at[slot, link], x_recv.at[slot, link], device)

    def x_local(slot):
        return pltpu.make_async_copy(x_hbm.at[clip_of(chip, core, slot)], frames(slot, tp), x_loc.at[slot])

    def x_wait(slot):
        pltpu.make_async_copy(x_hbm.at[0], frames(slot, tp), x_loc.at[slot]).wait()
        for link, owner in enumerate((t_sib, t_far, t_diag)):
            remote(x_hbm.at[0], frames(slot, owner), x_send.at[slot, link], x_recv.at[slot, link], sib).wait_recv()

    def at_rows(dst, base):
        shard = LOC_COLS if dst is not w2 else WIDTH
        return lambda owner, first, count: rows_of(dst, base + owner * shard + first, count)

    def at_columns(owner, first, count):
        return w1.at[pl.ds(pl.multiple_of(first, 16), count), pl.ds(pl.multiple_of(owner * WIDTH, WIDTH), WIDTH)]

    units = {
        "q": (0, wq_hbm, at_rows(wqv, 0), 0, 192), "k": (1, wk_hbm, at_rows(wk, 0), 0, 192),
        "v": (2, wv_hbm, at_rows(wqv, WIDTH), 0, 192), "o": (3, wo_hbm, at_rows(wo, 0), 0, 192),
        "w1a": (4, w1_hbm, at_columns, 0, 384), "w1b": (5, w1_hbm, at_columns, 384, 384),
        "w2a": (6, w2_hbm, at_rows(w2, 0), 0, 384), "w2b": (7, w2_hbm, at_rows(w2, 0), 384, 384),
    }

    def w_local(name):
        idx, src, place, first, count = units[name]
        return pltpu.make_async_copy(src.at[pl.ds(first, count), :], place(tp, first, count), w_loc.at[idx])

    def w_sib(name, owner):
        idx, src, place, first, count = units[name]
        return remote(src.at[pl.ds(first, count), :], place(owner, first, count), w_send.at[idx, 0], w_recv.at[idx, 0], sib)

    def w_far(name, owner):
        idx, src, place, first, count = units[name]
        half = count // 2
        return remote(rows_of(src, first + group * half, half), place(owner, first + group * half, half),
                      w_send.at[idx, 1], w_recv.at[idx, 1], far)

    def w_relay(name, owner, part, sem, recv, device):
        idx, src, place, first, count = units[name]
        half = count // 2
        piece = place(owner, first + part * half, half)
        return remote(piece, piece, w_send.at[idx, sem], w_recv.at[idx, recv], device)

    def w_start(name):
        w_far(name, tp).start()
        w_local(name).start()
        w_sib(name, tp).start()

    def w_stage1(name):
        w_far(name, t_far).wait_recv()
        w_relay(name, t_far, group, 3, 2, side).start()
        w_relay(name, t_far, group, 2, 3, sib).start()

    def w_stage2(name):
        w_relay(name, t_far, 1 - group, 3, 2, side).wait_recv()
        w_relay(name, t_far, 1 - group, 4, 4, sib).start()

    def w_wait_near(name):
        w_local(name).wait()
        w_sib(name, t_sib).wait_recv()

    def w_wait_far(name):
        w_relay(name, t_diag, group, 2, 3, sib).wait_recv()
        w_relay(name, t_diag, 1 - group, 4, 4, sib).wait_recv()

    def w_drain(name):
        w_sib(name, tp).wait_send()
        w_far(name, tp).wait_send()
        w_relay(name, t_far, group, 3, 2, side).wait_send()
        w_relay(name, t_far, group, 2, 3, sib).wait_send()
        w_relay(name, t_far, 1 - group, 4, 4, sib).wait_send()

    def s_copy(link, owner):
        device = (sib, far, diag)[link]
        return remote(loc, small.at[owner], s_send.at[link], s_recv.at[link], device)

    def e_local(slot, clip):
        return pltpu.make_async_copy(xbuf.at[slot], e_hbm.at[clip], e_loc.at[slot])

    def e_sib(slot, clip):
        return remote(xbuf.at[slot], e_hbm.at[clip], e_send.at[slot], e_recv.at[slot], sib)

    def e_far(slot, clip):
        return remote(xbuf.at[slot], e_hbm.at[clip], e_send.at[SLOTS + slot], e_recv.at[SLOTS + slot], far)

    def e_relay(slot, clip):
        sem = SLOTS + ONLY + slot
        return remote(e_hbm.at[clip], e_hbm.at[clip], e_send.at[sem], e_recv.at[sem], sib)

    for row, ref in enumerate((g1_ref, s1_ref, g2_ref, s2_ref, g3_ref, s3_ref, bo_ref, b2_ref)):
        rep_ref[row:row + 1, :] = ref[...].astype(F32).reshape(1, WIDTH)
    place = lax.broadcasted_iota(jnp.int32, (192, WIDTH), 0) + tp * 192 == lax.broadcasted_iota(jnp.int32, (192, WIDTH), 1)
    place = place.astype(F32).astype(BF16)
    loc[0:1, :] = b1_ref[...].astype(F32).reshape(1, WIDTH)
    for row, ref in ((1, bq_ref), (2, bv_ref)):
        vector = jnp.broadcast_to(ref[...].astype(F32).reshape(1, 192), (16, 192)).astype(BF16)
        loc[row:row + 1, :] = dot(vector, place)[0:1, :]
    loc[3:8, :] = jnp.zeros((5, WIDTH), F32)
    small[tp] = loc[...]

    barrier = pltpu.get_barrier_semaphore()
    for device in (sib, far, diag, side):
        pl.semaphore_signal(barrier, inc=1, device_id=device, device_id_type=MESH)
    pl.semaphore_wait(barrier, 4)

    for item in SEND_ORDER:
        if item == 0:
            for link in range(3):
                s_copy(link, tp).start()
        if isinstance(item, str):
            w_start(item)
        else:
            x_copy(item, 1).start()
            x_copy(item, 2).start()
            x_local(item).start()
            x_copy(item, 0).start()

    for link, owner in enumerate((t_sib, t_far, t_diag)):
        s_copy(link, owner).wait_recv()
    bias[0:1, 0:WIDTH] = small[0, 1:2, :] + small[1, 1:2, :] + small[2, 1:2, :] + small[3, 1:2, :]
    bias[0:1, WIDTH:2 * WIDTH] = small[0, 2:3, :] + small[1, 2:3, :] + small[2, 2:3, :] + small[3, 2:3, :]
    for owner in range(4):
        b1_row[0:1, owner * WIDTH:owner * WIDTH + WIDTH] = small[owner, 0:1, :]
    for name in ("q", "k", "v"):
        w_stage1(name)
    for name in ("q", "k", "v"):
        w_stage2(name)
    for name in ("q", "k", "v"):
        w_wait_near(name)
        w_wait_far(name)

    def rep(row):
        return rep_ref[row:row + 1, :]

    def norm_into(dst_store, src_load, gain, shift):
        for first in range(0, FRAMES, LN_ROWS):
            dst_store(first, norm_rows(src_load(first), gain, shift))

    def attention(slot, step):
        x_wait(slot)

        def put_a(first, value):
            abuf[first:first + LN_ROWS, :] = value

        norm_into(put_a, lambda first: xbuf[slot, pl.ds(first, LN_ROWS), :], rep(0), rep(1))
        scale = jnp.where(lax.broadcasted_iota(jnp.int32, (1, 2 * WIDTH), 1) < WIDTH, ATTN_SCALE, 1.0)
        ktbuf[...] = (dot(wk[...], abuf[...], NT) * ATTN_SCALE).astype(BF16)
        for col in range(0, 2 * WIDTH, 512):
            cols = slice(col, col + 512)
            qvbuf[:, cols] = ((dot(abuf[...], wqv[cols, :], NT) + bias[0:1, cols]) * scale[:, cols]).astype(BF16)

        lane = lax.broadcasted_iota(jnp.int32, (1, 128), 1)
        keep = [(lane < 64).astype(F32).astype(BF16), (lane >= 64).astype(F32).astype(BF16)]

        def pair_body(pair, _):
            cols = pl.ds(pl.multiple_of(pair * 128, 128), 128)
            keys_t = ktbuf[cols, :]
            values = qvbuf[:, pl.ds(pl.multiple_of(WIDTH + pair * 128, 128), 128)]

            def scores_of(head):
                return dot(qvbuf[:, cols] * keep[head], keys_t)

            scores = scores_of(0)
            outs = []
            for head in range(2):
                ahead = scores_of(1) if head == 0 else None
                top = jnp.max(scores, axis=-1, keepdims=True)
                weight = jnp.exp(scores - top)
                total = jnp.sum(weight, axis=-1, keepdims=True)
                outs.append(dot(weight.astype(BF16), values) * (1.0 / total))
                scores = ahead
            obuf[:, cols] = jnp.where(lane < 64, outs[0], outs[1]).astype(BF16)
            return 0

        lax.fori_loop(0, 6, pair_body, 0)

        @pl.when(step == 0)
        def _():
            w_stage1("o")
            w_stage2("o")
            w_wait_near("o")
            w_wait_far("o")

        for cols in WIDE:
            branch = (dot(obuf[...], wo[:, cols]) + rep_ref[6:7, cols]).astype(BF16)
            xbuf[slot, :, cols] = (xbuf[slot, :, cols].astype(F32) + branch.astype(F32)).astype(BF16)

        def put_m(first, value):
            mbuf[slot, pl.ds(first, LN_ROWS), :] = value

        norm_into(put_m, lambda first: xbuf[slot, pl.ds(first, LN_ROWS), :], rep(2), rep(3))

    def hidden_half(slot, which):
        def product(col):
            return dot(mbuf[slot], w1[:, pl.ds(pl.multiple_of(which * 1536 + col, 512), 512)])

        ahead = product(0)
        for col in range(0, 1536, 512):
            inner = ahead + b1_row[0:1, pl.ds(pl.multiple_of(which * 1536 + col, 512), 512)]
            if col + 512 < 1536:
                ahead = product(col + 512)
            gbuf[:, col:col + 512] = (0.5 * inner * (1.0 + lax.erf(inner * SQRT_HALF))).astype(BF16)

    def second_product(which, cols):
        return dot(gbuf[...], w2[pl.ds(pl.multiple_of(which * 1536, 1536), 1536), cols])

    def mlp_near(slot):
        hidden_half(slot, chip)
        for cols in WIDE:
            acc[slot, :, cols] = second_product(chip, cols)

    def mlp_far(slot):
        hidden_half(slot, other_chip)
        for cols in WIDE:
            branch = (acc[slot, :, cols] + second_product(other_chip, cols) + rep_ref[7:8, cols]).astype(BF16)
            xbuf[slot, :, cols] = (xbuf[slot, :, cols].astype(F32) + branch.astype(F32)).astype(BF16)

        def put_e(first, value):
            xbuf[slot, pl.ds(first, LN_ROWS), :] = value

        norm_into(put_e, lambda first: xbuf[slot, pl.ds(first, LN_ROWS), :], rep(4), rep(5))

        @pl.when(slot < ONLY)
        def _():
            clip = only_clip(chip, core, slot)
            e_far(slot, clip).start()
            e_local(slot, clip).start()
            e_sib(slot, clip).start()

        @pl.when(slot >= ONLY)
        def _():
            clip = core * SHARED + slot - ONLY
            e_local(slot, clip).start()
            e_sib(slot, clip).start()

    mlp_units = ("w1a", "w1b", "w2a", "w2b")

    def relays(step, place):
        for (when, where), todo in RELAYS.items():
            if where == place:
                @pl.when(step == when)
                def _():
                    for stage, name in todo:
                        (w_stage1 if stage == 1 else w_stage2)(name)

    def step_body(step, _):
        relays(step, 0)

        @pl.when(step < SLOTS)
        def _():
            attention(step, step)

        relays(step, 1)

        @pl.when(step == 0)
        def _():
            for name in mlp_units:
                w_wait_near(name)

        @pl.when(step < SLOTS)
        def _():
            mlp_near(step)

        relays(step, 2)

        @pl.when(step == LAG)
        def _():
            for name in mlp_units:
                w_wait_far(name)

        @pl.when(step >= LAG)
        def _():
            mlp_far(step - LAG)

        return 0

    lax.fori_loop(0, SLOTS + LAG, step_body, 0)

    for slot in range(ONLY):
        clip = only_clip(other_chip, core, slot)
        e_far(slot, clip).wait_recv()
        e_relay(slot, clip).start()
    for slot in range(SLOTS):
        clip = clip_of(chip, core, slot)
        e_local(slot, clip).wait()
        e_sib(slot, clip).wait_send()
        e_sib(slot, clip_of(chip, other_core, slot)).wait_recv()
    for slot in range(ONLY):
        e_far(slot, only_clip(chip, core, slot)).wait_send()
        e_relay(slot, only_clip(other_chip, core, slot)).wait_send()
        e_relay(slot, only_clip(other_chip, other_core, slot)).wait_recv()
    for slot in range(SLOTS):
        for link in range(3):
            x_copy(slot, link).wait_send()
    for name in units:
        w_drain(name)
    for link in range(3):
        s_copy(link, tp).wait_send()


def encode(x, weights, vectors):
    dma = pltpu.SemaphoreType.DMA
    any_spec = pl.BlockSpec(memory_space=pl.ANY)
    return pl.pallas_call(
        encoder_kernel,
        out_shape=jax.ShapeDtypeStruct((CLIPS, FRAMES, WIDTH), BF16),
        in_specs=[any_spec] * 7 + [pl.BlockSpec(memory_space=pltpu.VMEM)] * 11,
        out_specs=any_spec,
        scratch_shapes=[
            pltpu.VMEM((8, WIDTH), F32), pltpu.VMEM((8, WIDTH), F32), pltpu.VMEM((8, HIDDEN), F32),
            pltpu.VMEM((SLOTS, FRAMES, WIDTH), BF16),
            pltpu.VMEM((2 * WIDTH, WIDTH), BF16), pltpu.VMEM((WIDTH, WIDTH), BF16), pltpu.VMEM((WIDTH, WIDTH), BF16),
            pltpu.VMEM((WIDTH, HIDDEN), BF16), pltpu.VMEM((HIDDEN, WIDTH), BF16),
            pltpu.VMEM((4, 8, WIDTH), F32),
            pltpu.VMEM((FRAMES, WIDTH), BF16), pltpu.VMEM((FRAMES, 2 * WIDTH), BF16), pltpu.VMEM((WIDTH, FRAMES), BF16),
            pltpu.VMEM((FRAMES, WIDTH), BF16),
            pltpu.VMEM((SLOTS, FRAMES, WIDTH), BF16),
            pltpu.VMEM((FRAMES, 2 * WIDTH), BF16),
            pltpu.VMEM((SLOTS, FRAMES, WIDTH), F32),
            pltpu.VMEM((8, 2 * WIDTH), F32),
            dma((SLOTS, 3)), dma((SLOTS, 3)), dma((SLOTS,)),
            dma((8, 5)), dma((8, 5)), dma((8,)),
            dma((3,)), dma((3,)),
            dma((SLOTS + 2 * ONLY,)), dma((SLOTS + 2 * ONLY,)), dma((SLOTS,)),
        ],
        compiler_params=pltpu.CompilerParams(collective_id=0, has_side_effects=True, vmem_limit_bytes=64 * 1024 * 1024 - 128 * 1024),
        name="encoder",
    )(x, *weights, *vectors)


def cache_kernel(e_hbm, wk_hbm, wv_hbm, bias_ref, k_hbm, v_hbm, enc_hbm, weights, shift, ebuf, obuf, w_sem, e_sem, out_sem, enc_sem):
    tp = lax.axis_index("tp")

    def load(clip):
        return pltpu.make_async_copy(e_hbm.at[clip], ebuf.at[clip], e_sem.at[clip])

    def stores(clip, slot):
        copies = []
        for which, dst in enumerate((k_hbm, v_hbm)):
            for layer in range(4):
                rows = pl.ds(which * WIDTH + layer * LOC_COLS, LOC_COLS)
                copies.append(pltpu.make_async_copy(obuf.at[slot, rows, :], dst.at[layer, clip], out_sem.at[slot, which * 4 + layer]))
        return copies

    def enc_store(clip):
        own = pl.ds(pl.multiple_of(tp * LOC_FRAMES, LOC_FRAMES), LOC_FRAMES)
        return pltpu.make_async_copy(ebuf.at[clip, own, :], enc_hbm.at[clip], enc_sem.at[clip])

    load(0).start()
    weight_loads = [pltpu.make_async_copy(src.at[layer], weights.at[pl.ds(which * WIDTH + layer * LOC_COLS, LOC_COLS), :], w_sem.at[which, layer])
                    for which, src in enumerate((wk_hbm, wv_hbm)) for layer in range(4)]
    for copy in weight_loads:
        copy.start()
    for clip in range(1, CLIPS):
        load(clip).start()
    rows = jnp.concatenate([bias_ref[...].astype(F32), jnp.zeros((4, LOC_COLS), F32)], axis=0)
    for layer in range(4):
        pick = (lax.broadcasted_iota(jnp.int32, (8, 128), 0) == layer).astype(F32)
        shift[layer * LOC_COLS:(layer + 1) * LOC_COLS, :] = dot(rows, pick, TN)
    for copy in weight_loads:
        copy.wait()

    def body(step, _):
        for half in range(2):
            clip = 2 * step + half
            slot = clip % OUT_SLOTS
            load(clip).wait()
            enc_store(clip).start()

            @pl.when(clip >= OUT_SLOTS)
            def _():
                for copy in stores(clip - OUT_SLOTS, slot):
                    copy.wait()

        for half in range(2):
            clip = 2 * step + half
            slot = clip % OUT_SLOTS
            obuf[slot, 0:WIDTH, :] = dot(weights[0:WIDTH, :], ebuf[clip], NT).astype(BF16)
            obuf[slot, WIDTH:2 * WIDTH, :] = (dot(weights[WIDTH:2 * WIDTH, :], ebuf[clip], NT) + jnp.concatenate([shift[...]] * 4, axis=1)).astype(BF16)
        for half in range(2):
            clip = 2 * step + half
            for copy in stores(clip, clip % OUT_SLOTS):
                copy.start()
        return 0

    lax.fori_loop(0, CLIPS // 2, body, 0)
    for clip in range(CLIPS - OUT_SLOTS, CLIPS):
        for copy in stores(clip, clip % OUT_SLOTS):
            copy.wait()
    for clip in range(CLIPS):
        enc_store(clip).wait()


def caches(e_all, wck_t, wcv_t, bias):
    cache = jax.ShapeDtypeStruct((4, CLIPS, LOC_COLS, FRAMES), BF16)
    any_spec = pl.BlockSpec(memory_space=pl.ANY)
    dma = pltpu.SemaphoreType.DMA
    return pl.pallas_call(
        cache_kernel,
        out_shape=(cache, cache, jax.ShapeDtypeStruct((CLIPS, LOC_FRAMES, WIDTH), BF16)),
        in_specs=[any_spec, any_spec, any_spec, pl.BlockSpec(memory_space=pltpu.VMEM)],
        out_specs=(any_spec, any_spec, any_spec),
        scratch_shapes=[
            pltpu.VMEM((2 * WIDTH, WIDTH), BF16), pltpu.VMEM((WIDTH, 128), F32),
            pltpu.VMEM((CLIPS, FRAMES, WIDTH), BF16), pltpu.VMEM((OUT_SLOTS, 2 * WIDTH, FRAMES), BF16),
            dma((2, 4)), dma((CLIPS,)), dma((OUT_SLOTS, 8)), dma((CLIPS,)),
        ],
        compiler_params=pltpu.CompilerParams(vmem_limit_bytes=64 * 1024 * 1024 - 128 * 1024),
        name="caches",
    )(e_all, wck_t, wcv_t, bias)


def device_body(hidden_loc, ln1_gain, ln1_bias, w_q, b_q, w_k, w_v, b_v, w_o, b_o, ln2_gain, ln2_bias, w_fc1, b_fc1, w_fc2, b_fc2, post_gain, post_bias, w_ck, w_cv, b_cv):
    weights = (w_q.T, w_k.T, w_v.T, w_o, w_fc1, w_fc2)
    vectors = (ln1_gain, ln1_bias, ln2_gain, ln2_bias, post_gain, post_bias, b_o, b_fc2, b_fc1, b_q, b_v)
    e_all = encode(hidden_loc, weights, vectors)
    k_t, v_t, enc_loc = caches(e_all, w_ck.transpose(0, 2, 1), w_cv.transpose(0, 2, 1), b_cv)
    shape = (4, CLIPS, FRAMES, 3, HEAD_DIM)
    return enc_loc, k_t.transpose(0, 1, 3, 2).reshape(shape), v_t.transpose(0, 1, 3, 2).reshape(shape)


def solution(mesh):
    in_specs = (P("dp", "tp", None), P(), P(), P(None, "tp"), P("tp"), P(None, "tp"), P(None, "tp"), P("tp"), P("tp", None), P(), P(), P(), P(None, "tp"), P("tp"), P("tp", None), P(), P(), P(), P(None, None, "tp"), P(None, None, "tp"), P(None, "tp"))
    out_specs = (P("dp", "tp", None), P(None, "dp", None, "tp", None), P(None, "dp", None, "tp", None))
    return jax.shard_map(device_body, mesh=mesh, in_specs=in_specs, out_specs=out_specs, check_vma=False)
```

```python
import functools

import jax
import jax.numpy as jnp
from jax import lax
from jax.experimental import pallas as pl
from jax.experimental.pallas import tpu as pltpu
from jax.sharding import PartitionSpec as P

HEAD_DIM = 64
ATTN_SCALE = HEAD_DIM ** -0.25
LN_EPS = 1e-5
SQRT_HALF = 0.5 ** 0.5
MESH = pl.DeviceIdType.MESH
BF16, F32 = jnp.bfloat16, jnp.float32

CLIPS, FRAMES, WIDTH, HIDDEN = 16, 512, 768, 3072
LOC_FRAMES, LOC_COLS = FRAMES // 4, WIDTH // 4
WIDE = (slice(0, 512), slice(512, 768))
SHARED, ONLY = 4, 2
SLOTS = SHARED + ONLY
LAG = SLOTS // 2
LN_ROWS = 64
SEND_ORDER = ("q", "k", "v", 0, "o", 1, 2, "w1a", "w1b", 3, "w2a", "w2b", 4, 5)
RELAYS = {
    (0, 1): ((1, "o"),), (0, 5): ((2, "o"),),
    (2, 2): ((1, "w1a"),), (2, 5): ((1, "w1b"), (2, "w1a")),
    (3, 0): ((2, "w1b"),), (3, 3): ((1, "w2a"),), (3, 5): ((1, "w2b"), (2, "w2a")),
}
OUT_SLOTS, AHEAD = 6, 4

NT = (((1,), (1,)), ((), ()))
NN = (((1,), (0,)), ((), ()))
TN = (((0,), (0,)), ((), ()))


def dot(lhs, rhs, dims=NN):
    return lax.dot_general(lhs, rhs, dims, preferred_element_type=F32)


def norm_rows(values, gain, bias):
    centered = values.astype(F32)
    centered = centered - jnp.mean(centered, axis=-1, keepdims=True)
    row_var = jnp.mean(centered * centered, axis=-1, keepdims=True)
    return (centered * lax.rsqrt(row_var + LN_EPS) * gain + bias).astype(BF16)


def only_clip(chip, core, slot):
    return 2 * SHARED + (2 * chip + core) * ONLY + slot


def clip_of(chip, core, slot):
    return only_clip(chip, core, slot) if slot < ONLY else core * SHARED + slot - ONLY


def rows_of(ref, start, count):
    return ref.at[pl.ds(pl.multiple_of(start, 16), count), :]


def encoder_kernel(x_hbm, wq_hbm, wk_hbm, wv_hbm, wo_hbm, w1_hbm, w2_hbm,
                   g1_ref, s1_ref, g2_ref, s2_ref, g3_ref, s3_ref, bo_ref, b2_ref, b1_ref, bq_ref, bv_ref, e_hbm,
                   rep_ref, loc, b1_row, xbuf, wqv, wk, wo, w1, w2, small, abuf, qvbuf, ktbuf, obuf, mbuf, gbuf, acc, bias,
                   x_send, x_recv, x_loc, w_send, w_recv, w_loc, s_send, s_recv, e_send, e_recv, e_loc):
    group, tp = lax.axis_index("dp"), lax.axis_index("tp")
    chip, core = tp // 2, tp % 2
    other_chip, other_core = 1 - chip, 1 - core
    t_sib = 2 * chip + other_core
    t_far = 2 * other_chip + core
    t_diag = 2 * other_chip + other_core
    sib = {"dp": group, "tp": t_sib}
    far = {"dp": group, "tp": t_far}
    diag = {"dp": group, "tp": t_diag}
    side = {"dp": 1 - group, "tp": tp}

    def remote(src, dst, send, recv, device):
        return pltpu.make_async_remote_copy(src_ref=src, dst_ref=dst, send_sem=send, recv_sem=recv, device_id=device, device_id_type=MESH)

    def frames(slot, owner):
        return xbuf.at[slot, pl.ds(pl.multiple_of(owner * LOC_FRAMES, LOC_FRAMES), LOC_FRAMES), :]

    def x_copy(slot, link):
        device, there_chip, there_core = ((sib, chip, other_core), (far, other_chip, core), (diag, other_chip, other_core))[link]
        return remote(x_hbm.at[clip_of(there_chip, there_core, slot)], frames(slot, tp), x_send.at[slot, link], x_recv.at[slot, link], device)

    def x_local(slot):
        return pltpu.make_async_copy(x_hbm.at[clip_of(chip, core, slot)], frames(slot, tp), x_loc.at[slot])

    def x_wait(slot):
        pltpu.make_async_copy(x_hbm.at[0], frames(slot, tp), x_loc.at[slot]).wait()
        for link, owner in enumerate((t_sib, t_far, t_diag)):
            remote(x_hbm.at[0], frames(slot, owner), x_send.at[slot, link], x_recv.at[slot, link], sib).wait_recv()

    def at_rows(dst, base):
        shard = LOC_COLS if dst is not w2 else WIDTH
        return lambda owner, first, count: rows_of(dst, base + owner * shard + first, count)

    def at_columns(owner, first, count):
        return w1.at[pl.ds(pl.multiple_of(first, 16), count), pl.ds(pl.multiple_of(owner * WIDTH, WIDTH), WIDTH)]

    units = {
        "q": (0, wq_hbm, at_rows(wqv, 0), 0, 192), "k": (1, wk_hbm, at_rows(wk, 0), 0, 192),
        "v": (2, wv_hbm, at_rows(wqv, WIDTH), 0, 192), "o": (3, wo_hbm, at_rows(wo, 0), 0, 192),
        "w1a": (4, w1_hbm, at_columns, 0, 384), "w1b": (5, w1_hbm, at_columns, 384, 384),
        "w2a": (6, w2_hbm, at_rows(w2, 0), 0, 384), "w2b": (7, w2_hbm, at_rows(w2, 0), 384, 384),
    }

    def w_local(name):
        idx, src, place, first, count = units[name]
        return pltpu.make_async_copy(src.at[pl.ds(first, count), :], place(tp, first, count), w_loc.at[idx])

    def w_sib(name, owner):
        idx, src, place, first, count = units[name]
        return remote(src.at[pl.ds(first, count), :], place(owner, first, count), w_send.at[idx, 0], w_recv.at[idx, 0], sib)

    def w_far(name, owner):
        idx, src, place, first, count = units[name]
        half = count // 2
        return remote(rows_of(src, first + group * half, half), place(owner, first + group * half, half),
                      w_send.at[idx, 1], w_recv.at[idx, 1], far)

    def w_relay(name, owner, part, sem, recv, device):
        idx, src, place, first, count = units[name]
        half = count // 2
        piece = place(owner, first + part * half, half)
        return remote(piece, piece, w_send.at[idx, sem], w_recv.at[idx, recv], device)

    def w_start(name):
        w_far(name, tp).start()
        w_local(name).start()
        w_sib(name, tp).start()

    def w_stage1(name):
        w_far(name, t_far).wait_recv()
        w_relay(name, t_far, group, 3, 2, side).start()
        w_relay(name, t_far, group, 2, 3, sib).start()

    def w_stage2(name):
        w_relay(name, t_far, 1 - group, 3, 2, side).wait_recv()
        w_relay(name, t_far, 1 - group, 4, 4, sib).start()

    def w_wait_near(name):
        w_local(name).wait()
        w_sib(name, t_sib).wait_recv()

    def w_wait_far(name):
        w_relay(name, t_diag, group, 2, 3, sib).wait_recv()
        w_relay(name, t_diag, 1 - group, 4, 4, sib).wait_recv()

    def w_drain(name):
        w_sib(name, tp).wait_send()
        w_far(name, tp).wait_send()
        w_relay(name, t_far, group, 3, 2, side).wait_send()
        w_relay(name, t_far, group, 2, 3, sib).wait_send()
        w_relay(name, t_far, 1 - group, 4, 4, sib).wait_send()

    def s_copy(link, owner):
        device = (sib, far, diag)[link]
        return remote(loc, small.at[owner], s_send.at[link], s_recv.at[link], device)

    def e_local(slot, clip):
        return pltpu.make_async_copy(xbuf.at[slot], e_hbm.at[clip], e_loc.at[slot])

    def e_sib(slot, clip):
        return remote(xbuf.at[slot], e_hbm.at[clip], e_send.at[slot], e_recv.at[slot], sib)

    def e_far(slot, clip):
        return remote(xbuf.at[slot], e_hbm.at[clip], e_send.at[SLOTS + slot], e_recv.at[SLOTS + slot], far)

    def e_relay(slot, clip):
        sem = SLOTS + ONLY + slot
        return remote(e_hbm.at[clip], e_hbm.at[clip], e_send.at[sem], e_recv.at[sem], sib)

    barrier = pltpu.get_barrier_semaphore()
    for device in (sib, far, diag, side):
        pl.semaphore_signal(barrier, inc=1, device_id=device, device_id_type=MESH)

    for row, ref in enumerate((g1_ref, s1_ref, g2_ref, s2_ref, g3_ref, s3_ref, bo_ref, b2_ref)):
        rep_ref[row:row + 1, :] = ref[...].astype(F32).reshape(1, WIDTH)
    place = lax.broadcasted_iota(jnp.int32, (192, WIDTH), 0) + tp * 192 == lax.broadcasted_iota(jnp.int32, (192, WIDTH), 1)
    place = place.astype(F32).astype(BF16)
    loc[0:1, :] = b1_ref[...].astype(F32).reshape(1, WIDTH)
    for row, ref in ((1, bq_ref), (2, bv_ref)):
        vector = jnp.broadcast_to(ref[...].astype(F32).reshape(1, 192), (16, 192)).astype(BF16)
        loc[row:row + 1, :] = dot(vector, place)[0:1, :]
    loc[3:8, :] = jnp.zeros((5, WIDTH), F32)
    small[tp] = loc[...]

    pl.semaphore_wait(barrier, 4)

    for link in (1, 2, 0):
        s_copy(link, tp).start()
    for item in SEND_ORDER:
        if isinstance(item, str):
            w_start(item)
        else:
            x_copy(item, 1).start()
            x_copy(item, 2).start()
            x_local(item).start()
            x_copy(item, 0).start()

    w_stage1("q")
    w_stage1("k")
    w_stage2("q")
    w_stage1("v")
    w_stage2("k")
    for link, owner in enumerate((t_sib, t_far, t_diag)):
        s_copy(link, owner).wait_recv()
    bias[0:1, 0:WIDTH] = small[0, 1:2, :] + small[1, 1:2, :] + small[2, 1:2, :] + small[3, 1:2, :]
    bias[0:1, WIDTH:2 * WIDTH] = small[0, 2:3, :] + small[1, 2:3, :] + small[2, 2:3, :] + small[3, 2:3, :]
    for owner in range(4):
        b1_row[0:1, owner * WIDTH:owner * WIDTH + WIDTH] = small[owner, 0:1, :]
    w_stage2("v")
    for name in ("q", "k", "v"):
        w_wait_near(name)
        w_wait_far(name)

    def rep(row):
        return rep_ref[row:row + 1, :]

    def norm_into(dst_store, src_load, gain, shift):
        for first in range(0, FRAMES, LN_ROWS):
            dst_store(first, norm_rows(src_load(first), gain, shift))

    def attention(slot, step):
        x_wait(slot)

        def put_a(first, value):
            abuf[first:first + LN_ROWS, :] = value

        norm_into(put_a, lambda first: xbuf[slot, pl.ds(first, LN_ROWS), :], rep(0), rep(1))
        scale = jnp.where(lax.broadcasted_iota(jnp.int32, (1, 2 * WIDTH), 1) < WIDTH, ATTN_SCALE, 1.0)
        ktbuf[...] = (dot(wk[...], abuf[...], NT) * ATTN_SCALE).astype(BF16)
        for col in range(0, 2 * WIDTH, 512):
            cols = slice(col, col + 512)
            qvbuf[:, cols] = ((dot(abuf[...], wqv[cols, :], NT) + bias[0:1, cols]) * scale[:, cols]).astype(BF16)

        lane = lax.broadcasted_iota(jnp.int32, (1, 128), 1)
        keep = [(lane < 64).astype(F32).astype(BF16), (lane >= 64).astype(F32).astype(BF16)]

        def pair_body(pair, _):
            for (when, where), todo in RELAYS.items():
                @pl.when((step == when) & (pair == where))
                def _():
                    for stage, name in todo:
                        (w_stage1 if stage == 1 else w_stage2)(name)

            cols = pl.ds(pl.multiple_of(pair * 128, 128), 128)
            keys_t = ktbuf[cols, :]
            values = qvbuf[:, pl.ds(pl.multiple_of(WIDTH + pair * 128, 128), 128)]

            def scores_of(head):
                return dot(qvbuf[:, cols] * keep[head], keys_t)

            scores = scores_of(0)
            outs = []
            for head in range(2):
                ahead = scores_of(1) if head == 0 else None
                top = jnp.max(scores, axis=-1, keepdims=True)
                weight = jnp.exp(scores - top)
                total = jnp.sum(weight, axis=-1, keepdims=True)
                outs.append(dot(weight.astype(BF16), values) * (1.0 / total))
                scores = ahead
            obuf[:, cols] = jnp.where(lane < 64, outs[0], outs[1]).astype(BF16)
            return 0

        lax.fori_loop(0, 6, pair_body, 0)

        @pl.when(step == 0)
        def _():
            w_wait_near("o")
            w_wait_far("o")

        for cols in WIDE:
            branch = (dot(obuf[...], wo[:, cols]) + rep_ref[6:7, cols]).astype(BF16)
            xbuf[slot, :, cols] = (xbuf[slot, :, cols].astype(F32) + branch.astype(F32)).astype(BF16)

        def put_m(first, value):
            mbuf[slot, pl.ds(first, LN_ROWS), :] = value

        norm_into(put_m, lambda first: xbuf[slot, pl.ds(first, LN_ROWS), :], rep(2), rep(3))

    def hidden_half(slot, which):
        def product(col):
            return dot(mbuf[slot], w1[:, pl.ds(pl.multiple_of(which * 1536 + col, 512), 512)])

        ahead = product(0)
        for col in range(0, 1536, 512):
            inner = ahead + b1_row[0:1, pl.ds(pl.multiple_of(which * 1536 + col, 512), 512)]
            if col + 512 < 1536:
                ahead = product(col + 512)
            gbuf[:, col:col + 512] = (0.5 * inner * (1.0 + lax.erf(inner * SQRT_HALF))).astype(BF16)

    def second_product(which, cols):
        return dot(gbuf[...], w2[pl.ds(pl.multiple_of(which * 1536, 1536), 1536), cols])

    def mlp_near(slot):
        hidden_half(slot, chip)
        for cols in WIDE:
            acc[slot, :, cols] = second_product(chip, cols)

    def mlp_far(slot):
        hidden_half(slot, other_chip)
        for cols in WIDE:
            branch = (acc[slot, :, cols] + second_product(other_chip, cols) + rep_ref[7:8, cols]).astype(BF16)
            xbuf[slot, :, cols] = (xbuf[slot, :, cols].astype(F32) + branch.astype(F32)).astype(BF16)

        def put_e(first, value):
            xbuf[slot, pl.ds(first, LN_ROWS), :] = value

        norm_into(put_e, lambda first: xbuf[slot, pl.ds(first, LN_ROWS), :], rep(4), rep(5))

        @pl.when(slot < ONLY)
        def _():
            clip = only_clip(chip, core, slot)
            e_far(slot, clip).start()
            e_local(slot, clip).start()
            e_sib(slot, clip).start()

        @pl.when(slot >= ONLY)
        def _():
            clip = core * SHARED + slot - ONLY
            e_local(slot, clip).start()
            e_sib(slot, clip).start()

    mlp_units = ("w1a", "w1b", "w2a", "w2b")

    def step_body(step, _):
        attention(step, step)

        @pl.when(step == 0)
        def _():
            for name in mlp_units:
                w_wait_near(name)

        mlp_near(step)

        @pl.when(step == LAG)
        def _():
            w_stage2("w2b")
            for name in mlp_units:
                w_wait_far(name)

        @pl.when(step >= LAG)
        def _():
            def far_body(turn, _):
                mlp_far(2 * (step - LAG) + turn)
                return 0

            lax.fori_loop(0, 2, far_body, 0)

        return 0

    lax.fori_loop(0, SLOTS, step_body, 0)

    for slot in range(ONLY):
        clip = only_clip(other_chip, core, slot)
        e_far(slot, clip).wait_recv()
        e_relay(slot, clip).start()
    for slot in range(SLOTS):
        clip = clip_of(chip, core, slot)
        e_local(slot, clip).wait()
        e_sib(slot, clip).wait_send()
        e_sib(slot, clip_of(chip, other_core, slot)).wait_recv()
    for slot in range(ONLY):
        e_far(slot, only_clip(chip, core, slot)).wait_send()
        e_relay(slot, only_clip(other_chip, core, slot)).wait_send()
        e_relay(slot, only_clip(other_chip, other_core, slot)).wait_recv()
    for slot in range(SLOTS):
        for link in range(3):
            x_copy(slot, link).wait_send()
    for name in units:
        w_drain(name)
    for link in range(3):
        s_copy(link, tp).wait_send()


def encode(x, weights, vectors):
    dma = pltpu.SemaphoreType.DMA
    any_spec = pl.BlockSpec(memory_space=pl.ANY)
    return pl.pallas_call(
        encoder_kernel,
        out_shape=jax.ShapeDtypeStruct((CLIPS, FRAMES, WIDTH), BF16),
        in_specs=[any_spec] * 7 + [pl.BlockSpec(memory_space=pltpu.VMEM)] * 11,
        out_specs=any_spec,
        scratch_shapes=[
            pltpu.VMEM((8, WIDTH), F32), pltpu.VMEM((8, WIDTH), F32), pltpu.VMEM((8, HIDDEN), F32),
            pltpu.VMEM((SLOTS, FRAMES, WIDTH), BF16),
            pltpu.VMEM((2 * WIDTH, WIDTH), BF16), pltpu.VMEM((WIDTH, WIDTH), BF16), pltpu.VMEM((WIDTH, WIDTH), BF16),
            pltpu.VMEM((WIDTH, HIDDEN), BF16), pltpu.VMEM((HIDDEN, WIDTH), BF16),
            pltpu.VMEM((4, 8, WIDTH), F32),
            pltpu.VMEM((FRAMES, WIDTH), BF16), pltpu.VMEM((FRAMES, 2 * WIDTH), BF16), pltpu.VMEM((WIDTH, FRAMES), BF16),
            pltpu.VMEM((FRAMES, WIDTH), BF16),
            pltpu.VMEM((SLOTS, FRAMES, WIDTH), BF16),
            pltpu.VMEM((FRAMES, 2 * WIDTH), BF16),
            pltpu.VMEM((SLOTS, FRAMES, WIDTH), F32),
            pltpu.VMEM((8, 2 * WIDTH), F32),
            dma((SLOTS, 3)), dma((SLOTS, 3)), dma((SLOTS,)),
            dma((8, 5)), dma((8, 5)), dma((8,)),
            dma((3,)), dma((3,)),
            dma((SLOTS + 2 * ONLY,)), dma((SLOTS + 2 * ONLY,)), dma((SLOTS,)),
        ],
        compiler_params=pltpu.CompilerParams(collective_id=0, has_side_effects=True, vmem_limit_bytes=64 * 1024 * 1024 - 128 * 1024),
        name="encoder",
    )(x, *weights, *vectors)


def cache_kernel(e_hbm, wk_hbm, wv_hbm, bias_ref, k_hbm, v_hbm, enc_hbm, weights, shift, ebuf, obuf, w_sem, e_sem, out_sem, enc_sem):
    tp = lax.axis_index("tp")

    def load(clip):
        return pltpu.make_async_copy(e_hbm.at[clip], ebuf.at[clip], e_sem.at[clip])

    def stores(clip, slot):
        copies = []
        for which, dst in enumerate((k_hbm, v_hbm)):
            for layer in range(4):
                rows = pl.ds(which * WIDTH + layer * LOC_COLS, LOC_COLS)
                copies.append(pltpu.make_async_copy(obuf.at[slot, rows, :], dst.at[layer, clip], out_sem.at[slot, which * 4 + layer]))
        return copies

    def enc_store(clip):
        own = pl.ds(pl.multiple_of(tp * LOC_FRAMES, LOC_FRAMES), LOC_FRAMES)
        return pltpu.make_async_copy(ebuf.at[clip, own, :], enc_hbm.at[clip], enc_sem.at[clip])

    load(0).start()
    weight_loads = [pltpu.make_async_copy(src.at[layer], weights.at[pl.ds(which * WIDTH + layer * LOC_COLS, LOC_COLS), :], w_sem.at[which, layer])
                    for which, src in enumerate((wk_hbm, wv_hbm)) for layer in range(4)]
    for copy in weight_loads:
        copy.start()
    for clip in range(1, AHEAD):
        load(clip).start()
    rows = jnp.concatenate([bias_ref[...].astype(F32), jnp.zeros((4, LOC_COLS), F32)], axis=0)
    for layer in range(4):
        pick = (lax.broadcasted_iota(jnp.int32, (8, 128), 0) == layer).astype(F32)
        shift[layer * LOC_COLS:(layer + 1) * LOC_COLS, :] = dot(rows, pick, TN)
    for copy in weight_loads:
        copy.wait()

    def body(step, _):
        for half in range(2):
            clip = 2 * step + half
            slot = clip % OUT_SLOTS
            load(clip).wait()
            enc_store(clip).start()

            @pl.when(clip + AHEAD < CLIPS)
            def _():
                load(clip + AHEAD).start()

            @pl.when(clip >= OUT_SLOTS)
            def _():
                for copy in stores(clip - OUT_SLOTS, slot):
                    copy.wait()

        for half in range(2):
            clip = 2 * step + half
            slot = clip % OUT_SLOTS
            obuf[slot, 0:WIDTH, :] = dot(weights[0:WIDTH, :], ebuf[clip], NT).astype(BF16)
            obuf[slot, WIDTH:2 * WIDTH, :] = (dot(weights[WIDTH:2 * WIDTH, :], ebuf[clip], NT) + jnp.concatenate([shift[...]] * 4, axis=1)).astype(BF16)
        for half in range(2):
            clip = 2 * step + half
            for copy in stores(clip, clip % OUT_SLOTS):
                copy.start()
        return 0

    lax.fori_loop(0, CLIPS // 2, body, 0)
    for clip in range(CLIPS - OUT_SLOTS, CLIPS):
        for copy in stores(clip, clip % OUT_SLOTS):
            copy.wait()
    for clip in range(CLIPS):
        enc_store(clip).wait()


def caches(e_all, wck_t, wcv_t, bias):
    cache = jax.ShapeDtypeStruct((4, CLIPS, LOC_COLS, FRAMES), BF16)
    any_spec = pl.BlockSpec(memory_space=pl.ANY)
    dma = pltpu.SemaphoreType.DMA
    return pl.pallas_call(
        cache_kernel,
        out_shape=(cache, cache, jax.ShapeDtypeStruct((CLIPS, LOC_FRAMES, WIDTH), BF16)),
        in_specs=[any_spec, any_spec, any_spec, pl.BlockSpec(memory_space=pltpu.VMEM)],
        out_specs=(any_spec, any_spec, any_spec),
        scratch_shapes=[
            pltpu.VMEM((2 * WIDTH, WIDTH), BF16), pltpu.VMEM((WIDTH, 128), F32),
            pltpu.VMEM((CLIPS, FRAMES, WIDTH), BF16), pltpu.VMEM((OUT_SLOTS, 2 * WIDTH, FRAMES), BF16),
            dma((2, 4)), dma((CLIPS,)), dma((OUT_SLOTS, 8)), dma((CLIPS,)),
        ],
        compiler_params=pltpu.CompilerParams(vmem_limit_bytes=64 * 1024 * 1024 - 128 * 1024),
        name="caches",
    )(e_all, wck_t, wcv_t, bias)


def device_body(hidden_loc, ln1_gain, ln1_bias, w_q, b_q, w_k, w_v, b_v, w_o, b_o, ln2_gain, ln2_bias, w_fc1, b_fc1, w_fc2, b_fc2, post_gain, post_bias, w_ck, w_cv, b_cv):
    weights = (w_q.T, w_k.T, w_v.T, w_o, w_fc1, w_fc2)
    vectors = (ln1_gain, ln1_bias, ln2_gain, ln2_bias, post_gain, post_bias, b_o, b_fc2, b_fc1, b_q, b_v)
    e_all = encode(hidden_loc, weights, vectors)
    k_t, v_t, enc_loc = caches(e_all, w_ck.transpose(0, 2, 1), w_cv.transpose(0, 2, 1), b_cv)
    shape = (4, CLIPS, FRAMES, 3, HEAD_DIM)
    return enc_loc, k_t.transpose(0, 1, 3, 2).reshape(shape), v_t.transpose(0, 1, 3, 2).reshape(shape)


def solution(mesh):
    in_specs = (P("dp", "tp", None), P(), P(), P(None, "tp"), P("tp"), P(None, "tp"), P(None, "tp"), P("tp"), P("tp", None), P(), P(), P(), P(None, "tp"), P("tp"), P("tp", None), P(), P(), P(), P(None, None, "tp"), P(None, None, "tp"), P(None, "tp"))
    out_specs = (P("dp", "tp", None), P(None, "dp", None, "tp", None), P(None, "dp", None, "tp", None))
    return jax.shard_map(device_body, mesh=mesh, in_specs=in_specs, out_specs=out_specs, check_vma=False)
```

```python
import functools

import jax
import jax.numpy as jnp
from jax import lax
from jax.experimental import pallas as pl
from jax.experimental.pallas import tpu as pltpu
from jax.sharding import PartitionSpec as P

HEAD_DIM = 64
ATTN_SCALE = HEAD_DIM ** -0.25
LN_EPS = 1e-5
SQRT_HALF = 0.5 ** 0.5
MESH = pl.DeviceIdType.MESH
BF16, F32 = jnp.bfloat16, jnp.float32

CLIPS, FRAMES, WIDTH, HIDDEN = 16, 512, 768, 3072
LOC_FRAMES, LOC_COLS = FRAMES // 4, WIDTH // 4
WIDE = (slice(0, 512), slice(512, 768))
SHARED, ONLY = 4, 2
SLOTS = SHARED + ONLY
LAG = 4
FAR_TURNS = 3
LN_ROWS = 64
SEND_ORDER = ("q", "k", "v", 0, "o", 1, 2, "w1a", "w1b", 3, "w2a", "w2b", 4, 5)
RELAYS = {
    (0, 2): ((1, "o"),), (0, 5): ((2, "o"),),
    (2, 0): ((1, "w1a"),), (2, 5): ((1, "w1b"),),
    (3, 1): ((2, "w1a"),), (3, 3): ((2, "w1b"),), (3, 5): ((1, "w2a"),),
    (4, 0): ((1, "w2b"),), (4, 3): ((2, "w2a"),),
}
OUT_SLOTS, AHEAD = 6, 4

NT = (((1,), (1,)), ((), ()))
NN = (((1,), (0,)), ((), ()))
TN = (((0,), (0,)), ((), ()))


def dot(lhs, rhs, dims=NN):
    return lax.dot_general(lhs, rhs, dims, preferred_element_type=F32)


def norm_rows(values, gain, bias):
    centered = values.astype(F32)
    centered = centered - jnp.mean(centered, axis=-1, keepdims=True)
    row_var = jnp.mean(centered * centered, axis=-1, keepdims=True)
    return (centered * lax.rsqrt(row_var + LN_EPS) * gain + bias).astype(BF16)


def only_clip(chip, core, slot):
    return 2 * SHARED + (2 * chip + core) * ONLY + slot


def clip_of(chip, core, slot):
    return only_clip(chip, core, slot) if slot < ONLY else core * SHARED + slot - ONLY


def rows_of(ref, start, count):
    return ref.at[pl.ds(pl.multiple_of(start, 16), count), :]


def encoder_kernel(x_hbm, wq_hbm, wk_hbm, wv_hbm, wo_hbm, w1_hbm, w2_hbm,
                   g1_ref, s1_ref, g2_ref, s2_ref, g3_ref, s3_ref, bo_ref, b2_ref, b1_ref, bq_ref, bv_ref, e_hbm,
                   rep_ref, loc, b1_row, xbuf, wqv, wk, wo, w1, w2, small, abuf, qvbuf, ktbuf, obuf, mbuf, gbuf, acc, bias,
                   x_send, x_recv, x_loc, w_send, w_recv, w_loc, s_send, s_recv, e_send, e_recv, e_loc):
    group, tp = lax.axis_index("dp"), lax.axis_index("tp")
    chip, core = tp // 2, tp % 2
    other_chip, other_core = 1 - chip, 1 - core
    t_sib = 2 * chip + other_core
    t_far = 2 * other_chip + core
    t_diag = 2 * other_chip + other_core
    sib = {"dp": group, "tp": t_sib}
    far = {"dp": group, "tp": t_far}
    diag = {"dp": group, "tp": t_diag}
    side = {"dp": 1 - group, "tp": tp}

    def remote(src, dst, send, recv, device):
        return pltpu.make_async_remote_copy(src_ref=src, dst_ref=dst, send_sem=send, recv_sem=recv, device_id=device, device_id_type=MESH)

    def frames(slot, owner):
        return xbuf.at[slot, pl.ds(pl.multiple_of(owner * LOC_FRAMES, LOC_FRAMES), LOC_FRAMES), :]

    def x_copy(slot, link):
        device, there_chip, there_core = ((sib, chip, other_core), (far, other_chip, core), (diag, other_chip, other_core))[link]
        return remote(x_hbm.at[clip_of(there_chip, there_core, slot)], frames(slot, tp), x_send.at[slot, link], x_recv.at[slot, link], device)

    def x_local(slot):
        return pltpu.make_async_copy(x_hbm.at[clip_of(chip, core, slot)], frames(slot, tp), x_loc.at[slot])

    def x_wait(slot):
        pltpu.make_async_copy(x_hbm.at[0], frames(slot, tp), x_loc.at[slot]).wait()
        for link, owner in enumerate((t_sib, t_far, t_diag)):
            remote(x_hbm.at[0], frames(slot, owner), x_send.at[slot, link], x_recv.at[slot, link], sib).wait_recv()

    def at_rows(dst, base):
        shard = LOC_COLS if dst is not w2 else WIDTH
        return lambda owner, first, count: rows_of(dst, base + owner * shard + first, count)

    def at_columns(owner, first, count):
        return w1.at[pl.ds(pl.multiple_of(first, 16), count), pl.ds(pl.multiple_of(owner * WIDTH, WIDTH), WIDTH)]

    units = {
        "q": (0, wq_hbm, at_rows(wqv, 0), 0, 192), "k": (1, wk_hbm, at_rows(wk, 0), 0, 192),
        "v": (2, wv_hbm, at_rows(wqv, WIDTH), 0, 192), "o": (3, wo_hbm, at_rows(wo, 0), 0, 192),
        "w1a": (4, w1_hbm, at_columns, 0, 384), "w1b": (5, w1_hbm, at_columns, 384, 384),
        "w2a": (6, w2_hbm, at_rows(w2, 0), 0, 384), "w2b": (7, w2_hbm, at_rows(w2, 0), 384, 384),
    }

    def w_local(name):
        idx, src, place, first, count = units[name]
        return pltpu.make_async_copy(src.at[pl.ds(first, count), :], place(tp, first, count), w_loc.at[idx])

    def w_sib(name, owner):
        idx, src, place, first, count = units[name]
        return remote(src.at[pl.ds(first, count), :], place(owner, first, count), w_send.at[idx, 0], w_recv.at[idx, 0], sib)

    def w_far(name, owner):
        idx, src, place, first, count = units[name]
        half = count // 2
        return remote(rows_of(src, first + group * half, half), place(owner, first + group * half, half),
                      w_send.at[idx, 1], w_recv.at[idx, 1], far)

    def w_relay(name, owner, part, sem, recv, device):
        idx, src, place, first, count = units[name]
        half = count // 2
        piece = place(owner, first + part * half, half)
        return remote(piece, piece, w_send.at[idx, sem], w_recv.at[idx, recv], device)

    def w_start(name):
        w_far(name, tp).start()
        w_local(name).start()
        w_sib(name, tp).start()

    def w_stage1(name):
        w_far(name, t_far).wait_recv()
        w_relay(name, t_far, group, 3, 2, side).start()
        w_relay(name, t_far, group, 2, 3, sib).start()

    def w_stage2(name):
        w_relay(name, t_far, 1 - group, 3, 2, side).wait_recv()
        w_relay(name, t_far, 1 - group, 4, 4, sib).start()

    def w_wait_near(name):
        w_local(name).wait()
        w_sib(name, t_sib).wait_recv()

    def w_wait_far(name):
        w_relay(name, t_diag, group, 2, 3, sib).wait_recv()
        w_relay(name, t_diag, 1 - group, 4, 4, sib).wait_recv()

    def w_drain(name):
        w_sib(name, tp).wait_send()
        w_far(name, tp).wait_send()
        w_relay(name, t_far, group, 3, 2, side).wait_send()
        w_relay(name, t_far, group, 2, 3, sib).wait_send()
        w_relay(name, t_far, 1 - group, 4, 4, sib).wait_send()

    def s_copy(link, owner):
        device = (sib, far, diag)[link]
        return remote(loc, small.at[owner], s_send.at[link], s_recv.at[link], device)

    def e_local(slot, clip):
        return pltpu.make_async_copy(xbuf.at[slot], e_hbm.at[clip], e_loc.at[slot])

    def e_sib(slot, clip):
        return remote(xbuf.at[slot], e_hbm.at[clip], e_send.at[slot], e_recv.at[slot], sib)

    def e_far(slot, clip):
        return remote(xbuf.at[slot], e_hbm.at[clip], e_send.at[SLOTS + slot], e_recv.at[SLOTS + slot], far)

    def e_relay(slot, clip):
        sem = SLOTS + ONLY + slot
        return remote(e_hbm.at[clip], e_hbm.at[clip], e_send.at[sem], e_recv.at[sem], sib)

    barrier = pltpu.get_barrier_semaphore()
    for device in (sib, far, diag, side):
        pl.semaphore_signal(barrier, inc=1, device_id=device, device_id_type=MESH)

    for row, ref in enumerate((g1_ref, s1_ref, g2_ref, s2_ref, g3_ref, s3_ref, bo_ref, b2_ref)):
        rep_ref[row:row + 1, :] = ref[...].astype(F32).reshape(1, WIDTH)
    place = lax.broadcasted_iota(jnp.int32, (192, WIDTH), 0) + tp * 192 == lax.broadcasted_iota(jnp.int32, (192, WIDTH), 1)
    place = place.astype(F32).astype(BF16)
    loc[0:1, :] = b1_ref[...].astype(F32).reshape(1, WIDTH)
    for row, ref in ((1, bq_ref), (2, bv_ref)):
        vector = jnp.broadcast_to(ref[...].astype(F32).reshape(1, 192), (16, 192)).astype(BF16)
        loc[row:row + 1, :] = dot(vector, place)[0:1, :]
    loc[3:8, :] = jnp.zeros((5, WIDTH), F32)
    small[tp] = loc[...]

    pl.semaphore_wait(barrier, 4)

    for link in (1, 2, 0):
        s_copy(link, tp).start()
    for item in SEND_ORDER:
        if isinstance(item, str):
            w_start(item)
        else:
            x_copy(item, 1).start()
            x_copy(item, 2).start()
            x_local(item).start()
            x_copy(item, 0).start()

    w_stage1("q")
    w_stage1("k")
    w_stage2("q")
    w_stage1("v")
    w_stage2("k")
    for link, owner in enumerate((t_sib, t_far, t_diag)):
        s_copy(link, owner).wait_recv()
    bias[0:1, 0:WIDTH] = small[0, 1:2, :] + small[1, 1:2, :] + small[2, 1:2, :] + small[3, 1:2, :]
    bias[0:1, WIDTH:2 * WIDTH] = small[0, 2:3, :] + small[1, 2:3, :] + small[2, 2:3, :] + small[3, 2:3, :]
    for owner in range(4):
        b1_row[0:1, owner * WIDTH:owner * WIDTH + WIDTH] = small[owner, 0:1, :]
    w_stage2("v")
    for name in ("q", "k", "v"):
        w_wait_near(name)
        w_wait_far(name)

    def rep(row):
        return rep_ref[row:row + 1, :]

    def norm_into(dst_store, src_load, gain, shift):
        for first in range(0, FRAMES, LN_ROWS):
            dst_store(first, norm_rows(src_load(first), gain, shift))

    def attention(slot, step):
        x_wait(slot)

        def put_a(first, value):
            abuf[first:first + LN_ROWS, :] = value

        norm_into(put_a, lambda first: xbuf[slot, pl.ds(first, LN_ROWS), :], rep(0), rep(1))
        scale = jnp.where(lax.broadcasted_iota(jnp.int32, (1, 2 * WIDTH), 1) < WIDTH, ATTN_SCALE, 1.0)
        ktbuf[...] = (dot(wk[...], abuf[...], NT) * ATTN_SCALE).astype(BF16)
        for col in range(0, 2 * WIDTH, 512):
            cols = slice(col, col + 512)
            qvbuf[:, cols] = ((dot(abuf[...], wqv[cols, :], NT) + bias[0:1, cols]) * scale[:, cols]).astype(BF16)

        lane = lax.broadcasted_iota(jnp.int32, (1, 128), 1)
        keep = [(lane < 64).astype(F32).astype(BF16), (lane >= 64).astype(F32).astype(BF16)]

        def pair_body(pair, _):
            for (when, where), todo in RELAYS.items():
                @pl.when((step == when) & (pair == where))
                def _():
                    for stage, name in todo:
                        (w_stage1 if stage == 1 else w_stage2)(name)

            cols = pl.ds(pl.multiple_of(pair * 128, 128), 128)
            keys_t = ktbuf[cols, :]
            values = qvbuf[:, pl.ds(pl.multiple_of(WIDTH + pair * 128, 128), 128)]

            def scores_of(head):
                return dot(qvbuf[:, cols] * keep[head], keys_t)

            scores = scores_of(0)
            outs = []
            for head in range(2):
                ahead = scores_of(1) if head == 0 else None
                top = jnp.max(scores, axis=-1, keepdims=True)
                weight = jnp.exp(scores - top)
                total = jnp.sum(weight, axis=-1, keepdims=True)
                outs.append(dot(weight.astype(BF16), values) * (1.0 / total))
                scores = ahead
            obuf[:, cols] = jnp.where(lane < 64, outs[0], outs[1]).astype(BF16)
            return 0

        lax.fori_loop(0, 6, pair_body, 0)

        @pl.when(step == 0)
        def _():
            w_wait_near("o")
            w_wait_far("o")

        for cols in WIDE:
            branch = (dot(obuf[...], wo[:, cols]) + rep_ref[6:7, cols]).astype(BF16)
            xbuf[slot, :, cols] = (xbuf[slot, :, cols].astype(F32) + branch.astype(F32)).astype(BF16)

        def put_m(first, value):
            mbuf[slot, pl.ds(first, LN_ROWS), :] = value

        norm_into(put_m, lambda first: xbuf[slot, pl.ds(first, LN_ROWS), :], rep(2), rep(3))

    def hidden_half(slot, which):
        def product(col):
            return dot(mbuf[slot], w1[:, pl.ds(pl.multiple_of(which * 1536 + col, 512), 512)])

        ahead = product(0)
        for col in range(0, 1536, 512):
            inner = ahead + b1_row[0:1, pl.ds(pl.multiple_of(which * 1536 + col, 512), 512)]
            if col + 512 < 1536:
                ahead = product(col + 512)
            gbuf[:, col:col + 512] = (0.5 * inner * (1.0 + lax.erf(inner * SQRT_HALF))).astype(BF16)

    def second_product(which, cols):
        return dot(gbuf[...], w2[pl.ds(pl.multiple_of(which * 1536, 1536), 1536), cols])

    def mlp_near(slot):
        hidden_half(slot, chip)
        for cols in WIDE:
            acc[slot, :, cols] = second_product(chip, cols)

    def mlp_far(slot):
        hidden_half(slot, other_chip)
        for cols in WIDE:
            branch = (acc[slot, :, cols] + second_product(other_chip, cols) + rep_ref[7:8, cols]).astype(BF16)
            xbuf[slot, :, cols] = (xbuf[slot, :, cols].astype(F32) + branch.astype(F32)).astype(BF16)

        def put_e(first, value):
            xbuf[slot, pl.ds(first, LN_ROWS), :] = value

        norm_into(put_e, lambda first: xbuf[slot, pl.ds(first, LN_ROWS), :], rep(4), rep(5))

        @pl.when(slot < ONLY)
        def _():
            clip = only_clip(chip, core, slot)
            e_far(slot, clip).start()
            e_local(slot, clip).start()
            e_sib(slot, clip).start()

        @pl.when(slot >= ONLY)
        def _():
            clip = core * SHARED + slot - ONLY
            e_local(slot, clip).start()
            e_sib(slot, clip).start()

    mlp_units = ("w1a", "w1b", "w2a", "w2b")

    def step_body(step, _):
        attention(step, step)

        @pl.when(step == 0)
        def _():
            for name in mlp_units:
                w_wait_near(name)

        mlp_near(step)

        @pl.when(step == LAG)
        def _():
            w_stage2("w2b")
            for name in mlp_units:
                w_wait_far(name)

        @pl.when(step >= LAG)
        def _():
            def far_body(turn, _):
                mlp_far(FAR_TURNS * (step - LAG) + turn)
                return 0

            lax.fori_loop(0, FAR_TURNS, far_body, 0)

        return 0

    lax.fori_loop(0, SLOTS, step_body, 0)

    for slot in range(ONLY):
        clip = only_clip(other_chip, core, slot)
        e_far(slot, clip).wait_recv()
        e_relay(slot, clip).start()
    for slot in range(SLOTS):
        clip = clip_of(chip, core, slot)
        e_local(slot, clip).wait()
        e_sib(slot, clip).wait_send()
        e_sib(slot, clip_of(chip, other_core, slot)).wait_recv()
    for slot in range(ONLY):
        e_far(slot, only_clip(chip, core, slot)).wait_send()
        e_relay(slot, only_clip(other_chip, core, slot)).wait_send()
        e_relay(slot, only_clip(other_chip, other_core, slot)).wait_recv()
    for slot in range(SLOTS):
        for link in range(3):
            x_copy(slot, link).wait_send()
    for name in units:
        w_drain(name)
    for link in range(3):
        s_copy(link, tp).wait_send()


def encode(x, weights, vectors):
    dma = pltpu.SemaphoreType.DMA
    any_spec = pl.BlockSpec(memory_space=pl.ANY)
    return pl.pallas_call(
        encoder_kernel,
        out_shape=jax.ShapeDtypeStruct((CLIPS, FRAMES, WIDTH), BF16),
        in_specs=[any_spec] * 7 + [pl.BlockSpec(memory_space=pltpu.VMEM)] * 11,
        out_specs=any_spec,
        scratch_shapes=[
            pltpu.VMEM((8, WIDTH), F32), pltpu.VMEM((8, WIDTH), F32), pltpu.VMEM((8, HIDDEN), F32),
            pltpu.VMEM((SLOTS, FRAMES, WIDTH), BF16),
            pltpu.VMEM((2 * WIDTH, WIDTH), BF16), pltpu.VMEM((WIDTH, WIDTH), BF16), pltpu.VMEM((WIDTH, WIDTH), BF16),
            pltpu.VMEM((WIDTH, HIDDEN), BF16), pltpu.VMEM((HIDDEN, WIDTH), BF16),
            pltpu.VMEM((4, 8, WIDTH), F32),
            pltpu.VMEM((FRAMES, WIDTH), BF16), pltpu.VMEM((FRAMES, 2 * WIDTH), BF16), pltpu.VMEM((WIDTH, FRAMES), BF16),
            pltpu.VMEM((FRAMES, WIDTH), BF16),
            pltpu.VMEM((SLOTS, FRAMES, WIDTH), BF16),
            pltpu.VMEM((FRAMES, 2 * WIDTH), BF16),
            pltpu.VMEM((SLOTS, FRAMES, WIDTH), F32),
            pltpu.VMEM((8, 2 * WIDTH), F32),
            dma((SLOTS, 3)), dma((SLOTS, 3)), dma((SLOTS,)),
            dma((8, 5)), dma((8, 5)), dma((8,)),
            dma((3,)), dma((3,)),
            dma((SLOTS + 2 * ONLY,)), dma((SLOTS + 2 * ONLY,)), dma((SLOTS,)),
        ],
        compiler_params=pltpu.CompilerParams(collective_id=0, has_side_effects=True, vmem_limit_bytes=64 * 1024 * 1024 - 128 * 1024),
        name="encoder",
    )(x, *weights, *vectors)


def cache_kernel(e_hbm, wk_hbm, wv_hbm, bias_ref, k_hbm, v_hbm, enc_hbm, weights, shift, ebuf, obuf, w_sem, e_sem, out_sem, enc_sem):
    tp = lax.axis_index("tp")

    def load(clip):
        return pltpu.make_async_copy(e_hbm.at[clip], ebuf.at[clip], e_sem.at[clip])

    def stores(clip, slot):
        copies = []
        for which, dst in enumerate((k_hbm, v_hbm)):
            for layer in range(4):
                rows = pl.ds(which * WIDTH + layer * LOC_COLS, LOC_COLS)
                copies.append(pltpu.make_async_copy(obuf.at[slot, rows, :], dst.at[layer, clip], out_sem.at[slot, which * 4 + layer]))
        return copies

    def enc_store(clip):
        own = pl.ds(pl.multiple_of(tp * LOC_FRAMES, LOC_FRAMES), LOC_FRAMES)
        return pltpu.make_async_copy(ebuf.at[clip, own, :], enc_hbm.at[clip], enc_sem.at[clip])

    load(0).start()
    weight_loads = [pltpu.make_async_copy(src.at[layer], weights.at[pl.ds(which * WIDTH + layer * LOC_COLS, LOC_COLS), :], w_sem.at[which, layer])
                    for which, src in enumerate((wk_hbm, wv_hbm)) for layer in range(4)]
    for copy in weight_loads:
        copy.start()
    for clip in range(1, AHEAD):
        load(clip).start()
    rows = jnp.concatenate([bias_ref[...].astype(F32), jnp.zeros((4, LOC_COLS), F32)], axis=0)
    for layer in range(4):
        pick = (lax.broadcasted_iota(jnp.int32, (8, 128), 0) == layer).astype(F32)
        shift[layer * LOC_COLS:(layer + 1) * LOC_COLS, :] = dot(rows, pick, TN)
    for copy in weight_loads:
        copy.wait()

    def body(step, _):
        for half in range(2):
            clip = 2 * step + half
            slot = clip % OUT_SLOTS
            load(clip).wait()
            enc_store(clip).start()

            @pl.when(clip + AHEAD < CLIPS)
            def _():
                load(clip + AHEAD).start()

            @pl.when(clip >= OUT_SLOTS)
            def _():
                for copy in stores(clip - OUT_SLOTS, slot):
                    copy.wait()

        for half in range(2):
            clip = 2 * step + half
            slot = clip % OUT_SLOTS
            obuf[slot, 0:WIDTH, :] = dot(weights[0:WIDTH, :], ebuf[clip], NT).astype(BF16)
            obuf[slot, WIDTH:2 * WIDTH, :] = (dot(weights[WIDTH:2 * WIDTH, :], ebuf[clip], NT) + jnp.concatenate([shift[...]] * 4, axis=1)).astype(BF16)
        for half in range(2):
            clip = 2 * step + half
            for copy in stores(clip, clip % OUT_SLOTS):
                copy.start()
        return 0

    lax.fori_loop(0, CLIPS // 2, body, 0)
    for clip in range(CLIPS - OUT_SLOTS, CLIPS):
        for copy in stores(clip, clip % OUT_SLOTS):
            copy.wait()
    for clip in range(CLIPS):
        enc_store(clip).wait()


def caches(e_all, wck_t, wcv_t, bias):
    cache = jax.ShapeDtypeStruct((4, CLIPS, LOC_COLS, FRAMES), BF16)
    any_spec = pl.BlockSpec(memory_space=pl.ANY)
    dma = pltpu.SemaphoreType.DMA
    return pl.pallas_call(
        cache_kernel,
        out_shape=(cache, cache, jax.ShapeDtypeStruct((CLIPS, LOC_FRAMES, WIDTH), BF16)),
        in_specs=[any_spec, any_spec, any_spec, pl.BlockSpec(memory_space=pltpu.VMEM)],
        out_specs=(any_spec, any_spec, any_spec),
        scratch_shapes=[
            pltpu.VMEM((2 * WIDTH, WIDTH), BF16), pltpu.VMEM((WIDTH, 128), F32),
            pltpu.VMEM((CLIPS, FRAMES, WIDTH), BF16), pltpu.VMEM((OUT_SLOTS, 2 * WIDTH, FRAMES), BF16),
            dma((2, 4)), dma((CLIPS,)), dma((OUT_SLOTS, 8)), dma((CLIPS,)),
        ],
        compiler_params=pltpu.CompilerParams(vmem_limit_bytes=64 * 1024 * 1024 - 128 * 1024),
        name="caches",
    )(e_all, wck_t, wcv_t, bias)


def device_body(hidden_loc, ln1_gain, ln1_bias, w_q, b_q, w_k, w_v, b_v, w_o, b_o, ln2_gain, ln2_bias, w_fc1, b_fc1, w_fc2, b_fc2, post_gain, post_bias, w_ck, w_cv, b_cv):
    weights = (w_q.T, w_k.T, w_v.T, w_o, w_fc1, w_fc2)
    vectors = (ln1_gain, ln1_bias, ln2_gain, ln2_bias, post_gain, post_bias, b_o, b_fc2, b_fc1, b_q, b_v)
    e_all = encode(hidden_loc, weights, vectors)
    k_t, v_t, enc_loc = caches(e_all, w_ck.transpose(0, 2, 1), w_cv.transpose(0, 2, 1), b_cv)
    shape = (4, CLIPS, FRAMES, 3, HEAD_DIM)
    return enc_loc, k_t.transpose(0, 1, 3, 2).reshape(shape), v_t.transpose(0, 1, 3, 2).reshape(shape)


def solution(mesh):
    in_specs = (P("dp", "tp", None), P(), P(), P(None, "tp"), P("tp"), P(None, "tp"), P(None, "tp"), P("tp"), P("tp", None), P(), P(), P(), P(None, "tp"), P("tp"), P("tp", None), P(), P(), P(), P(None, None, "tp"), P(None, None, "tp"), P(None, "tp"))
    out_specs = (P("dp", "tp", None), P(None, "dp", None, "tp", None), P(None, "dp", None, "tp", None))
    return jax.shard_map(device_body, mesh=mesh, in_specs=in_specs, out_specs=out_specs, check_vma=False)
```

```python
import functools

import jax
import jax.numpy as jnp
from jax import lax
from jax.experimental import pallas as pl
from jax.experimental.pallas import tpu as pltpu
from jax.sharding import PartitionSpec as P

HEAD_DIM = 64
ATTN_SCALE = HEAD_DIM ** -0.25
LN_EPS = 1e-5
SQRT_HALF = 0.5 ** 0.5
MESH = pl.DeviceIdType.MESH
BF16, F32 = jnp.bfloat16, jnp.float32

CLIPS, FRAMES, WIDTH, HIDDEN = 16, 512, 768, 3072
LOC_FRAMES, LOC_COLS = FRAMES // 4, WIDTH // 4
WIDE = (slice(0, 512), slice(512, 768))
SHARED, ONLY = 4, 2
SLOTS = SHARED + ONLY
OTHERS = CLIPS - SLOTS
LAG = 4
FAR_TURNS = 3
LN_ROWS = 64
SEND_ORDER = ("q", "k", "v", 0, "o", 1, 2, "w1a", "w1b", 3, "w2a", "w2b", 4, 5)
RELAYS = {
    (0, 2): ((1, "o"),), (0, 5): ((2, "o"),),
    (2, 0): ((1, "w1a"),), (2, 5): ((1, "w1b"),),
    (3, 1): ((2, "w1a"),), (3, 3): ((2, "w1b"),), (3, 5): ((1, "w2a"),),
    (4, 0): ((1, "w2b"),), (4, 3): ((2, "w2a"),),
}
OUT_SLOTS, AHEAD = 6, 4

NT = (((1,), (1,)), ((), ()))
NN = (((1,), (0,)), ((), ()))
TN = (((0,), (0,)), ((), ()))


def dot(lhs, rhs, dims=NN):
    return lax.dot_general(lhs, rhs, dims, preferred_element_type=F32)


def norm_rows(values, gain, bias):
    centered = values.astype(F32)
    centered = centered - jnp.mean(centered, axis=-1, keepdims=True)
    row_var = jnp.mean(centered * centered, axis=-1, keepdims=True)
    return (centered * lax.rsqrt(row_var + LN_EPS) * gain + bias).astype(BF16)


def only_clip(chip, core, slot):
    return 2 * SHARED + (2 * chip + core) * ONLY + slot


def clip_of(chip, core, slot):
    return only_clip(chip, core, slot) if slot < ONLY else core * SHARED + slot - ONLY


def rows_of(ref, start, count):
    return ref.at[pl.ds(pl.multiple_of(start, 16), count), :]


def cache_weight_loads(wk_hbm, wv_hbm, dst, sems):
    return [pltpu.make_async_copy(src.at[layer], dst.at[pl.ds(which * WIDTH + layer * LOC_COLS, LOC_COLS), :], sems.at[which, layer])
            for which, src in enumerate((wk_hbm, wv_hbm)) for layer in range(4)]


def lay_out_shift(bias_ref, shift):
    rows = jnp.concatenate([bias_ref[...].astype(F32), jnp.zeros((4, LOC_COLS), F32)], axis=0)
    for layer in range(4):
        pick = (lax.broadcasted_iota(jnp.int32, (8, 128), 0) == layer).astype(F32)
        shift[layer * LOC_COLS:(layer + 1) * LOC_COLS, :] = dot(rows, pick, TN)


def cache_products(dst, slot, weights, shift, clips, clip):
    dst[slot, 0:WIDTH, :] = dot(weights[0:WIDTH, :], clips[clip], NT).astype(BF16)
    dst[slot, WIDTH:2 * WIDTH, :] = (dot(weights[WIDTH:2 * WIDTH, :], clips[clip], NT) + jnp.concatenate([shift[...]] * 4, axis=1)).astype(BF16)


def encoder_kernel(x_hbm, wq_hbm, wk_hbm, wv_hbm, wo_hbm, w1_hbm, w2_hbm,
                   g1_ref, s1_ref, g2_ref, s2_ref, g3_ref, s3_ref, bo_ref, b2_ref, b1_ref, bq_ref, bv_ref, wck_hbm, wcv_hbm, bcv_ref, e_hbm, part_hbm,
                   rep_ref, loc, b1_row, xbuf, wqv, wk, wo, w1, w2, small, abuf, qvbuf, ktbuf, obuf, mbuf, gbuf, acc, bias, cw, shift, cbuf,
                   x_send, x_recv, x_loc, w_send, w_recv, w_loc, s_send, s_recv, e_send, e_recv, e_loc, cw_sem, c_sem):
    group, tp = lax.axis_index("dp"), lax.axis_index("tp")
    chip, core = tp // 2, tp % 2
    other_chip, other_core = 1 - chip, 1 - core
    t_sib = 2 * chip + other_core
    t_far = 2 * other_chip + core
    t_diag = 2 * other_chip + other_core
    sib = {"dp": group, "tp": t_sib}
    far = {"dp": group, "tp": t_far}
    diag = {"dp": group, "tp": t_diag}
    side = {"dp": 1 - group, "tp": tp}

    def remote(src, dst, send, recv, device):
        return pltpu.make_async_remote_copy(src_ref=src, dst_ref=dst, send_sem=send, recv_sem=recv, device_id=device, device_id_type=MESH)

    def frames(slot, owner):
        return xbuf.at[slot, pl.ds(pl.multiple_of(owner * LOC_FRAMES, LOC_FRAMES), LOC_FRAMES), :]

    def x_copy(slot, link):
        device, there_chip, there_core = ((sib, chip, other_core), (far, other_chip, core), (diag, other_chip, other_core))[link]
        return remote(x_hbm.at[clip_of(there_chip, there_core, slot)], frames(slot, tp), x_send.at[slot, link], x_recv.at[slot, link], device)

    def x_local(slot):
        return pltpu.make_async_copy(x_hbm.at[clip_of(chip, core, slot)], frames(slot, tp), x_loc.at[slot])

    def x_wait(slot):
        pltpu.make_async_copy(x_hbm.at[0], frames(slot, tp), x_loc.at[slot]).wait()
        for link, owner in enumerate((t_sib, t_far, t_diag)):
            remote(x_hbm.at[0], frames(slot, owner), x_send.at[slot, link], x_recv.at[slot, link], sib).wait_recv()

    def at_rows(dst, base):
        shard = LOC_COLS if dst is not w2 else WIDTH
        return lambda owner, first, count: rows_of(dst, base + owner * shard + first, count)

    def at_columns(owner, first, count):
        return w1.at[pl.ds(pl.multiple_of(first, 16), count), pl.ds(pl.multiple_of(owner * WIDTH, WIDTH), WIDTH)]

    units = {
        "q": (0, wq_hbm, at_rows(wqv, 0), 0, 192), "k": (1, wk_hbm, at_rows(wk, 0), 0, 192),
        "v": (2, wv_hbm, at_rows(wqv, WIDTH), 0, 192), "o": (3, wo_hbm, at_rows(wo, 0), 0, 192),
        "w1a": (4, w1_hbm, at_columns, 0, 384), "w1b": (5, w1_hbm, at_columns, 384, 384),
        "w2a": (6, w2_hbm, at_rows(w2, 0), 0, 384), "w2b": (7, w2_hbm, at_rows(w2, 0), 384, 384),
    }

    def w_local(name):
        idx, src, place, first, count = units[name]
        return pltpu.make_async_copy(src.at[pl.ds(first, count), :], place(tp, first, count), w_loc.at[idx])

    def w_sib(name, owner):
        idx, src, place, first, count = units[name]
        return remote(src.at[pl.ds(first, count), :], place(owner, first, count), w_send.at[idx, 0], w_recv.at[idx, 0], sib)

    def w_far(name, owner):
        idx, src, place, first, count = units[name]
        half = count // 2
        return remote(rows_of(src, first + group * half, half), place(owner, first + group * half, half),
                      w_send.at[idx, 1], w_recv.at[idx, 1], far)

    def w_relay(name, owner, part, sem, recv, device):
        idx, src, place, first, count = units[name]
        half = count // 2
        piece = place(owner, first + part * half, half)
        return remote(piece, piece, w_send.at[idx, sem], w_recv.at[idx, recv], device)

    def w_start(name):
        w_far(name, tp).start()
        w_local(name).start()
        w_sib(name, tp).start()

    def w_stage1(name):
        w_far(name, t_far).wait_recv()
        w_relay(name, t_far, group, 3, 2, side).start()
        w_relay(name, t_far, group, 2, 3, sib).start()

    def w_stage2(name):
        w_relay(name, t_far, 1 - group, 3, 2, side).wait_recv()
        w_relay(name, t_far, 1 - group, 4, 4, sib).start()

    def w_wait_near(name):
        w_local(name).wait()
        w_sib(name, t_sib).wait_recv()

    def w_wait_far(name):
        w_relay(name, t_diag, group, 2, 3, sib).wait_recv()
        w_relay(name, t_diag, 1 - group, 4, 4, sib).wait_recv()

    def w_drain(name):
        w_sib(name, tp).wait_send()
        w_far(name, tp).wait_send()
        w_relay(name, t_far, group, 3, 2, side).wait_send()
        w_relay(name, t_far, group, 2, 3, sib).wait_send()
        w_relay(name, t_far, 1 - group, 4, 4, sib).wait_send()

    def s_copy(link, owner):
        device = (sib, far, diag)[link]
        return remote(loc, small.at[owner], s_send.at[link], s_recv.at[link], device)

    def e_local(slot, clip):
        return pltpu.make_async_copy(xbuf.at[slot], e_hbm.at[clip], e_loc.at[slot])

    def e_sib(slot, clip):
        return remote(xbuf.at[slot], e_hbm.at[clip], e_send.at[slot], e_recv.at[slot], sib)

    def e_far(slot, clip):
        return remote(xbuf.at[slot], e_hbm.at[clip], e_send.at[SLOTS + slot], e_recv.at[SLOTS + slot], far)

    def e_relay(slot, clip):
        sem = SLOTS + ONLY + slot
        return remote(e_hbm.at[clip], e_hbm.at[clip], e_send.at[sem], e_recv.at[sem], sib)

    barrier = pltpu.get_barrier_semaphore()
    for device in (sib, far, diag, side):
        pl.semaphore_signal(barrier, inc=1, device_id=device, device_id_type=MESH)

    for row, ref in enumerate((g1_ref, s1_ref, g2_ref, s2_ref, g3_ref, s3_ref, bo_ref, b2_ref)):
        rep_ref[row:row + 1, :] = ref[...].astype(F32).reshape(1, WIDTH)
    place = lax.broadcasted_iota(jnp.int32, (192, WIDTH), 0) + tp * 192 == lax.broadcasted_iota(jnp.int32, (192, WIDTH), 1)
    place = place.astype(F32).astype(BF16)
    loc[0:1, :] = b1_ref[...].astype(F32).reshape(1, WIDTH)
    for row, ref in ((1, bq_ref), (2, bv_ref)):
        vector = jnp.broadcast_to(ref[...].astype(F32).reshape(1, 192), (16, 192)).astype(BF16)
        loc[row:row + 1, :] = dot(vector, place)[0:1, :]
    loc[3:8, :] = jnp.zeros((5, WIDTH), F32)
    small[tp] = loc[...]

    pl.semaphore_wait(barrier, 4)

    for link in (1, 2, 0):
        s_copy(link, tp).start()
    for item in SEND_ORDER:
        if isinstance(item, str):
            w_start(item)
        else:
            x_copy(item, 1).start()
            x_copy(item, 2).start()
            x_local(item).start()
            x_copy(item, 0).start()

    cache_loads = cache_weight_loads(wck_hbm, wcv_hbm, cw, cw_sem)
    for copy in cache_loads:
        copy.start()
    lay_out_shift(bcv_ref, shift)

    w_stage1("q")
    w_stage1("k")
    w_stage2("q")
    w_stage1("v")
    w_stage2("k")
    for link, owner in enumerate((t_sib, t_far, t_diag)):
        s_copy(link, owner).wait_recv()
    bias[0:1, 0:WIDTH] = small[0, 1:2, :] + small[1, 1:2, :] + small[2, 1:2, :] + small[3, 1:2, :]
    bias[0:1, WIDTH:2 * WIDTH] = small[0, 2:3, :] + small[1, 2:3, :] + small[2, 2:3, :] + small[3, 2:3, :]
    for owner in range(4):
        b1_row[0:1, owner * WIDTH:owner * WIDTH + WIDTH] = small[owner, 0:1, :]
    w_stage2("v")
    for name in ("q", "k", "v"):
        w_wait_near(name)
        w_wait_far(name)

    def rep(row):
        return rep_ref[row:row + 1, :]

    def norm_into(dst_store, src_load, gain, shift):
        for first in range(0, FRAMES, LN_ROWS):
            dst_store(first, norm_rows(src_load(first), gain, shift))

    def attention(slot, step):
        x_wait(slot)

        def put_a(first, value):
            abuf[first:first + LN_ROWS, :] = value

        norm_into(put_a, lambda first: xbuf[slot, pl.ds(first, LN_ROWS), :], rep(0), rep(1))
        scale = jnp.where(lax.broadcasted_iota(jnp.int32, (1, 2 * WIDTH), 1) < WIDTH, ATTN_SCALE, 1.0)
        ktbuf[...] = (dot(wk[...], abuf[...], NT) * ATTN_SCALE).astype(BF16)
        for col in range(0, 2 * WIDTH, 512):
            cols = slice(col, col + 512)
            qvbuf[:, cols] = ((dot(abuf[...], wqv[cols, :], NT) + bias[0:1, cols]) * scale[:, cols]).astype(BF16)

        lane = lax.broadcasted_iota(jnp.int32, (1, 128), 1)
        keep = [(lane < 64).astype(F32).astype(BF16), (lane >= 64).astype(F32).astype(BF16)]

        def pair_body(pair, _):
            for (when, where), todo in RELAYS.items():
                @pl.when((step == when) & (pair == where))
                def _():
                    for stage, name in todo:
                        (w_stage1 if stage == 1 else w_stage2)(name)

            cols = pl.ds(pl.multiple_of(pair * 128, 128), 128)
            keys_t = ktbuf[cols, :]
            values = qvbuf[:, pl.ds(pl.multiple_of(WIDTH + pair * 128, 128), 128)]

            def scores_of(head):
                return dot(qvbuf[:, cols] * keep[head], keys_t)

            scores = scores_of(0)
            outs = []
            for head in range(2):
                ahead = scores_of(1) if head == 0 else None
                top = jnp.max(scores, axis=-1, keepdims=True)
                weight = jnp.exp(scores - top)
                total = jnp.sum(weight, axis=-1, keepdims=True)
                outs.append(dot(weight.astype(BF16), values) * (1.0 / total))
                scores = ahead
            obuf[:, cols] = jnp.where(lane < 64, outs[0], outs[1]).astype(BF16)
            return 0

        lax.fori_loop(0, 6, pair_body, 0)

        @pl.when(step == 0)
        def _():
            w_wait_near("o")
            w_wait_far("o")

        for cols in WIDE:
            branch = (dot(obuf[...], wo[:, cols]) + rep_ref[6:7, cols]).astype(BF16)
            xbuf[slot, :, cols] = (xbuf[slot, :, cols].astype(F32) + branch.astype(F32)).astype(BF16)

        def put_m(first, value):
            mbuf[slot, pl.ds(first, LN_ROWS), :] = value

        norm_into(put_m, lambda first: xbuf[slot, pl.ds(first, LN_ROWS), :], rep(2), rep(3))

    def hidden_half(slot, which):
        def product(col):
            return dot(mbuf[slot], w1[:, pl.ds(pl.multiple_of(which * 1536 + col, 512), 512)])

        ahead = product(0)
        for col in range(0, 1536, 512):
            inner = ahead + b1_row[0:1, pl.ds(pl.multiple_of(which * 1536 + col, 512), 512)]
            if col + 512 < 1536:
                ahead = product(col + 512)
            gbuf[:, col:col + 512] = (0.5 * inner * (1.0 + lax.erf(inner * SQRT_HALF))).astype(BF16)

    def second_product(which, cols):
        return dot(gbuf[...], w2[pl.ds(pl.multiple_of(which * 1536, 1536), 1536), cols])

    def mlp_near(slot):
        hidden_half(slot, chip)
        for cols in WIDE:
            acc[slot, :, cols] = second_product(chip, cols)

    def mlp_far(slot):
        hidden_half(slot, other_chip)
        for cols in WIDE:
            branch = (acc[slot, :, cols] + second_product(other_chip, cols) + rep_ref[7:8, cols]).astype(BF16)
            xbuf[slot, :, cols] = (xbuf[slot, :, cols].astype(F32) + branch.astype(F32)).astype(BF16)

        def put_e(first, value):
            xbuf[slot, pl.ds(first, LN_ROWS), :] = value

        norm_into(put_e, lambda first: xbuf[slot, pl.ds(first, LN_ROWS), :], rep(4), rep(5))

        @pl.when(slot < ONLY)
        def _():
            clip = only_clip(chip, core, slot)
            e_far(slot, clip).start()
            e_local(slot, clip).start()
            e_sib(slot, clip).start()

        @pl.when(slot >= ONLY)
        def _():
            clip = core * SHARED + slot - ONLY
            e_local(slot, clip).start()
            e_sib(slot, clip).start()

    mlp_units = ("w1a", "w1b", "w2a", "w2b")

    def step_body(step, _):
        attention(step, step)

        @pl.when(step == 0)
        def _():
            for name in mlp_units:
                w_wait_near(name)

        mlp_near(step)

        @pl.when(step == LAG)
        def _():
            w_stage2("w2b")
            for name in mlp_units:
                w_wait_far(name)

        @pl.when(step >= LAG)
        def _():
            def far_body(turn, _):
                mlp_far(FAR_TURNS * (step - LAG) + turn)
                return 0

            lax.fori_loop(0, FAR_TURNS, far_body, 0)

        return 0

    lax.fori_loop(0, SLOTS, step_body, 0)

    for copy in cache_loads:
        copy.wait()

    def c_store(slot):
        return pltpu.make_async_copy(cbuf.at[slot % 2], part_hbm.at[slot], c_sem.at[slot % 2])

    def cache_body(slot, _):
        @pl.when(slot >= 2)
        def _():
            c_store(slot - 2).wait()

        cache_products(cbuf, slot % 2, cw, shift, xbuf, slot)
        c_store(slot).start()
        return 0

    lax.fori_loop(0, SLOTS, cache_body, 0)
    for slot in range(SLOTS - 2, SLOTS):
        c_store(slot).wait()

    for slot in range(ONLY):
        clip = only_clip(other_chip, core, slot)
        e_far(slot, clip).wait_recv()
        e_relay(slot, clip).start()
    for slot in range(SLOTS):
        clip = clip_of(chip, core, slot)
        e_local(slot, clip).wait()
        e_sib(slot, clip).wait_send()
        e_sib(slot, clip_of(chip, other_core, slot)).wait_recv()
    for slot in range(ONLY):
        e_far(slot, only_clip(chip, core, slot)).wait_send()
        e_relay(slot, only_clip(other_chip, core, slot)).wait_send()
        e_relay(slot, only_clip(other_chip, other_core, slot)).wait_recv()
    for slot in range(SLOTS):
        for link in range(3):
            x_copy(slot, link).wait_send()
    for name in units:
        w_drain(name)
    for link in range(3):
        s_copy(link, tp).wait_send()


def encode(x, weights, vectors, cache_inputs):
    dma = pltpu.SemaphoreType.DMA
    any_spec, vmem_spec = pl.BlockSpec(memory_space=pl.ANY), pl.BlockSpec(memory_space=pltpu.VMEM)
    return pl.pallas_call(
        encoder_kernel,
        out_shape=(jax.ShapeDtypeStruct((CLIPS, FRAMES, WIDTH), BF16), jax.ShapeDtypeStruct((SLOTS, 2 * WIDTH, FRAMES), BF16)),
        in_specs=[any_spec] * 7 + [vmem_spec] * 11 + [any_spec, any_spec, vmem_spec],
        out_specs=(any_spec, any_spec),
        scratch_shapes=[
            pltpu.VMEM((8, WIDTH), F32), pltpu.VMEM((8, WIDTH), F32), pltpu.VMEM((8, HIDDEN), F32),
            pltpu.VMEM((SLOTS, FRAMES, WIDTH), BF16),
            pltpu.VMEM((2 * WIDTH, WIDTH), BF16), pltpu.VMEM((WIDTH, WIDTH), BF16), pltpu.VMEM((WIDTH, WIDTH), BF16),
            pltpu.VMEM((WIDTH, HIDDEN), BF16), pltpu.VMEM((HIDDEN, WIDTH), BF16),
            pltpu.VMEM((4, 8, WIDTH), F32),
            pltpu.VMEM((FRAMES, WIDTH), BF16), pltpu.VMEM((FRAMES, 2 * WIDTH), BF16), pltpu.VMEM((WIDTH, FRAMES), BF16),
            pltpu.VMEM((FRAMES, WIDTH), BF16),
            pltpu.VMEM((SLOTS, FRAMES, WIDTH), BF16),
            pltpu.VMEM((FRAMES, 2 * WIDTH), BF16),
            pltpu.VMEM((SLOTS, FRAMES, WIDTH), F32),
            pltpu.VMEM((8, 2 * WIDTH), F32),
            pltpu.VMEM((2 * WIDTH, WIDTH), BF16), pltpu.VMEM((WIDTH, 128), F32), pltpu.VMEM((2, 2 * WIDTH, FRAMES), BF16),
            dma((SLOTS, 3)), dma((SLOTS, 3)), dma((SLOTS,)),
            dma((8, 5)), dma((8, 5)), dma((8,)),
            dma((3,)), dma((3,)),
            dma((SLOTS + 2 * ONLY,)), dma((SLOTS + 2 * ONLY,)), dma((SLOTS,)),
            dma((2, 4)), dma((2,)),
        ],
        compiler_params=pltpu.CompilerParams(collective_id=0, has_side_effects=True, vmem_limit_bytes=64 * 1024 * 1024 - 128 * 1024),
        name="encoder",
    )(x, *weights, *vectors, *cache_inputs)


def cache_kernel(e_hbm, part_hbm, wk_hbm, wv_hbm, bias_ref, k_hbm, v_hbm, enc_hbm,
                 weights, shift, ebuf, obuf, pbuf, encbuf, w_sem, e_sem, out_sem, enc_sem, p_sem, pout_sem, own_sem):
    tp = lax.axis_index("tp")
    chip, core = tp // 2, tp % 2
    own_frames = pl.ds(pl.multiple_of(tp * LOC_FRAMES, LOC_FRAMES), LOC_FRAMES)

    def other(index):
        shared = (1 - core) * SHARED + index
        only = 2 * SHARED + ((tp + 1 + (index - SHARED) // ONLY) % 4) * ONLY + (index - SHARED) % ONLY
        return jnp.where(index < SHARED, shared, only)

    def load(index):
        return pltpu.make_async_copy(e_hbm.at[other(index)], ebuf.at[index], e_sem.at[index])

    def stores(src, slot, clip, sems):
        copies = []
        for which, dst in enumerate((k_hbm, v_hbm)):
            for layer in range(4):
                rows = pl.ds(which * WIDTH + layer * LOC_COLS, LOC_COLS)
                copies.append(pltpu.make_async_copy(src.at[slot, rows, :], dst.at[layer, clip], sems.at[slot, which * 4 + layer]))
        return copies

    def enc_store(index):
        return pltpu.make_async_copy(ebuf.at[index, own_frames, :], enc_hbm.at[other(index)], enc_sem.at[index])

    def own_load(slot):
        return pltpu.make_async_copy(e_hbm.at[clip_of(chip, core, slot), own_frames, :], encbuf.at[slot], own_sem.at[0, slot])

    def own_store(slot):
        return pltpu.make_async_copy(encbuf.at[slot], enc_hbm.at[clip_of(chip, core, slot)], own_sem.at[1, slot])

    def part_load(slot):
        return pltpu.make_async_copy(part_hbm.at[slot], pbuf.at[slot], p_sem.at[slot])

    load(0).start()
    weight_loads = cache_weight_loads(wk_hbm, wv_hbm, weights, w_sem)
    for copy in weight_loads:
        copy.start()
    for index in range(1, AHEAD):
        load(index).start()
    for slot in range(SLOTS):
        part_load(slot).start()
        own_load(slot).start()
    lay_out_shift(bias_ref, shift)
    for copy in weight_loads:
        copy.wait()

    def forward(slot):
        part_load(slot).wait()
        for copy in stores(pbuf, slot, clip_of(chip, core, slot), pout_sem):
            copy.start()
        own_load(slot).wait()
        own_store(slot).start()

    def body(step, _):
        for half in range(2):
            index = 2 * step + half
            load(index).wait()
            enc_store(index).start()

            @pl.when(index + AHEAD < OTHERS)
            def _():
                load(index + AHEAD).start()

            @pl.when(index >= OUT_SLOTS)
            def _():
                for copy in stores(obuf, index % OUT_SLOTS, other(index - OUT_SLOTS), out_sem):
                    copy.wait()

        for half in range(2):
            index = 2 * step + half
            cache_products(obuf, index % OUT_SLOTS, weights, shift, ebuf, index)
        for half in range(2):
            index = 2 * step + half
            for copy in stores(obuf, index % OUT_SLOTS, other(index), out_sem):
                copy.start()
        for slot in range(SLOTS):
            @pl.when(step == min(slot, OTHERS // 2 - 1))
            def _():
                forward(slot)
        return 0

    lax.fori_loop(0, OTHERS // 2, body, 0)
    for index in range(OTHERS - OUT_SLOTS, OTHERS):
        for copy in stores(obuf, index % OUT_SLOTS, other(index), out_sem):
            copy.wait()
    for index in range(OTHERS):
        enc_store(index).wait()
    for slot in range(SLOTS):
        own_store(slot).wait()
        for copy in stores(pbuf, slot, clip_of(chip, core, slot), pout_sem):
            copy.wait()


def caches(e_all, part, cache_inputs):
    cache = jax.ShapeDtypeStruct((4, CLIPS, LOC_COLS, FRAMES), BF16)
    any_spec = pl.BlockSpec(memory_space=pl.ANY)
    dma = pltpu.SemaphoreType.DMA
    return pl.pallas_call(
        cache_kernel,
        out_shape=(cache, cache, jax.ShapeDtypeStruct((CLIPS, LOC_FRAMES, WIDTH), BF16)),
        in_specs=[any_spec] * 4 + [pl.BlockSpec(memory_space=pltpu.VMEM)],
        out_specs=(any_spec, any_spec, any_spec),
        scratch_shapes=[
            pltpu.VMEM((2 * WIDTH, WIDTH), BF16), pltpu.VMEM((WIDTH, 128), F32),
            pltpu.VMEM((OTHERS, FRAMES, WIDTH), BF16), pltpu.VMEM((OUT_SLOTS, 2 * WIDTH, FRAMES), BF16),
            pltpu.VMEM((SLOTS, 2 * WIDTH, FRAMES), BF16), pltpu.VMEM((SLOTS, LOC_FRAMES, WIDTH), BF16),
            dma((2, 4)), dma((OTHERS,)), dma((OUT_SLOTS, 8)), dma((OTHERS,)), dma((SLOTS,)), dma((SLOTS, 8)), dma((2, SLOTS)),
        ],
        compiler_params=pltpu.CompilerParams(vmem_limit_bytes=64 * 1024 * 1024 - 128 * 1024),
        name="caches",
    )(e_all, part, *cache_inputs)


def device_body(hidden_loc, ln1_gain, ln1_bias, w_q, b_q, w_k, w_v, b_v, w_o, b_o, ln2_gain, ln2_bias, w_fc1, b_fc1, w_fc2, b_fc2, post_gain, post_bias, w_ck, w_cv, b_cv):
    weights = (w_q.T, w_k.T, w_v.T, w_o, w_fc1, w_fc2)
    vectors = (ln1_gain, ln1_bias, ln2_gain, ln2_bias, post_gain, post_bias, b_o, b_fc2, b_fc1, b_q, b_v)
    cache_inputs = (w_ck.transpose(0, 2, 1), w_cv.transpose(0, 2, 1), b_cv)
    e_all, part = encode(hidden_loc, weights, vectors, cache_inputs)
    k_t, v_t, enc_loc = caches(e_all, part, cache_inputs)
    shape = (4, CLIPS, FRAMES, 3, HEAD_DIM)
    return enc_loc, k_t.transpose(0, 1, 3, 2).reshape(shape), v_t.transpose(0, 1, 3, 2).reshape(shape)


def solution(mesh):
    in_specs = (P("dp", "tp", None), P(), P(), P(None, "tp"), P("tp"), P(None, "tp"), P(None, "tp"), P("tp"), P("tp", None), P(), P(), P(), P(None, "tp"), P("tp"), P("tp", None), P(), P(), P(), P(None, None, "tp"), P(None, None, "tp"), P(None, "tp"))
    out_specs = (P("dp", "tp", None), P(None, "dp", None, "tp", None), P(None, "dp", None, "tp", None))
    return jax.shard_map(device_body, mesh=mesh, in_specs=in_specs, out_specs=out_specs, check_vma=False)
```

```python
import functools

import jax
import jax.numpy as jnp
from jax import lax
from jax.experimental import pallas as pl
from jax.experimental.pallas import tpu as pltpu
from jax.sharding import PartitionSpec as P

HEAD_DIM = 64
ATTN_SCALE = HEAD_DIM ** -0.25
LN_EPS = 1e-5
SQRT_HALF = 0.5 ** 0.5
MESH = pl.DeviceIdType.MESH
BF16, F32 = jnp.bfloat16, jnp.float32

CLIPS, FRAMES, WIDTH, HIDDEN = 16, 512, 768, 3072
LOC_FRAMES, LOC_COLS = FRAMES // 4, WIDTH // 4
WIDE = (slice(0, 512), slice(512, 768))
SHARED, ONLY = 4, 2
SLOTS = SHARED + ONLY
TURN = 4
LN_ROWS = 64
SEND_ORDER = ("q", "k", "v", 0, "o", 1, 2, "w1a", "w1b", 3, "w2a", "w2b", 4, 5)
RELAYS = {
    (0, 0): ((1, "o"),), (0, 2): ((2, "o"),),
    (1, 3): ((1, "w1a"),), (2, 1): ((1, "w1b"),), (2, 3): ((2, "w1a"),),
    (3, 0): ((2, "w1b"),), (3, 1): ((1, "w2a"),), (3, 3): ((1, "w2b"), (2, "w2a")),
}
OUT_SLOTS, AHEAD = 6, 2

NT = (((1,), (1,)), ((), ()))
NN = (((1,), (0,)), ((), ()))
TN = (((0,), (0,)), ((), ()))


def dot(lhs, rhs, dims=NN):
    return lax.dot_general(lhs, rhs, dims, preferred_element_type=F32)


def norm_rows(values, gain, bias):
    centered = values.astype(F32)
    centered = centered - jnp.mean(centered, axis=-1, keepdims=True)
    row_var = jnp.mean(centered * centered, axis=-1, keepdims=True)
    return (centered * lax.rsqrt(row_var + LN_EPS) * gain + bias).astype(BF16)


def only_clip(chip, core, slot):
    return 2 * SHARED + (2 * chip + core) * ONLY + slot


def clip_of(chip, core, slot):
    return only_clip(chip, core, slot) if slot < ONLY else core * SHARED + slot - ONLY


def rows_of(ref, start, count):
    return ref.at[pl.ds(pl.multiple_of(start, 16), count), :]


def encoder_kernel(x_hbm, wq_hbm, wk_hbm, wv_hbm, wo_hbm, w1_hbm, w2_hbm,
                   g1_ref, s1_ref, g2_ref, s2_ref, g3_ref, s3_ref, bo_ref, b2_ref, b1_ref, bq_ref, bv_ref, e_hbm,
                   rep_ref, loc, b1_row, xbuf, wqv, wk, wo, w1, w2, small, abuf, qvbuf, ktbuf, obuf, mbuf, gbuf, acc, bias,
                   x_send, x_recv, x_loc, w_send, w_recv, w_loc, s_send, s_recv, e_send, e_recv, e_loc):
    group, tp = lax.axis_index("dp"), lax.axis_index("tp")
    chip, core = tp // 2, tp % 2
    other_chip, other_core = 1 - chip, 1 - core
    t_sib = 2 * chip + other_core
    t_far = 2 * other_chip + core
    t_diag = 2 * other_chip + other_core
    sib = {"dp": group, "tp": t_sib}
    far = {"dp": group, "tp": t_far}
    diag = {"dp": group, "tp": t_diag}
    side = {"dp": 1 - group, "tp": tp}

    def remote(src, dst, send, recv, device):
        return pltpu.make_async_remote_copy(src_ref=src, dst_ref=dst, send_sem=send, recv_sem=recv, device_id=device, device_id_type=MESH)

    def frames(slot, owner):
        return xbuf.at[slot, pl.ds(pl.multiple_of(owner * LOC_FRAMES, LOC_FRAMES), LOC_FRAMES), :]

    def x_copy(slot, link):
        device, there_chip, there_core = ((sib, chip, other_core), (far, other_chip, core), (diag, other_chip, other_core))[link]
        return remote(x_hbm.at[clip_of(there_chip, there_core, slot)], frames(slot, tp), x_send.at[slot, link], x_recv.at[slot, link], device)

    def x_local(slot):
        return pltpu.make_async_copy(x_hbm.at[clip_of(chip, core, slot)], frames(slot, tp), x_loc.at[slot])

    def x_wait(slot):
        pltpu.make_async_copy(x_hbm.at[0], frames(slot, tp), x_loc.at[slot]).wait()
        for link, owner in enumerate((t_sib, t_far, t_diag)):
            remote(x_hbm.at[0], frames(slot, owner), x_send.at[slot, link], x_recv.at[slot, link], sib).wait_recv()

    def at_rows(dst, base):
        shard = LOC_COLS if dst is not w2 else WIDTH
        return lambda owner, first, count: rows_of(dst, base + owner * shard + first, count)

    def at_columns(owner, first, count):
        return w1.at[pl.ds(pl.multiple_of(first, 16), count), pl.ds(pl.multiple_of(owner * WIDTH, WIDTH), WIDTH)]

    units = {
        "q": (0, wq_hbm, at_rows(wqv, 0), 0, 192), "k": (1, wk_hbm, at_rows(wk, 0), 0, 192),
        "v": (2, wv_hbm, at_rows(wqv, WIDTH), 0, 192), "o": (3, wo_hbm, at_rows(wo, 0), 0, 192),
        "w1a": (4, w1_hbm, at_columns, 0, 384), "w1b": (5, w1_hbm, at_columns, 384, 384),
        "w2a": (6, w2_hbm, at_rows(w2, 0), 0, 384), "w2b": (7, w2_hbm, at_rows(w2, 0), 384, 384),
    }

    def w_local(name):
        idx, src, place, first, count = units[name]
        return pltpu.make_async_copy(src.at[pl.ds(first, count), :], place(tp, first, count), w_loc.at[idx])

    def w_sib(name, owner):
        idx, src, place, first, count = units[name]
        return remote(src.at[pl.ds(first, count), :], place(owner, first, count), w_send.at[idx, 0], w_recv.at[idx, 0], sib)

    def w_far(name, owner):
        idx, src, place, first, count = units[name]
        half = count // 2
        return remote(rows_of(src, first + group * half, half), place(owner, first + group * half, half),
                      w_send.at[idx, 1], w_recv.at[idx, 1], far)

    def w_relay(name, owner, part, sem, recv, device):
        idx, src, place, first, count = units[name]
        half = count // 2
        piece = place(owner, first + part * half, half)
        return remote(piece, piece, w_send.at[idx, sem], w_recv.at[idx, recv], device)

    def w_start(name):
        w_far(name, tp).start()
        w_local(name).start()
        w_sib(name, tp).start()

    def w_stage1(name):
        w_far(name, t_far).wait_recv()
        w_relay(name, t_far, group, 3, 2, side).start()
        w_relay(name, t_far, group, 2, 3, sib).start()

    def w_stage2(name):
        w_relay(name, t_far, 1 - group, 3, 2, side).wait_recv()
        w_relay(name, t_far, 1 - group, 4, 4, sib).start()

    def w_wait_near(name):
        w_local(name).wait()
        w_sib(name, t_sib).wait_recv()

    def w_wait_far(name):
        w_relay(name, t_diag, group, 2, 3, sib).wait_recv()
        w_relay(name, t_diag, 1 - group, 4, 4, sib).wait_recv()

    def w_drain(name):
        w_sib(name, tp).wait_send()
        w_far(name, tp).wait_send()
        w_relay(name, t_far, group, 3, 2, side).wait_send()
        w_relay(name, t_far, group, 2, 3, sib).wait_send()
        w_relay(name, t_far, 1 - group, 4, 4, sib).wait_send()

    def s_copy(link, owner):
        device = (sib, far, diag)[link]
        return remote(loc, small.at[owner], s_send.at[link], s_recv.at[link], device)

    def e_local(slot, clip):
        return pltpu.make_async_copy(xbuf.at[slot], e_hbm.at[clip], e_loc.at[slot])

    def e_sib(slot, clip):
        return remote(xbuf.at[slot], e_hbm.at[clip], e_send.at[slot], e_recv.at[slot], sib)

    def e_far(slot, clip):
        return remote(xbuf.at[slot], e_hbm.at[clip], e_send.at[SLOTS + slot], e_recv.at[SLOTS + slot], far)

    def e_relay(slot, clip):
        sem = SLOTS + ONLY + slot
        return remote(e_hbm.at[clip], e_hbm.at[clip], e_send.at[sem], e_recv.at[sem], sib)

    barrier = pltpu.get_barrier_semaphore()
    for device in (sib, far, diag, side):
        pl.semaphore_signal(barrier, inc=1, device_id=device, device_id_type=MESH)

    for row, ref in enumerate((g1_ref, s1_ref, g2_ref, s2_ref, g3_ref, s3_ref, bo_ref, b2_ref)):
        rep_ref[row:row + 1, :] = ref[...].astype(F32).reshape(1, WIDTH)
    place = lax.broadcasted_iota(jnp.int32, (192, WIDTH), 0) + tp * 192 == lax.broadcasted_iota(jnp.int32, (192, WIDTH), 1)
    place = place.astype(F32).astype(BF16)
    loc[0:1, :] = b1_ref[...].astype(F32).reshape(1, WIDTH)
    for row, ref in ((1, bq_ref), (2, bv_ref)):
        vector = jnp.broadcast_to(ref[...].astype(F32).reshape(1, 192), (16, 192)).astype(BF16)
        loc[row:row + 1, :] = dot(vector, place)[0:1, :]
    loc[3:8, :] = jnp.zeros((5, WIDTH), F32)
    small[tp] = loc[...]

    pl.semaphore_wait(barrier, 4)

    for link in (1, 2, 0):
        s_copy(link, tp).start()
    for item in SEND_ORDER:
        if isinstance(item, str):
            w_start(item)
        else:
            x_copy(item, 1).start()
            x_copy(item, 2).start()
            x_local(item).start()
            x_copy(item, 0).start()

    w_stage1("q")
    w_stage1("k")
    w_stage2("q")
    w_stage1("v")
    w_stage2("k")
    for link, owner in enumerate((t_sib, t_far, t_diag)):
        s_copy(link, owner).wait_recv()
    bias[0:1, 0:WIDTH] = small[0, 1:2, :] + small[1, 1:2, :] + small[2, 1:2, :] + small[3, 1:2, :]
    bias[0:1, WIDTH:2 * WIDTH] = small[0, 2:3, :] + small[1, 2:3, :] + small[2, 2:3, :] + small[3, 2:3, :]
    for owner in range(4):
        b1_row[0:1, owner * WIDTH:owner * WIDTH + WIDTH] = small[owner, 0:1, :]
    w_stage2("v")
    for name in ("q", "k", "v"):
        w_wait_near(name)
        w_wait_far(name)

    def rep(row):
        return rep_ref[row:row + 1, :]

    def norm_into(dst_store, src_load, gain, shift):
        for first in range(0, FRAMES, LN_ROWS):
            dst_store(first, norm_rows(src_load(first), gain, shift))

    def relays(step, place):
        for (when, where), todo in RELAYS.items():
            if where == place:
                @pl.when(step == when)
                def _():
                    for stage, name in todo:
                        (w_stage1 if stage == 1 else w_stage2)(name)

    def attention(slot, step):
        x_wait(slot)

        def put_a(first, value):
            abuf[first:first + LN_ROWS, :] = value

        norm_into(put_a, lambda first: xbuf[slot, pl.ds(first, LN_ROWS), :], rep(0), rep(1))
        scale = jnp.where(lax.broadcasted_iota(jnp.int32, (1, 2 * WIDTH), 1) < WIDTH, ATTN_SCALE, 1.0)
        ktbuf[...] = (dot(wk[...], abuf[...], NT) * ATTN_SCALE).astype(BF16)
        for col in range(0, 2 * WIDTH, 512):
            cols = slice(col, col + 512)
            qvbuf[:, cols] = ((dot(abuf[...], wqv[cols, :], NT) + bias[0:1, cols]) * scale[:, cols]).astype(BF16)

        lane = lax.broadcasted_iota(jnp.int32, (1, 128), 1)
        keep = [(lane < 64).astype(F32).astype(BF16), (lane >= 64).astype(F32).astype(BF16)]

        def pair_body(pair, _):
            cols = pl.ds(pl.multiple_of(pair * 128, 128), 128)
            keys_t = ktbuf[cols, :]
            values = qvbuf[:, pl.ds(pl.multiple_of(WIDTH + pair * 128, 128), 128)]

            def scores_of(head):
                return dot(qvbuf[:, cols] * keep[head], keys_t)

            scores = scores_of(0)
            outs = []
            for head in range(2):
                ahead = scores_of(1) if head == 0 else None
                top = jnp.max(scores, axis=-1, keepdims=True)
                weight = jnp.exp(scores - top)
                total = jnp.sum(weight, axis=-1, keepdims=True)
                outs.append(dot(weight.astype(BF16), values) * (1.0 / total))
                scores = ahead
            obuf[:, cols] = jnp.where(lane < 64, outs[0], outs[1]).astype(BF16)
            return 0

        relays(step, 0)
        lax.fori_loop(0, 3, pair_body, 0)
        relays(step, 1)
        lax.fori_loop(3, 6, pair_body, 0)
        relays(step, 2)

        @pl.when(step == 0)
        def _():
            w_wait_near("o")
            w_wait_far("o")

        for cols in WIDE:
            branch = (dot(obuf[...], wo[:, cols]) + rep_ref[6:7, cols]).astype(BF16)
            xbuf[slot, :, cols] = (xbuf[slot, :, cols].astype(F32) + branch.astype(F32)).astype(BF16)

        def put_m(first, value):
            mbuf[slot, pl.ds(first, LN_ROWS), :] = value

        norm_into(put_m, lambda first: xbuf[slot, pl.ds(first, LN_ROWS), :], rep(2), rep(3))

    def hidden_half(slot, which):
        def product(col):
            return dot(mbuf[slot], w1[:, pl.ds(pl.multiple_of(which * 1536 + col, 512), 512)])

        ahead = product(0)
        for col in range(0, 1536, 512):
            inner = ahead + b1_row[0:1, pl.ds(pl.multiple_of(which * 1536 + col, 512), 512)]
            if col + 512 < 1536:
                ahead = product(col + 512)
            gbuf[:, col:col + 512] = (0.5 * inner * (1.0 + lax.erf(inner * SQRT_HALF))).astype(BF16)

    def second_product(which, cols):
        return dot(gbuf[...], w2[pl.ds(pl.multiple_of(which * 1536, 1536), 1536), cols])

    def mlp_near(slot):
        hidden_half(slot, chip)
        for cols in WIDE:
            acc[slot, :, cols] = second_product(chip, cols)

    def mlp_far(slot):
        hidden_half(slot, other_chip)
        for cols in WIDE:
            branch = (acc[slot, :, cols] + second_product(other_chip, cols) + rep_ref[7:8, cols]).astype(BF16)
            xbuf[slot, :, cols] = (xbuf[slot, :, cols].astype(F32) + branch.astype(F32)).astype(BF16)

        def put_e(first, value):
            xbuf[slot, pl.ds(first, LN_ROWS), :] = value

        norm_into(put_e, lambda first: xbuf[slot, pl.ds(first, LN_ROWS), :], rep(4), rep(5))

        @pl.when(slot < ONLY)
        def _():
            clip = only_clip(chip, core, slot)
            e_far(slot, clip).start()
            e_local(slot, clip).start()
            e_sib(slot, clip).start()

        @pl.when(slot >= ONLY)
        def _():
            clip = core * SHARED + slot - ONLY
            e_local(slot, clip).start()
            e_sib(slot, clip).start()

    mlp_units = ("w1a", "w1b", "w2a", "w2b")

    def far_body(slot, _):
        mlp_far(slot)
        return 0

    def step_body(step, _):
        @pl.when(step == TURN)
        def _():
            w_stage2("w2b")
            for name in mlp_units:
                w_wait_far(name)

        @pl.when((step == TURN) | (step == SLOTS))
        def _():
            lax.fori_loop(step - TURN, (step - TURN) * (SLOTS - ONLY) // (SLOTS - TURN) + ONLY, far_body, 0)

        @pl.when(step < SLOTS)
        def _():
            attention(step, step)

            @pl.when(step == 0)
            def _():
                for name in mlp_units:
                    w_wait_near(name)

            mlp_near(step)
            relays(step, 3)

        return 0

    lax.fori_loop(0, SLOTS + 1, step_body, 0)

    for slot in range(ONLY):
        clip = only_clip(other_chip, core, slot)
        e_far(slot, clip).wait_recv()
        e_relay(slot, clip).start()
    for slot in range(SLOTS):
        clip = clip_of(chip, core, slot)
        e_local(slot, clip).wait()
        e_sib(slot, clip).wait_send()
        e_sib(slot, clip_of(chip, other_core, slot)).wait_recv()
    for slot in range(ONLY):
        e_far(slot, only_clip(chip, core, slot)).wait_send()
        e_relay(slot, only_clip(other_chip, core, slot)).wait_send()
        e_relay(slot, only_clip(other_chip, other_core, slot)).wait_recv()
    for slot in range(SLOTS):
        for link in range(3):
            x_copy(slot, link).wait_send()
    for name in units:
        w_drain(name)
    for link in range(3):
        s_copy(link, tp).wait_send()


def encode(x, weights, vectors):
    dma = pltpu.SemaphoreType.DMA
    any_spec = pl.BlockSpec(memory_space=pl.ANY)
    return pl.pallas_call(
        encoder_kernel,
        out_shape=jax.ShapeDtypeStruct((CLIPS, FRAMES, WIDTH), BF16),
        in_specs=[any_spec] * 7 + [pl.BlockSpec(memory_space=pltpu.VMEM)] * 11,
        out_specs=any_spec,
        scratch_shapes=[
            pltpu.VMEM((8, WIDTH), F32), pltpu.VMEM((8, WIDTH), F32), pltpu.VMEM((8, HIDDEN), F32),
            pltpu.VMEM((SLOTS, FRAMES, WIDTH), BF16),
            pltpu.VMEM((2 * WIDTH, WIDTH), BF16), pltpu.VMEM((WIDTH, WIDTH), BF16), pltpu.VMEM((WIDTH, WIDTH), BF16),
            pltpu.VMEM((WIDTH, HIDDEN), BF16), pltpu.VMEM((HIDDEN, WIDTH), BF16),
            pltpu.VMEM((4, 8, WIDTH), F32),
            pltpu.VMEM((FRAMES, WIDTH), BF16), pltpu.VMEM((FRAMES, 2 * WIDTH), BF16), pltpu.VMEM((WIDTH, FRAMES), BF16),
            pltpu.VMEM((FRAMES, WIDTH), BF16),
            pltpu.VMEM((SLOTS, FRAMES, WIDTH), BF16),
            pltpu.VMEM((FRAMES, 2 * WIDTH), BF16),
            pltpu.VMEM((SLOTS, FRAMES, WIDTH), F32),
            pltpu.VMEM((8, 2 * WIDTH), F32),
            dma((SLOTS, 3)), dma((SLOTS, 3)), dma((SLOTS,)),
            dma((8, 5)), dma((8, 5)), dma((8,)),
            dma((3,)), dma((3,)),
            dma((SLOTS + 2 * ONLY,)), dma((SLOTS + 2 * ONLY,)), dma((SLOTS,)),
        ],
        compiler_params=pltpu.CompilerParams(collective_id=0, has_side_effects=True, vmem_limit_bytes=64 * 1024 * 1024 - 128 * 1024),
        name="encoder",
    )(x, *weights, *vectors)


def cache_kernel(e_hbm, wk_hbm, wv_hbm, bias_ref, k_hbm, v_hbm, enc_hbm, weights, shift, ebuf, obuf, w_sem, e_sem, out_sem, enc_sem):
    tp = lax.axis_index("tp")

    def load(clip):
        return pltpu.make_async_copy(e_hbm.at[clip], ebuf.at[clip], e_sem.at[clip])

    def stores(clip, slot):
        copies = []
        for which, dst in enumerate((k_hbm, v_hbm)):
            for layer in range(4):
                rows = pl.ds(which * WIDTH + layer * LOC_COLS, LOC_COLS)
                copies.append(pltpu.make_async_copy(obuf.at[slot, rows, :], dst.at[layer, clip], out_sem.at[slot, which * 4 + layer]))
        return copies

    def enc_store(clip):
        own = pl.ds(pl.multiple_of(tp * LOC_FRAMES, LOC_FRAMES), LOC_FRAMES)
        return pltpu.make_async_copy(ebuf.at[clip, own, :], enc_hbm.at[clip], enc_sem.at[clip])

    load(0).start()
    weight_loads = [pltpu.make_async_copy(src.at[layer], weights.at[pl.ds(which * WIDTH + layer * LOC_COLS, LOC_COLS), :], w_sem.at[which, layer])
                    for which, src in enumerate((wk_hbm, wv_hbm)) for layer in range(4)]
    for copy in weight_loads:
        copy.start()
    for clip in range(1, AHEAD):
        load(clip).start()
    rows = jnp.concatenate([bias_ref[...].astype(F32), jnp.zeros((4, LOC_COLS), F32)], axis=0)
    for layer in range(4):
        pick = (lax.broadcasted_iota(jnp.int32, (8, 128), 0) == layer).astype(F32)
        shift[layer * LOC_COLS:(layer + 1) * LOC_COLS, :] = dot(rows, pick, TN)
    for copy in weight_loads:
        copy.wait()

    def body(step, _):
        for half in range(2):
            clip = 2 * step + half
            slot = clip % OUT_SLOTS
            load(clip).wait()
            enc_store(clip).start()

            @pl.when(clip + AHEAD < CLIPS)
            def _():
                load(clip + AHEAD).start()

            @pl.when(clip >= OUT_SLOTS)
            def _():
                for copy in stores(clip - OUT_SLOTS, slot):
                    copy.wait()

        for half in range(2):
            clip = 2 * step + half
            slot = clip % OUT_SLOTS
            obuf[slot, 0:WIDTH, :] = dot(weights[0:WIDTH, :], ebuf[clip], NT).astype(BF16)
            obuf[slot, WIDTH:2 * WIDTH, :] = (dot(weights[WIDTH:2 * WIDTH, :], ebuf[clip], NT) + jnp.concatenate([shift[...]] * 4, axis=1)).astype(BF16)
        for half in range(2):
            clip = 2 * step + half
            for copy in stores(clip, clip % OUT_SLOTS):
                copy.start()
        return 0

    lax.fori_loop(0, CLIPS // 2, body, 0)
    for clip in range(CLIPS - OUT_SLOTS, CLIPS):
        for copy in stores(clip, clip % OUT_SLOTS):
            copy.wait()
    for clip in range(CLIPS):
        enc_store(clip).wait()


def caches(e_all, wck_t, wcv_t, bias):
    cache = jax.ShapeDtypeStruct((4, CLIPS, LOC_COLS, FRAMES), BF16)
    any_spec = pl.BlockSpec(memory_space=pl.ANY)
    dma = pltpu.SemaphoreType.DMA
    return pl.pallas_call(
        cache_kernel,
        out_shape=(cache, cache, jax.ShapeDtypeStruct((CLIPS, LOC_FRAMES, WIDTH), BF16)),
        in_specs=[any_spec, any_spec, any_spec, pl.BlockSpec(memory_space=pltpu.VMEM)],
        out_specs=(any_spec, any_spec, any_spec),
        scratch_shapes=[
            pltpu.VMEM((2 * WIDTH, WIDTH), BF16), pltpu.VMEM((WIDTH, 128), F32),
            pltpu.VMEM((CLIPS, FRAMES, WIDTH), BF16), pltpu.VMEM((OUT_SLOTS, 2 * WIDTH, FRAMES), BF16),
            dma((2, 4)), dma((CLIPS,)), dma((OUT_SLOTS, 8)), dma((CLIPS,)),
        ],
        compiler_params=pltpu.CompilerParams(vmem_limit_bytes=64 * 1024 * 1024 - 128 * 1024),
        name="caches",
    )(e_all, wck_t, wcv_t, bias)


def device_body(hidden_loc, ln1_gain, ln1_bias, w_q, b_q, w_k, w_v, b_v, w_o, b_o, ln2_gain, ln2_bias, w_fc1, b_fc1, w_fc2, b_fc2, post_gain, post_bias, w_ck, w_cv, b_cv):
    weights = (w_q.T, w_k.T, w_v.T, w_o, w_fc1, w_fc2)
    vectors = (ln1_gain, ln1_bias, ln2_gain, ln2_bias, post_gain, post_bias, b_o, b_fc2, b_fc1, b_q, b_v)
    e_all = encode(hidden_loc, weights, vectors)
    k_t, v_t, enc_loc = caches(e_all, w_ck.transpose(0, 2, 1), w_cv.transpose(0, 2, 1), b_cv)
    shape = (4, CLIPS, FRAMES, 3, HEAD_DIM)
    return enc_loc, k_t.transpose(0, 1, 3, 2).reshape(shape), v_t.transpose(0, 1, 3, 2).reshape(shape)


def solution(mesh):
    in_specs = (P("dp", "tp", None), P(), P(), P(None, "tp"), P("tp"), P(None, "tp"), P(None, "tp"), P("tp"), P("tp", None), P(), P(), P(), P(None, "tp"), P("tp"), P("tp", None), P(), P(), P(), P(None, None, "tp"), P(None, None, "tp"), P(None, "tp"))
    out_specs = (P("dp", "tp", None), P(None, "dp", None, "tp", None), P(None, "dp", None, "tp", None))
    return jax.shard_map(device_body, mesh=mesh, in_specs=in_specs, out_specs=out_specs, check_vma=False)
```

```python
import functools

import jax
import jax.numpy as jnp
from jax import lax
from jax.experimental import pallas as pl
from jax.experimental.pallas import tpu as pltpu
from jax.sharding import PartitionSpec as P

HEAD_DIM = 64
ATTN_SCALE = HEAD_DIM ** -0.25
LN_EPS = 1e-5
SQRT_HALF = 0.5 ** 0.5
MESH = pl.DeviceIdType.MESH
BF16, F32 = jnp.bfloat16, jnp.float32

CLIPS, FRAMES, WIDTH, HIDDEN = 16, 512, 768, 3072
LOC_FRAMES, LOC_COLS = FRAMES // 4, WIDTH // 4
WIDE = (slice(0, 512), slice(512, 768))
SHARED, ONLY = 4, 2
SLOTS = SHARED + ONLY
TURN = 5
LN_ROWS = 64
SEND_ORDER = ("q", "k", "v", 0, "o", 1, 2, "w1a", "w1b", 3, "w2a", 4, "w2b", "w2c", 5)
RELAYS = {
    (0, 0): ((1, "o"),), (0, 2): ((2, "o"),),
    (1, 3): ((1, "w1a"),), (2, 1): ((1, "w1b"),), (2, 3): ((2, "w1a"),),
    (3, 0): ((2, "w1b"),), (3, 3): ((1, "w2a"),), (4, 1): ((1, "w2b"),), (4, 2): ((1, "w2c"), (2, "w2a")), (4, 3): ((2, "w2b"),),
}
OUT_SLOTS, AHEAD = 6, 2

NT = (((1,), (1,)), ((), ()))
NN = (((1,), (0,)), ((), ()))
TN = (((0,), (0,)), ((), ()))


def dot(lhs, rhs, dims=NN):
    return lax.dot_general(lhs, rhs, dims, preferred_element_type=F32)


def norm_rows(values, gain, bias):
    centered = values.astype(F32)
    centered = centered - jnp.mean(centered, axis=-1, keepdims=True)
    row_var = jnp.mean(centered * centered, axis=-1, keepdims=True)
    return (centered * lax.rsqrt(row_var + LN_EPS) * gain + bias).astype(BF16)


def only_clip(chip, core, slot):
    return 2 * SHARED + (2 * chip + core) * ONLY + slot


def clip_of(chip, core, slot):
    return only_clip(chip, core, slot) if slot < ONLY else core * SHARED + slot - ONLY


def rows_of(ref, start, count):
    return ref.at[pl.ds(pl.multiple_of(start, 16), count), :]


def encoder_kernel(x_hbm, wq_hbm, wk_hbm, wv_hbm, wo_hbm, w1_hbm, w2_hbm,
                   g1_ref, s1_ref, g2_ref, s2_ref, g3_ref, s3_ref, bo_ref, b2_ref, b1_ref, bq_ref, bv_ref, e_hbm,
                   rep_ref, loc, b1_row, xbuf, wqv, wk, wo, w1, w2, small, abuf, qvbuf, ktbuf, obuf, mbuf, gbuf, acc, bias,
                   x_send, x_recv, x_loc, w_send, w_recv, w_loc, s_send, s_recv, e_send, e_recv, e_loc):
    group, tp = lax.axis_index("dp"), lax.axis_index("tp")
    chip, core = tp // 2, tp % 2
    other_chip, other_core = 1 - chip, 1 - core
    t_sib = 2 * chip + other_core
    t_far = 2 * other_chip + core
    t_diag = 2 * other_chip + other_core
    sib = {"dp": group, "tp": t_sib}
    far = {"dp": group, "tp": t_far}
    diag = {"dp": group, "tp": t_diag}
    side = {"dp": 1 - group, "tp": tp}

    def remote(src, dst, send, recv, device):
        return pltpu.make_async_remote_copy(src_ref=src, dst_ref=dst, send_sem=send, recv_sem=recv, device_id=device, device_id_type=MESH)

    def frames(slot, owner):
        return xbuf.at[slot, pl.ds(pl.multiple_of(owner * LOC_FRAMES, LOC_FRAMES), LOC_FRAMES), :]

    def x_copy(slot, link):
        device, there_chip, there_core = ((sib, chip, other_core), (far, other_chip, core), (diag, other_chip, other_core))[link]
        return remote(x_hbm.at[clip_of(there_chip, there_core, slot)], frames(slot, tp), x_send.at[slot, link], x_recv.at[slot, link], device)

    def x_local(slot):
        return pltpu.make_async_copy(x_hbm.at[clip_of(chip, core, slot)], frames(slot, tp), x_loc.at[slot])

    def x_wait(slot):
        pltpu.make_async_copy(x_hbm.at[0], frames(slot, tp), x_loc.at[slot]).wait()
        for link, owner in enumerate((t_sib, t_far, t_diag)):
            remote(x_hbm.at[0], frames(slot, owner), x_send.at[slot, link], x_recv.at[slot, link], sib).wait_recv()

    def at_rows(dst, base):
        shard = LOC_COLS if dst is not w2 else WIDTH
        return lambda owner, first, count: rows_of(dst, base + owner * shard + first, count)

    def at_columns(owner, first, count):
        return w1.at[pl.ds(pl.multiple_of(first, 16), count), pl.ds(pl.multiple_of(owner * WIDTH, WIDTH), WIDTH)]

    units = {
        "q": (0, wq_hbm, at_rows(wqv, 0), 0, 192), "k": (1, wk_hbm, at_rows(wk, 0), 0, 192),
        "v": (2, wv_hbm, at_rows(wqv, WIDTH), 0, 192), "o": (3, wo_hbm, at_rows(wo, 0), 0, 192),
        "w1a": (4, w1_hbm, at_columns, 0, 384), "w1b": (5, w1_hbm, at_columns, 384, 384),
        "w2a": (6, w2_hbm, at_rows(w2, 0), 0, 384), "w2b": (7, w2_hbm, at_rows(w2, 0), 384, 192),
        "w2c": (8, w2_hbm, at_rows(w2, 0), 576, 192),
    }

    def w_local(name):
        idx, src, place, first, count = units[name]
        return pltpu.make_async_copy(src.at[pl.ds(first, count), :], place(tp, first, count), w_loc.at[idx])

    def w_sib(name, owner):
        idx, src, place, first, count = units[name]
        return remote(src.at[pl.ds(first, count), :], place(owner, first, count), w_send.at[idx, 0], w_recv.at[idx, 0], sib)

    def w_far(name, owner):
        idx, src, place, first, count = units[name]
        half = count // 2
        return remote(rows_of(src, first + group * half, half), place(owner, first + group * half, half),
                      w_send.at[idx, 1], w_recv.at[idx, 1], far)

    def w_relay(name, owner, part, sem, recv, device):
        idx, src, place, first, count = units[name]
        half = count // 2
        piece = place(owner, first + part * half, half)
        return remote(piece, piece, w_send.at[idx, sem], w_recv.at[idx, recv], device)

    def w_start(name):
        w_far(name, tp).start()
        w_local(name).start()
        w_sib(name, tp).start()

    def w_stage1(name):
        w_far(name, t_far).wait_recv()
        w_relay(name, t_far, group, 3, 2, side).start()
        w_relay(name, t_far, group, 2, 3, sib).start()

    def w_stage2(name):
        w_relay(name, t_far, 1 - group, 3, 2, side).wait_recv()
        w_relay(name, t_far, 1 - group, 4, 4, sib).start()

    def w_wait_near(name):
        w_local(name).wait()
        w_sib(name, t_sib).wait_recv()

    def w_wait_far(name):
        w_relay(name, t_diag, group, 2, 3, sib).wait_recv()
        w_relay(name, t_diag, 1 - group, 4, 4, sib).wait_recv()

    def w_drain(name):
        w_sib(name, tp).wait_send()
        w_far(name, tp).wait_send()
        w_relay(name, t_far, group, 3, 2, side).wait_send()
        w_relay(name, t_far, group, 2, 3, sib).wait_send()
        w_relay(name, t_far, 1 - group, 4, 4, sib).wait_send()

    def s_copy(link, owner):
        device = (sib, far, diag)[link]
        return remote(loc, small.at[owner], s_send.at[link], s_recv.at[link], device)

    def e_local(slot, clip):
        return pltpu.make_async_copy(xbuf.at[slot], e_hbm.at[clip], e_loc.at[slot])

    def e_sib(slot, clip):
        return remote(xbuf.at[slot], e_hbm.at[clip], e_send.at[slot], e_recv.at[slot], sib)

    def e_far(slot, clip):
        return remote(xbuf.at[slot], e_hbm.at[clip], e_send.at[SLOTS + slot], e_recv.at[SLOTS + slot], far)

    def e_relay(slot, clip):
        sem = SLOTS + ONLY + slot
        return remote(e_hbm.at[clip], e_hbm.at[clip], e_send.at[sem], e_recv.at[sem], sib)

    barrier = pltpu.get_barrier_semaphore()
    for device in (sib, far, diag, side):
        pl.semaphore_signal(barrier, inc=1, device_id=device, device_id_type=MESH)

    for row, ref in enumerate((g1_ref, s1_ref, g2_ref, s2_ref, g3_ref, s3_ref, bo_ref, b2_ref)):
        rep_ref[row:row + 1, :] = ref[...].astype(F32).reshape(1, WIDTH)
    place = lax.broadcasted_iota(jnp.int32, (192, WIDTH), 0) + tp * 192 == lax.broadcasted_iota(jnp.int32, (192, WIDTH), 1)
    place = place.astype(F32).astype(BF16)
    loc[0:1, :] = b1_ref[...].astype(F32).reshape(1, WIDTH)
    for row, ref in ((1, bq_ref), (2, bv_ref)):
        vector = jnp.broadcast_to(ref[...].astype(F32).reshape(1, 192), (16, 192)).astype(BF16)
        loc[row:row + 1, :] = dot(vector, place)[0:1, :]
    loc[3:8, :] = jnp.zeros((5, WIDTH), F32)
    small[tp] = loc[...]

    pl.semaphore_wait(barrier, 4)

    for link in (1, 2, 0):
        s_copy(link, tp).start()
    for item in SEND_ORDER:
        if isinstance(item, str):
            w_start(item)
        else:
            x_copy(item, 1).start()
            x_copy(item, 2).start()
            x_local(item).start()
            x_copy(item, 0).start()

    w_stage1("q")
    w_stage1("k")
    w_stage2("q")
    w_stage1("v")
    w_stage2("k")
    for link, owner in enumerate((t_sib, t_far, t_diag)):
        s_copy(link, owner).wait_recv()
    bias[0:1, 0:WIDTH] = small[0, 1:2, :] + small[1, 1:2, :] + small[2, 1:2, :] + small[3, 1:2, :]
    bias[0:1, WIDTH:2 * WIDTH] = small[0, 2:3, :] + small[1, 2:3, :] + small[2, 2:3, :] + small[3, 2:3, :]
    for owner in range(4):
        b1_row[0:1, owner * WIDTH:owner * WIDTH + WIDTH] = small[owner, 0:1, :]
    w_stage2("v")
    for name in ("q", "k", "v"):
        w_wait_near(name)
        w_wait_far(name)

    def rep(row):
        return rep_ref[row:row + 1, :]

    def norm_into(dst_store, src_load, gain, shift):
        for first in range(0, FRAMES, LN_ROWS):
            dst_store(first, norm_rows(src_load(first), gain, shift))

    def relays(step, place):
        for (when, where), todo in RELAYS.items():
            if where == place:
                @pl.when(step == when)
                def _():
                    for stage, name in todo:
                        (w_stage1 if stage == 1 else w_stage2)(name)

    def attention(slot, step):
        x_wait(slot)

        def put_a(first, value):
            abuf[first:first + LN_ROWS, :] = value

        norm_into(put_a, lambda first: xbuf[slot, pl.ds(first, LN_ROWS), :], rep(0), rep(1))
        scale = jnp.where(lax.broadcasted_iota(jnp.int32, (1, 2 * WIDTH), 1) < WIDTH, ATTN_SCALE, 1.0)
        ktbuf[...] = (dot(wk[...], abuf[...], NT) * ATTN_SCALE).astype(BF16)
        for col in range(0, 2 * WIDTH, 512):
            cols = slice(col, col + 512)
            qvbuf[:, cols] = ((dot(abuf[...], wqv[cols, :], NT) + bias[0:1, cols]) * scale[:, cols]).astype(BF16)

        lane = lax.broadcasted_iota(jnp.int32, (1, 128), 1)
        keep = [(lane < 64).astype(F32).astype(BF16), (lane >= 64).astype(F32).astype(BF16)]

        def pair_body(pair, _):
            cols = pl.ds(pl.multiple_of(pair * 128, 128), 128)
            keys_t = ktbuf[cols, :]
            values = qvbuf[:, pl.ds(pl.multiple_of(WIDTH + pair * 128, 128), 128)]

            def scores_of(head):
                return dot(qvbuf[:, cols] * keep[head], keys_t)

            scores = scores_of(0)
            outs = []
            for head in range(2):
                ahead = scores_of(1) if head == 0 else None
                top = jnp.max(scores, axis=-1, keepdims=True)
                weight = jnp.exp(scores - top)
                total = jnp.sum(weight, axis=-1, keepdims=True)
                outs.append(dot(weight.astype(BF16), values) * (1.0 / total))
                scores = ahead
            obuf[:, cols] = jnp.where(lane < 64, outs[0], outs[1]).astype(BF16)
            return 0

        relays(step, 0)
        lax.fori_loop(0, 3, pair_body, 0)
        relays(step, 1)
        lax.fori_loop(3, 6, pair_body, 0)
        relays(step, 2)

        @pl.when(step == 0)
        def _():
            w_wait_near("o")
            w_wait_far("o")

        for cols in WIDE:
            branch = (dot(obuf[...], wo[:, cols]) + rep_ref[6:7, cols]).astype(BF16)
            xbuf[slot, :, cols] = (xbuf[slot, :, cols].astype(F32) + branch.astype(F32)).astype(BF16)

        def put_m(first, value):
            mbuf[slot, pl.ds(first, LN_ROWS), :] = value

        norm_into(put_m, lambda first: xbuf[slot, pl.ds(first, LN_ROWS), :], rep(2), rep(3))

    def hidden_half(slot, which):
        def product(col):
            return dot(mbuf[slot], w1[:, pl.ds(pl.multiple_of(which * 1536 + col, 512), 512)])

        ahead = product(0)
        for col in range(0, 1536, 512):
            inner = ahead + b1_row[0:1, pl.ds(pl.multiple_of(which * 1536 + col, 512), 512)]
            if col + 512 < 1536:
                ahead = product(col + 512)
            gbuf[:, col:col + 512] = (0.5 * inner * (1.0 + lax.erf(inner * SQRT_HALF))).astype(BF16)

    def second_product(which, cols):
        return dot(gbuf[...], w2[pl.ds(pl.multiple_of(which * 1536, 1536), 1536), cols])

    def mlp_near(slot):
        hidden_half(slot, chip)
        for cols in WIDE:
            acc[slot, :, cols] = second_product(chip, cols)

    def mlp_far(slot):
        hidden_half(slot, other_chip)
        for cols in WIDE:
            branch = (acc[slot, :, cols] + second_product(other_chip, cols) + rep_ref[7:8, cols]).astype(BF16)
            xbuf[slot, :, cols] = (xbuf[slot, :, cols].astype(F32) + branch.astype(F32)).astype(BF16)

        def put_e(first, value):
            xbuf[slot, pl.ds(first, LN_ROWS), :] = value

        norm_into(put_e, lambda first: xbuf[slot, pl.ds(first, LN_ROWS), :], rep(4), rep(5))

        @pl.when(slot < ONLY)
        def _():
            clip = only_clip(chip, core, slot)
            e_far(slot, clip).start()
            e_local(slot, clip).start()
            e_sib(slot, clip).start()

        @pl.when(slot >= ONLY)
        def _():
            clip = core * SHARED + slot - ONLY
            e_local(slot, clip).start()
            e_sib(slot, clip).start()

    mlp_units = ("w1a", "w1b", "w2a", "w2b", "w2c")

    def far_body(slot, _):
        mlp_far(slot)
        return 0

    def step_body(step, _):
        @pl.when(step == TURN)
        def _():
            w_stage2("w2c")
            for name in mlp_units:
                w_wait_far(name)

        @pl.when((step == TURN) | (step == SLOTS))
        def _():
            turn = (step - TURN) // (SLOTS - TURN)
            lax.fori_loop(turn * ONLY, turn * (SLOTS - ONLY) + ONLY, far_body, 0)

        @pl.when(step < SLOTS)
        def _():
            attention(step, step)

            @pl.when(step == 0)
            def _():
                for name in mlp_units:
                    w_wait_near(name)

            mlp_near(step)
            relays(step, 3)

        return 0

    lax.fori_loop(0, SLOTS + 1, step_body, 0)

    for slot in range(ONLY):
        clip = only_clip(other_chip, core, slot)
        e_far(slot, clip).wait_recv()
        e_relay(slot, clip).start()
    for slot in range(SLOTS):
        clip = clip_of(chip, core, slot)
        e_local(slot, clip).wait()
        e_sib(slot, clip).wait_send()
        e_sib(slot, clip_of(chip, other_core, slot)).wait_recv()
    for slot in range(ONLY):
        e_far(slot, only_clip(chip, core, slot)).wait_send()
        e_relay(slot, only_clip(other_chip, core, slot)).wait_send()
        e_relay(slot, only_clip(other_chip, other_core, slot)).wait_recv()
    for slot in range(SLOTS):
        for link in range(3):
            x_copy(slot, link).wait_send()
    for name in units:
        w_drain(name)
    for link in range(3):
        s_copy(link, tp).wait_send()


def encode(x, weights, vectors):
    dma = pltpu.SemaphoreType.DMA
    any_spec = pl.BlockSpec(memory_space=pl.ANY)
    return pl.pallas_call(
        encoder_kernel,
        out_shape=jax.ShapeDtypeStruct((CLIPS, FRAMES, WIDTH), BF16),
        in_specs=[any_spec] * 7 + [pl.BlockSpec(memory_space=pltpu.VMEM)] * 11,
        out_specs=any_spec,
        scratch_shapes=[
            pltpu.VMEM((8, WIDTH), F32), pltpu.VMEM((8, WIDTH), F32), pltpu.VMEM((8, HIDDEN), F32),
            pltpu.VMEM((SLOTS, FRAMES, WIDTH), BF16),
            pltpu.VMEM((2 * WIDTH, WIDTH), BF16), pltpu.VMEM((WIDTH, WIDTH), BF16), pltpu.VMEM((WIDTH, WIDTH), BF16),
            pltpu.VMEM((WIDTH, HIDDEN), BF16), pltpu.VMEM((HIDDEN, WIDTH), BF16),
            pltpu.VMEM((4, 8, WIDTH), F32),
            pltpu.VMEM((FRAMES, WIDTH), BF16), pltpu.VMEM((FRAMES, 2 * WIDTH), BF16), pltpu.VMEM((WIDTH, FRAMES), BF16),
            pltpu.VMEM((FRAMES, WIDTH), BF16),
            pltpu.VMEM((SLOTS, FRAMES, WIDTH), BF16),
            pltpu.VMEM((FRAMES, 2 * WIDTH), BF16),
            pltpu.VMEM((SLOTS, FRAMES, WIDTH), F32),
            pltpu.VMEM((8, 2 * WIDTH), F32),
            dma((SLOTS, 3)), dma((SLOTS, 3)), dma((SLOTS,)),
            dma((9, 5)), dma((9, 5)), dma((9,)),
            dma((3,)), dma((3,)),
            dma((SLOTS + 2 * ONLY,)), dma((SLOTS + 2 * ONLY,)), dma((SLOTS,)),
        ],
        compiler_params=pltpu.CompilerParams(collective_id=0, has_side_effects=True, vmem_limit_bytes=64 * 1024 * 1024 - 128 * 1024),
        name="encoder",
    )(x, *weights, *vectors)


def cache_kernel(e_hbm, wk_hbm, wv_hbm, bias_ref, k_hbm, v_hbm, enc_hbm, weights, shift, ebuf, obuf, w_sem, e_sem, out_sem, enc_sem):
    tp = lax.axis_index("tp")

    def load(clip):
        return pltpu.make_async_copy(e_hbm.at[clip], ebuf.at[clip], e_sem.at[clip])

    def stores(clip, slot):
        copies = []
        for which, dst in enumerate((k_hbm, v_hbm)):
            for layer in range(4):
                rows = pl.ds(which * WIDTH + layer * LOC_COLS, LOC_COLS)
                copies.append(pltpu.make_async_copy(obuf.at[slot, rows, :], dst.at[layer, clip], out_sem.at[slot, which * 4 + layer]))
        return copies

    def enc_store(clip):
        own = pl.ds(pl.multiple_of(tp * LOC_FRAMES, LOC_FRAMES), LOC_FRAMES)
        return pltpu.make_async_copy(ebuf.at[clip, own, :], enc_hbm.at[clip], enc_sem.at[clip])

    load(0).start()
    weight_loads = [pltpu.make_async_copy(src.at[layer], weights.at[pl.ds(which * WIDTH + layer * LOC_COLS, LOC_COLS), :], w_sem.at[which, layer])
                    for which, src in enumerate((wk_hbm, wv_hbm)) for layer in range(4)]
    for copy in weight_loads:
        copy.start()
    for clip in range(1, AHEAD):
        load(clip).start()
    rows = jnp.concatenate([bias_ref[...].astype(F32), jnp.zeros((4, LOC_COLS), F32)], axis=0)
    for layer in range(4):
        pick = (lax.broadcasted_iota(jnp.int32, (8, 128), 0) == layer).astype(F32)
        shift[layer * LOC_COLS:(layer + 1) * LOC_COLS, :] = dot(rows, pick, TN)
    for copy in weight_loads:
        copy.wait()

    def body(step, _):
        for half in range(2):
            clip = 2 * step + half
            slot = clip % OUT_SLOTS
            load(clip).wait()
            enc_store(clip).start()

            @pl.when(clip + AHEAD < CLIPS)
            def _():
                load(clip + AHEAD).start()

            @pl.when(clip >= OUT_SLOTS)
            def _():
                for copy in stores(clip - OUT_SLOTS, slot):
                    copy.wait()

        for half in range(2):
            clip = 2 * step + half
            slot = clip % OUT_SLOTS
            obuf[slot, 0:WIDTH, :] = dot(weights[0:WIDTH, :], ebuf[clip], NT).astype(BF16)
            obuf[slot, WIDTH:2 * WIDTH, :] = (dot(weights[WIDTH:2 * WIDTH, :], ebuf[clip], NT) + jnp.concatenate([shift[...]] * 4, axis=1)).astype(BF16)
        for half in range(2):
            clip = 2 * step + half
            for copy in stores(clip, clip % OUT_SLOTS):
                copy.start()
        return 0

    lax.fori_loop(0, CLIPS // 2, body, 0)
    for clip in range(CLIPS - OUT_SLOTS, CLIPS):
        for copy in stores(clip, clip % OUT_SLOTS):
            copy.wait()
    for clip in range(CLIPS):
        enc_store(clip).wait()


def caches(e_all, wck_t, wcv_t, bias):
    cache = jax.ShapeDtypeStruct((4, CLIPS, LOC_COLS, FRAMES), BF16)
    any_spec = pl.BlockSpec(memory_space=pl.ANY)
    dma = pltpu.SemaphoreType.DMA
    return pl.pallas_call(
        cache_kernel,
        out_shape=(cache, cache, jax.ShapeDtypeStruct((CLIPS, LOC_FRAMES, WIDTH), BF16)),
        in_specs=[any_spec, any_spec, any_spec, pl.BlockSpec(memory_space=pltpu.VMEM)],
        out_specs=(any_spec, any_spec, any_spec),
        scratch_shapes=[
            pltpu.VMEM((2 * WIDTH, WIDTH), BF16), pltpu.VMEM((WIDTH, 128), F32),
            pltpu.VMEM((CLIPS, FRAMES, WIDTH), BF16), pltpu.VMEM((OUT_SLOTS, 2 * WIDTH, FRAMES), BF16),
            dma((2, 4)), dma((CLIPS,)), dma((OUT_SLOTS, 8)), dma((CLIPS,)),
        ],
        compiler_params=pltpu.CompilerParams(vmem_limit_bytes=64 * 1024 * 1024 - 128 * 1024),
        name="caches",
    )(e_all, wck_t, wcv_t, bias)


def device_body(hidden_loc, ln1_gain, ln1_bias, w_q, b_q, w_k, w_v, b_v, w_o, b_o, ln2_gain, ln2_bias, w_fc1, b_fc1, w_fc2, b_fc2, post_gain, post_bias, w_ck, w_cv, b_cv):
    weights = (w_q.T, w_k.T, w_v.T, w_o, w_fc1, w_fc2)
    vectors = (ln1_gain, ln1_bias, ln2_gain, ln2_bias, post_gain, post_bias, b_o, b_fc2, b_fc1, b_q, b_v)
    e_all = encode(hidden_loc, weights, vectors)
    k_t, v_t, enc_loc = caches(e_all, w_ck.transpose(0, 2, 1), w_cv.transpose(0, 2, 1), b_cv)
    shape = (4, CLIPS, FRAMES, 3, HEAD_DIM)
    return enc_loc, k_t.transpose(0, 1, 3, 2).reshape(shape), v_t.transpose(0, 1, 3, 2).reshape(shape)


def solution(mesh):
    in_specs = (P("dp", "tp", None), P(), P(), P(None, "tp"), P("tp"), P(None, "tp"), P(None, "tp"), P("tp"), P("tp", None), P(), P(), P(), P(None, "tp"), P("tp"), P("tp", None), P(), P(), P(), P(None, None, "tp"), P(None, None, "tp"), P(None, "tp"))
    out_specs = (P("dp", "tp", None), P(None, "dp", None, "tp", None), P(None, "dp", None, "tp", None))
    return jax.shard_map(device_body, mesh=mesh, in_specs=in_specs, out_specs=out_specs, check_vma=False)
```
